32 devices in a mesh: grp: 2 (over x), space: 16 (over z, y, core).
Axes of the slice: x: 2, y: 2, z: 4, core: 2. Of those that a mesh axis runs over, the one named last changes fastest.
Arguments:
- propagator: bfloat16 [4, 3, 4, 12, 32768], P('grp', None, None, None, 'space'), parts along dimension 0, may hold values from -6 to 6
- eigvecs: bfloat16 [4, 3, 256, 32768], P('grp', None, None, 'space'), parts along dimension 0, may hold values from -6 to 6
- operator_weights: float32 [256, 2, 256], P('grp'), parts along dimension 0, may hold values from -0.375 to 0.375
- sink_time: int32 [2], P('grp'), parts along dimension 0, may hold values from 0 to 127
- term_index: int32 [48, 3], replicated, may hold values from 0 to 11
- term_sign: int32 [48], replicated, may hold values from 0 to 1
- solver_order: int32 [32768], P('space'), may hold values from 0 to 32767, as said below
Outputs:
- solver_source: bfloat16 [4, 3, 4, 12, 32768], P('grp', None, None, None, 'space'), parts along dimension 0
The draws below stay inside these ranges and needn't reach their ends.
There are 2 independent parts, one for each index of `grp`. The reference program is written for one: setup_inputs(seed, part) draws one part's arguments, and reference() takes and returns one part's arrays. A program takes and returns all parts, laid end to end along the dimension named above; an argument that names none is the same for every part. Nothing has to cross between parts.
Inputs may be any that keep to these rules, and one draw needn't show every extreme that they name: solver_order is a permutation of the sites; split into blocks of 2048 positions and each block into pieces of 128, piece d of block e holds only sites d * 2048 to (d + 1) * 2048 - 1.
All inputs are finite; a program needn't handle non-finite values.
Results may differ from the reference program's by a relative error of at most 0.006.
Values may be sent and summed in bfloat16 or wider, within the bound.
A program may use at most 64 MiB of HBM per device.

```python
import math
import jax
import jax.numpy as jnp
from jax import lax

NVEC = 256
NMOM = 4
NTERM = 48
EXTENT = 64
TIME_EXTENT = 128
SITES_DEV = 2048
SITES = 32768
PAIR = 128


def one_permutation(block_key):
    return jax.random.permutation(block_key, SITES_DEV)


def draw_solver_order(key, part):
    owners_count = SITES // SITES_DEV
    block_keys = jax.random.split(jax.random.fold_in(key, 17), owners_count)
    shuffled = jax.vmap(one_permutation)(block_keys).astype(jnp.int32).reshape(owners_count, owners_count, PAIR)
    owner_start = (jnp.arange(owners_count, dtype=jnp.int32) * SITES_DEV)[:, None, None]
    ordered = (shuffled + owner_start).transpose(1, 0, 2)
    return ordered.reshape(SITES)


def place_ends(values, stream_key, smallest, top_value):
    spot = [jax.random.randint(jax.random.fold_in(stream_key, axis), (), 0, length) for axis, length in enumerate(values.shape)]
    main_axis = values.shape.index(max(values.shape))
    next_to = spot[:main_axis] + [(spot[main_axis] + 1) % values.shape[main_axis]] + spot[main_axis + 1:]
    return values.at[tuple(spot)].set(smallest).at[tuple(next_to)].set(top_value)


def spiked(entries, own_key, source, target, blocks, factor):
    def block_of(dim):
        return (jnp.arange(entries.shape[dim]) // (entries.shape[dim] // blocks)).reshape((-1,) + (1,) * (entries.ndim - 1 - dim))

    near = jax.random.permutation(own_key, blocks)[block_of(target)]
    far = (block_of(target) + blocks // 2) % blocks
    return jnp.where((block_of(source) == near) | (block_of(source) == far), factor * entries, entries)


def steps_of(rng, extent, shards, smallest, top_value):
    loudness = 1.0
    for position, parts in shards:
        draws = jax.random.uniform(jax.random.fold_in(jax.random.fold_in(rng, 6), position), (parts,), jnp.float32, smallest / len(shards), top_value / len(shards))
        loudness = loudness * jnp.repeat(jnp.exp(draws), extent[position] // parts).reshape((-1,) + (1,) * (len(extent) - 1 - position))
    return loudness


def normal_values(own_key, dims, scale, bound, cuts=(), kind=jnp.bfloat16):
    result = jax.random.normal(own_key, dims, jnp.float32) * scale
    if len(cuts) > 0:
        result = steps_of(own_key, dims, cuts, -0.22, 0.18) * result
    return jnp.clip(result, min=-bound, max=bound).astype(kind)


def gaussian_with(key, dims, spread, limit, cuts, heavy, held_as=jnp.bfloat16):
    values = spread * jax.random.normal(key, dims, jnp.float32)
    if cuts:
        values = values * steps_of(key, dims, cuts, -0.22, 0.18)
    return jnp.clip(spiked(values, jax.random.fold_in(key, 3), *heavy), -limit, limit).astype(held_as)


def setup_inputs(seed: int = 0, part: int = 0) -> dict:
    splits = jax.random.split(jax.random.key(seed), 8)
    part_splits = jax.random.split(jax.random.fold_in(splits[7], part), 8)
    return {
        "propagator": normal_values(part_splits[0], (2, 3, 4, 12, SITES), 1.0, 6.0, ((4, 16),)),
        "eigvecs": gaussian_with(part_splits[1], (2, 3, NVEC, SITES), 1.0, 6.0, ((3, 16),), (3, 2, 16, 2.0)),
        "operator_weights": normal_values(part_splits[2], (TIME_EXTENT, 2, NVEC), NVEC ** -0.5, 0.375, (), jnp.float32),
        "sink_time": jax.random.randint(part_splits[3], (1,), 0, TIME_EXTENT).astype(jnp.int32),
        "term_index": place_ends(jax.random.randint(splits[4], (NTERM, 3), 0, 12), jax.random.fold_in(splits[4], 1), 0, 11).astype(jnp.int32),
        "term_sign": place_ends(jax.random.randint(splits[5], (NTERM,), 0, 2), jax.random.fold_in(splits[5], 1), 0, 1).astype(jnp.int32),
        "solver_order": draw_solver_order(jax.random.fold_in(splits[7], 71), part),
    }


MOMENTA = ((0, 0, 0), (1, 0, 0), (0, 1, 0), (0, 0, 1))
PRECISE = lax.Precision.HIGHEST

def phase_tables(offset, length):
    site_index = offset + jnp.arange(length, dtype=jnp.int32)
    coord_x = site_index % EXTENT
    coord_y = site_index // EXTENT % EXTENT
    coord_z = site_index // (EXTENT * EXTENT)
    windings = jnp.stack([(step_x * coord_x + step_y * coord_y + step_z * coord_z) % EXTENT for step_x, step_y, step_z in MOMENTA])
    angles = windings.astype(jnp.float32) * (2.0 * math.pi / EXTENT)
    return (jnp.cos(angles), jnp.sin(angles))

def phased_rows(prop_colour, cosine_table, sine_table):
    real_part = prop_colour[0].astype(jnp.float32)[None]
    imag_part = prop_colour[1].astype(jnp.float32)[None]
    cos_rows = cosine_table[:, None, None, :]
    sin_rows = sine_table[:, None, None, :]
    turned = jnp.stack([cos_rows * real_part + sin_rows * imag_part, cos_rows * imag_part - sin_rows * real_part])
    return turned.astype(jnp.bfloat16).reshape(-1, turned.shape[-1])

def project(eig_colour, phased, scale_in):
    from_real = jnp.dot(eig_colour[0], phased.T, preferred_element_type=jnp.float32).reshape(-1, 2, NMOM, 48)
    from_imag = jnp.dot(eig_colour[1], phased.T, preferred_element_type=jnp.float32).reshape(-1, 2, NMOM, 48)
    real_part = from_real[:, 0] + from_imag[:, 1]
    imag_part = from_real[:, 1] - from_imag[:, 0]
    return jnp.stack([real_part, imag_part]) * scale_in

def assemble(pieces):
    stacked = jnp.stack(pieces)
    vectors = stacked.shape[2]
    return stacked.transpose(3, 1, 2, 0, 4).reshape(NMOM, 2, vectors, 144)

def weighted_total(blocks, weights):
    real_sum = jnp.einsum('k,pkc->pc', weights[0], blocks[:, 0], precision=PRECISE) - jnp.einsum('k,pkc->pc', weights[1], blocks[:, 1], precision=PRECISE)
    imag_sum = jnp.einsum('k,pkc->pc', weights[0], blocks[:, 1], precision=PRECISE) + jnp.einsum('k,pkc->pc', weights[1], blocks[:, 0], precision=PRECISE)
    return jnp.stack([real_sum, imag_sum], axis=1)

def term_tables(term_index, term_sign):
    channels = jnp.arange(12, dtype=jnp.int32)
    first_pick = (term_index[:, 0:1] == channels[None]).astype(jnp.float32)
    second_pick = (term_index[:, 1:2] == channels[None]).astype(jnp.float32)
    sign_values = (2 * term_sign - 1).astype(jnp.float32)
    placement = (term_index[None, :, 2] == channels[:, None]).astype(jnp.float32) * sign_values[None]
    return (first_pick, second_pick, placement)

def contract(blocks, weighted, first_pick, second_pick, placement):
    vectors = blocks.shape[2]
    block_grid = blocks.reshape(NMOM, 2, vectors, 12, 12)
    first_terms = jnp.einsum('mi,pqkij->pqkmj', first_pick, block_grid, precision=PRECISE)
    second_terms = jnp.einsum('mi,pqij->pqmj', second_pick, weighted.reshape(NMOM, 2, 12, 12), precision=PRECISE)[:, :, None]
    real_part = first_terms[:, 0] * second_terms[:, 0] - first_terms[:, 1] * second_terms[:, 1]
    imag_part = first_terms[:, 0] * second_terms[:, 1] + first_terms[:, 1] * second_terms[:, 0]
    product = jnp.stack([real_part, imag_part], axis=1)
    return jnp.einsum('cm,pqkmj->pqkcj', placement, product, precision=PRECISE).reshape(NMOM, 2, vectors, 144)

def rebuild(coeffs, eig_colour, colour, cosine_table, sine_table, scale_out):
    vectors = coeffs.shape[2]
    colour_block = coeffs.reshape(NMOM, 2, vectors, 3, 48)[:, :, :, colour]
    coeff_table = colour_block.transpose(2, 1, 0, 3).reshape(vectors, 2 * NMOM * 48)
    from_real = jnp.dot(coeff_table.T, eig_colour[0], preferred_element_type=jnp.float32).reshape(2, NMOM, 48, -1)
    from_imag = jnp.dot(coeff_table.T, eig_colour[1], preferred_element_type=jnp.float32).reshape(2, NMOM, 48, -1)
    real_part = from_real[0] - from_imag[1]
    imag_part = from_real[1] + from_imag[0]
    cos_rows = cosine_table[:, None, :]
    sin_rows = sine_table[:, None, :]
    out_real = lax.optimization_barrier(jnp.sum(cos_rows * real_part - sin_rows * imag_part, axis=0))
    out_imag = lax.optimization_barrier(jnp.sum(cos_rows * imag_part + sin_rows * real_part, axis=0))
    return jnp.stack([out_real, out_imag]) * scale_out

def reference(propagator, eigvecs, operator_weights, sink_time, term_index, term_sign, solver_order):
    cosine_table, sine_table = phase_tables(0, SITES)
    scale_in = 1.0 / math.sqrt(3.0 * SITES)
    pieces = []
    for colour in range(3):
        phased = phased_rows(propagator[:, colour], cosine_table, sine_table)
        pieces.append(project(eigvecs[:, colour], phased, scale_in))
    blocks = assemble(pieces)
    weights = lax.dynamic_index_in_dim(operator_weights, sink_time[0], 0, keepdims=False)
    first_pick, second_pick, placement = term_tables(term_index, term_sign)
    weighted = weighted_total(blocks, weights)
    coeffs = contract(blocks, weighted, first_pick, second_pick, placement).astype(jnp.bfloat16)
    scale_out = 1.0 / math.sqrt(NMOM * NVEC)
    colours = [rebuild(coeffs, eigvecs[:, colour], colour, cosine_table, sine_table, scale_out) for colour in range(3)]
    source = jnp.stack(colours, axis=1).astype(jnp.bfloat16).reshape(2, 3, 4, 12, SITES)
    return jnp.take(source, solver_order, axis=4)
```

```python
import functools
import math

import jax
import jax.numpy as jnp
from jax import lax
from jax.experimental import pallas as pl
from jax.experimental.pallas import tpu as pltpu
from jax.sharding import PartitionSpec as P

NMOM = 4
EXTENT = 64
MOMENTA = ((0, 0, 0), (1, 0, 0), (0, 1, 0), (0, 0, 1))
F32 = jnp.float32
BF16 = jnp.bfloat16
MESH = pl.DeviceIdType.MESH


def swap_halves(x):
    top, bottom = x[..., :4, :], x[..., 4:, :]
    return jnp.concatenate([-bottom, top], axis=-2)


def dot_exact(a, b):
    high = b.astype(BF16)
    low = (b - high.astype(F32)).astype(BF16)
    return jnp.dot(a, high, preferred_element_type=F32) + jnp.dot(a, low, preferred_element_type=F32)


def kernel(
    n, units, columns, scale_in, scale_out, chunk, moving, fixed, direct,
    prop_hbm, eig_hbm, sink, table_hbm, term_rows, term_sign, order, out,
    prop, eig, table_weights, trig, acc, blocks, from_core, summed, from_chips, coeffs, lhs,
    source, wanted, onehot, staged,
    load_sem, core_recv, chip_recv, all_recv, fwd_recv, sems,
):
    me = lax.axis_index("space")
    chips = n // 2
    half = chips // 2
    core = lax.rem(me, 2)
    chip = me // 2
    side = chip // half
    partner = me + 1 - 2 * core
    length = eig.shape[-1]
    nvec = eig.shape[2]
    piece = order.shape[-1]
    filled = NMOM * columns // (2 * units)
    steps = length // chunk
    plan = (0,) + moving
    base_rows = columns * 8
    rows = len(plan) * base_rows
    core_send, chip_send, all_send, fwd_send, index_send, index_recv, out_send, out_recv, own_sem = (
        sems.at[i] for i in range(9)
    )

    def each(lower, upper, body):
        def step(i, carry):
            body(i)
            return carry

        lax.fori_loop(lower, upper, step, 0)

    def far_chips(body):
        each(0, half, lambda t: body((1 - side) * half + lax.rem(chip + t, half)))

    def near_chips(body):
        each(1, half, lambda t: body(side * half + lax.rem(chip + t, half)))

    def remote(src, dst, send_sem, recv_sem, device):
        return pltpu.make_async_remote_copy(
            src_ref=src, dst_ref=dst, send_sem=send_sem, recv_sem=recv_sem,
            device_id={"space": device}, device_id_type=MESH,
        )

    def sent(ref, sem):
        remote(ref, ref, sem, sem, partner).wait_send()

    def landed(ref, sem):
        remote(ref, ref, sem, sem, partner).wait_recv()

    loads = []
    for colour in range(3):
        pair = (
            pltpu.make_async_copy(prop_hbm.at[:, colour], prop.at[:, colour], load_sem.at[colour]),
            pltpu.make_async_copy(eig_hbm.at[:, colour], eig.at[:, colour], load_sem.at[3 + colour]),
        )
        for load in pair:
            load.start()
        loads.append(pair)
    table_load = pltpu.make_async_copy(table_hbm, table_weights, load_sem.at[6])
    table_load.start()

    barrier = pltpu.get_barrier_semaphore()
    each(1, n, lambda t: pl.semaphore_signal(
        barrier, inc=1, device_id={"space": lax.rem(me + t, n)}, device_id_type=MESH
    ))

    bits = EXTENT.bit_length() - 1
    low = EXTENT - 1

    def angles(p, site):
        coords = (site & low, (site >> bits) & low, site >> (2 * bits))
        winding = sum(step * coord for step, coord in zip(MOMENTA[p], coords) if step) & low
        return winding.astype(F32) * (2.0 * math.pi / EXTENT)

    tiles = length // 128
    compact = me * length + 128 * lax.broadcasted_iota(
        jnp.int32, (tiles, 128), 0
    ) + lax.broadcasted_iota(jnp.int32, (tiles, 128), 1)
    for slot, p in enumerate(moving):
        angle = angles(p, compact)
        for part, values in enumerate((jnp.cos(angle), jnp.sin(angle))):
            trig[2 * slot + part : 2 * slot + part + 1, :] = jnp.concatenate(
                [values[tile : tile + 1] for tile in range(tiles)], axis=1
            )
    turns = []
    for p in fixed:
        angle = angles(p, me * length + jnp.zeros((1, nvec), jnp.int32))
        turns.append((jnp.cos(angle)[None], jnp.sin(angle)[None]))

    if filled < chips:
        blocks[:, filled:] = jnp.zeros((3, chips - filled) + blocks.shape[2:], F32)

    def core_copy(colour):
        return remote(
            blocks.at[colour, :, 1 - core], from_core.at[colour], core_send,
            core_recv.at[colour], partner,
        )

    def send_sums(colour):
        core_copy(colour).wait_recv()

        def send(other):
            summed[colour, pl.ds(other, 1)] = (
                blocks[colour, pl.ds(other, 1), pl.ds(core, 1)][:, 0]
                + from_core[colour, pl.ds(other, 1)]
            ).astype(BF16)
            remote(
                summed.at[colour, other], from_chips.at[colour, chip], chip_send,
                chip_recv.at[colour], other * 2 + core,
            ).start()

        far_chips(send)
        near_chips(send)

    for colour in range(3):
        for load in loads[colour]:
            load.wait()
        acc[...] = jnp.zeros_like(acc)

        def project(step, colour=colour):
            sites = pl.ds(pl.multiple_of(step * chunk, chunk), chunk)
            real = prop[0, colour, :, :, sites].astype(F32)
            imag = prop[1, colour, :, :, sites].astype(F32)
            straight = jnp.concatenate([real, imag], axis=1)
            crossed = jnp.concatenate([imag, -real], axis=1)
            first, second = [straight], [crossed]
            for slot in range(len(moving)):
                cosine = trig[2 * slot : 2 * slot + 1, sites][None]
                sine = trig[2 * slot + 1 : 2 * slot + 2, sites][None]
                first.append(cosine * straight + sine * crossed)
                second.append(cosine * crossed - sine * straight)
            first = jnp.concatenate(first).reshape(rows, chunk).astype(BF16)
            second = jnp.concatenate(second).reshape(rows, chunk).astype(BF16)
            dims = (((1,), (1,)), ((), ()))
            acc[...] += lax.dot_general(
                first, eig[0, colour, :, sites], dims, preferred_element_type=F32
            ) + lax.dot_general(
                second, eig[1, colour, :, sites], dims, preferred_element_type=F32
            )

        each(0, steps, project)
        made = (acc[...] * scale_in).reshape(len(plan) * columns, 8, nvec)
        still = made[:columns]
        crossed = swap_halves(still)
        made = jnp.concatenate(
            [made] + [cosine * still - sine * crossed for cosine, sine in turns]
        )
        blocks[colour, :filled] = made.reshape(filled, 2, units, 8, nvec)
        if colour == 0:
            pl.semaphore_wait(barrier, n - 1)
            core_copy(0).start()

            def send_index(t):
                peer = lax.rem(me + t, n)
                remote(order.at[peer], wanted.at[me], index_send, index_recv, peer).start()

            each(1, n, send_index)
            wanted[pl.ds(me, 1)] = order[pl.ds(me, 1)]
        else:
            core_copy(colour).start()
            send_sums(colour - 1)
    send_sums(2)

    landed(wanted.at[pl.ds(0, n - 1)], index_recv)

    def build(peer_chip):
        position = lax.broadcasted_iota(jnp.int32, (length, piece), 0)
        for which in range(2):
            local = wanted[pl.ds(peer_chip * 2 + which, 1)][0] - me * length
            onehot[pl.ds(peer_chip, 1), :, which * piece : (which + 1) * piece] = jnp.where(
                position == local, 1.0, 0.0
            ).astype(BF16)[None]

    each(0, chips, build)

    terms = term_rows.shape[1]
    eye = lax.broadcasted_iota(jnp.int32, (terms, terms), 0) == lax.broadcasted_iota(
        jnp.int32, (terms, terms), 1
    )
    lane = lax.broadcasted_iota(jnp.int32, (terms, 24), 1)
    lane_channel = (4 * (lane >> 3) + (lane & 3)).astype(F32)
    lane_imag = (lane >> 2) & 1
    picks = []
    for which in range(2):
        row = term_rows[which : which + 1, :].astype(F32)
        column = jnp.sum(jnp.where(eye, row, 0.0), axis=1, keepdims=True)
        for part in range(2):
            hit = (lane_channel == column) & (lane_imag == part)
            picks.append(jnp.where(hit, 1.0, 0.0))
    picks = jnp.concatenate(picks).astype(BF16)
    sub = lax.broadcasted_iota(jnp.int32, (24, terms), 0)
    target = 4 * (sub >> 3) + (sub & 3) == term_rows[2:3, :]
    signs = (2 * term_sign[...] - 1).astype(F32)
    place_real = jnp.where(target & (((sub >> 2) & 1) == 0), signs, 0.0).astype(BF16)
    place_imag = jnp.where(target & (((sub >> 2) & 1) == 1), signs, 0.0).astype(BF16)
    table_load.wait()
    weights = table_weights[sink[0]]
    weight_real, weight_imag = weights[0:1, :], weights[1:2, :]

    totals = []
    for colour in range(3):
        own = blocks[colour, pl.ds(chip, 1), pl.ds(core, 1)][:, 0]
        own = (own + from_core[colour, pl.ds(chip, 1)]).reshape(units * 8, nvec)
        landed(from_chips.at[colour, pl.ds(0, chips - 1)], chip_recv.at[colour])

        def add_sum(t, total, colour=colour):
            other = lax.rem(chip + chips - t, chips)
            part = from_chips[colour, pl.ds(other, 1)].astype(F32)
            return total + part.reshape(units * 8, nvec)

        totals.append(lax.fori_loop(1, chips, add_sum, own))

    block = jnp.concatenate([
        jnp.concatenate([total[unit * 8 : (unit + 1) * 8] for total in totals])
        for unit in range(units)
    ], axis=1)
    picked = dot_exact(picks, block)
    first_real, first_imag = picked[:terms], picked[terms : 2 * terms]
    other_real, other_imag = picked[2 * terms : 3 * terms], picked[3 * terms :]
    real_products, imag_products = [], []
    for unit in range(units):
        lanes = slice(unit * nvec, (unit + 1) * nvec)
        o_real, o_imag = other_real[:, lanes], other_imag[:, lanes]
        f_real, f_imag = first_real[:, lanes], first_imag[:, lanes]
        second_real = jnp.sum(weight_real * o_real - weight_imag * o_imag, axis=1, keepdims=True)
        second_imag = jnp.sum(weight_real * o_imag + weight_imag * o_real, axis=1, keepdims=True)
        real_products.append(f_real * second_real - f_imag * second_imag)
        imag_products.append(f_real * second_imag + f_imag * second_real)
    made = dot_exact(place_real, jnp.concatenate(real_products, axis=1)) + dot_exact(
        place_imag, jnp.concatenate(imag_products, axis=1)
    )
    for unit in range(units):
        part = made[:, unit * nvec : (unit + 1) * nvec].reshape(3, 8, nvec).astype(BF16)
        for colour in range(3):
            coeffs[colour, pl.ds(core, 1), pl.ds(chip, 1), unit] = part[colour : colour + 1][None]

    for colour in range(3):
        def send_coeffs(other, colour=colour):
            remote(
                coeffs.at[colour, core, chip], coeffs.at[colour, core, chip], all_send,
                all_recv.at[colour], other * 2 + core,
            ).start()

        far_chips(send_coeffs)
        near_chips(send_coeffs)

    def relay(colour):
        landed(coeffs.at[colour, core, pl.ds(0, chips - 1)], all_recv.at[colour])
        remote(
            coeffs.at[colour, core], coeffs.at[colour, core], fwd_send, fwd_recv.at[colour], partner
        ).start()

    def place_of(colour):
        if direct:
            return out.at[:, colour, :, :, pl.ds(pl.multiple_of(me * piece, piece), piece)]
        return out.at[me, colour]

    relay(0)
    for colour in range(3):
        landed(coeffs.at[colour, 1 - core], fwd_recv.at[colour])
        table = jnp.stack([coeffs[colour, 0], coeffs[colour, 1]], axis=1).astype(F32)
        table = table.reshape(n * units, 8, nvec)[: NMOM * columns].reshape(NMOM, columns, 8, nvec)
        still = table[0]
        for i, (cosine, sine) in enumerate(turns):
            turned = table[len(plan) + i]
            still = still + cosine * turned + sine * swap_halves(turned)
        real_rows, imag_rows = [], []
        for slot in range(len(plan)):
            group = still if slot == 0 else table[slot]
            reals = jnp.concatenate([group[j, :4] for j in range(columns)])
            imags = jnp.concatenate([group[j, 4:] for j in range(columns)])
            real_rows += [reals, imags]
            imag_rows += [-imags, reals]
        lhs[0] = jnp.concatenate(real_rows).astype(BF16)
        lhs[1] = jnp.concatenate(imag_rows).astype(BF16)

        def rebuild(step, colour=colour):
            sites = pl.ds(pl.multiple_of(step * chunk, chunk), chunk)
            grid = jnp.dot(
                lhs[0], eig[0, colour, :, sites], preferred_element_type=F32
            ) + jnp.dot(lhs[1], eig[1, colour, :, sites], preferred_element_type=F32)
            grid = grid.reshape(len(plan), 2, base_rows // 2, chunk)
            real, imag = grid[0, 0], grid[0, 1]
            for slot in range(len(moving)):
                cosine = trig[2 * slot : 2 * slot + 1, sites]
                sine = trig[2 * slot + 1 : 2 * slot + 2, sites]
                real = real + cosine * grid[slot + 1, 0] - sine * grid[slot + 1, 1]
                imag = imag + cosine * grid[slot + 1, 1] + sine * grid[slot + 1, 0]
            source[: base_rows // 2, sites] = (real * scale_out).astype(BF16)
            source[base_rows // 2 :, sites] = (imag * scale_out).astype(BF16)

        each(0, steps, rebuild)
        if colour < 2:
            relay(colour + 1)

        def choose(peer_chip, colour=colour):
            chosen = jnp.dot(
                source[...], onehot[pl.ds(peer_chip, 1)][0], preferred_element_type=F32
            )
            for which in range(2):
                values = chosen[:, which * piece : (which + 1) * piece]
                staged[pl.ds(peer_chip * 2 + which, 1), colour] = values.reshape(
                    1, 2, columns, 4, piece
                ).astype(BF16)

        def send_pieces(other, colour=colour):
            choose(other)
            for which in range(2):
                peer = other * 2 + which
                remote(staged.at[peer, colour], place_of(colour), out_send, out_recv, peer).start()

        if colour < 2:
            far_chips(send_pieces)
            near_chips(send_pieces)
        else:
            near_chips(send_pieces)
            far_chips(send_pieces)
        choose(chip)
        remote(staged.at[partner, colour], place_of(colour), out_send, out_recv, partner).start()
        pltpu.make_async_copy(staged.at[me, colour], place_of(colour), own_sem).start()

    sent(from_core, core_send)
    sent(summed.at[:, pl.ds(0, chips - 1)], chip_send)
    sent(coeffs.at[:, 0, pl.ds(0, chips - 1)], all_send)
    sent(coeffs.at[:, 0], fwd_send)
    sent(wanted.at[pl.ds(0, n - 1)], index_send)
    pltpu.make_async_copy(staged.at[0], staged.at[0], own_sem).wait()
    sent(staged.at[pl.ds(0, n - 1)], out_send)
    landed(staged.at[pl.ds(0, n - 1)], out_recv)


def on_device(
    propagator, eigvecs, operator_weights, sink_time, term_index, term_sign, solver_order
):
    columns, length = propagator.shape[3:]
    nvec = eigvecs.shape[2]
    n = lax.axis_size("space")
    chips = n // 2
    piece = length // n
    units = -(-NMOM * columns // n)
    fixed = tuple(
        p for p in range(1, NMOM)
        if MOMENTA[p][:2] == (0, 0) and EXTENT * EXTENT % length == 0
    )
    moving = tuple(p for p in range(1, NMOM) if p not in fixed)
    assert fixed == tuple(range(len(moving) + 1, NMOM))
    rows = (1 + len(moving)) * columns * 8
    site_rows = columns * 8
    unit = (units, 8, nvec)
    direct = piece % 128 == 0
    out_shape = (2, 3, columns, 4, length) if direct else (n, 3, 2, columns, 4, piece)
    propagator = propagator.transpose(0, 1, 3, 2, 4)
    vmem = pl.BlockSpec(memory_space=pltpu.VMEM)
    smem = pl.BlockSpec(memory_space=pltpu.SMEM)
    hbm = pl.BlockSpec(memory_space=pl.ANY)
    dma = pltpu.SemaphoreType.DMA
    gathered = pl.pallas_call(
        functools.partial(
            kernel, n, units, columns, 1.0 / math.sqrt(3.0 * length * n),
            1.0 / math.sqrt(NMOM * nvec), 512, moving, fixed, direct,
        ),
        out_shape=jax.ShapeDtypeStruct(out_shape, BF16),
        in_specs=[hbm, hbm, smem, hbm, vmem, vmem, vmem],
        out_specs=hbm,
        scratch_shapes=[
            pltpu.VMEM(propagator.shape, BF16),
            pltpu.VMEM(eigvecs.shape, BF16),
            pltpu.VMEM(operator_weights.shape, F32),
            pltpu.VMEM((2 * len(moving), length), F32),
            pltpu.VMEM((rows, nvec), F32),
            pltpu.VMEM((3, chips, 2) + unit, F32),
            pltpu.VMEM((3, chips) + unit, F32),
            pltpu.VMEM((3, chips) + unit, BF16),
            pltpu.VMEM((3, chips) + unit, BF16),
            pltpu.VMEM((3, 2, chips) + unit, BF16),
            pltpu.VMEM((2, rows, nvec), BF16),
            pltpu.VMEM((site_rows, length), BF16),
            pltpu.VMEM((n, 1, piece), jnp.int32),
            pltpu.VMEM((chips, length, 2 * piece), BF16),
            pltpu.VMEM((n, 3, 2, columns, 4, piece), BF16),
            dma((7,)), dma((3,)), dma((3,)), dma((3,)), dma((3,)), dma((9,)),
        ],
        compiler_params=pltpu.CompilerParams(
            collective_id=0, has_side_effects=True, vmem_limit_bytes=60 * 2**20
        ),
    )(
        propagator, eigvecs, sink_time, operator_weights,
        term_index.T, term_sign.reshape(1, -1), solver_order.reshape(n, 1, piece),
    )
    if direct:
        return gathered.transpose(0, 1, 3, 2, 4)
    placed = gathered.transpose(2, 1, 4, 3, 0, 5)
    return placed.reshape(2, 3, 4, columns, length)


def solution(mesh):
    return jax.shard_map(
        on_device,
        mesh=mesh,
        in_specs=(
            P("grp", None, None, None, "space"),
            P("grp", None, None, "space"),
            P("grp", None, None),
            P("grp"),
            P(),
            P(),
            P("space"),
        ),
        out_specs=P("grp", None, None, None, "space"),
        check_vma=False,
    )
```

```python
import functools
import math

import jax
import jax.numpy as jnp
from jax import lax
from jax.experimental import pallas as pl
from jax.experimental.pallas import tpu as pltpu
from jax.sharding import PartitionSpec as P

NMOM = 4
EXTENT = 64
MOMENTA = ((0, 0, 0), (1, 0, 0), (0, 1, 0), (0, 0, 1))
F32 = jnp.float32
BF16 = jnp.bfloat16
MESH = pl.DeviceIdType.MESH


def swap_halves(x):
    top, bottom = x[..., :4, :], x[..., 4:, :]
    return jnp.concatenate([-bottom, top], axis=-2)


def dot_exact(a, b):
    high = b.astype(BF16)
    low = (b - high.astype(F32)).astype(BF16)
    return jnp.dot(a, high, preferred_element_type=F32) + jnp.dot(a, low, preferred_element_type=F32)


def kernel(
    n, groups, columns, scale_in, scale_out, chunk, moving, fixed, direct,
    prop_hbm, eig_hbm, sink, table_hbm, term_rows, term_sign, order, out,
    prop, eig, table_weights, trig, turn, acc, blocks, from_core, summed, from_chips, ready, coeffs,
    lhs, source, wanted, onehot, staged,
    load_sem, core_recv, chip_recv, all_recv, fwd_recv, sems,
):
    me = lax.axis_index("space")
    chips = n // 2
    half = chips // 2
    core = lax.rem(me, 2)
    chip = me // 2
    side = chip // half
    partner = me + 1 - 2 * core
    length = eig.shape[-1]
    nvec = eig.shape[2]
    piece = order.shape[-1]
    steps = length // chunk
    slots = 1 + len(moving)
    core_send, chip_send, all_send, fwd_send, index_send, index_recv, out_send, out_recv, own_sem = (
        sems.at[i] for i in range(9)
    )

    def each(lower, upper, body):
        def step(i, carry):
            body(i)
            return carry

        lax.fori_loop(lower, upper, step, 0)

    def far_chips(body):
        each(0, half, lambda t: body((1 - side) * half + lax.rem(chip + t, half)))

    def near_chips(body):
        each(1, half, lambda t: body(side * half + lax.rem(chip + t, half)))

    def remote(src, dst, send_sem, recv_sem, device):
        return pltpu.make_async_remote_copy(
            src_ref=src, dst_ref=dst, send_sem=send_sem, recv_sem=recv_sem,
            device_id={"space": device}, device_id_type=MESH,
        )

    def sent(ref, sem):
        remote(ref, ref, sem, sem, partner).wait_send()

    def landed(ref, sem):
        remote(ref, ref, sem, sem, partner).wait_recv()

    class Group:
        def __init__(self, index, start, depth):
            self.index, self.start, self.depth = index, start, depth
            self.first = 2 * start
            self.owners = 2 * depth
            self.left, self.width = 4 * start, 4 * depth
            below = chip - (half - start - depth)
            above = chip - (half + start)
            self.owns = ((below >= 0) & (below < depth)) | ((above >= 0) & (above < depth))
            self.mine = self.first + jnp.where(chip < half, below, depth + above)

        def chip_of(self, owner):
            return jnp.where(
                owner < self.depth, half - self.start - self.depth + owner,
                half + self.start + owner - self.depth,
            )

        def each_owner(self, body):
            def step(t):
                owner = lax.rem(t + (1 - side) * self.depth, self.owners)
                other = self.chip_of(owner)

                @pl.when(other != chip)
                def _():
                    body(self.first + owner, other)

            each(0, self.owners, step)

    plan, start = [], 0
    for index, depth in enumerate(groups):
        plan.append(Group(index, start, depth))
        start += depth

    loads = []
    for colour in range(3):
        loads.append((
            pltpu.make_async_copy(prop_hbm.at[:, colour], prop.at[:, colour], load_sem.at[colour]),
            pltpu.make_async_copy(eig_hbm.at[:, colour], eig.at[:, colour], load_sem.at[3 + colour]),
        ))

    def load(colour):
        for copy in loads[colour]:
            copy.start()

    load(0)
    barrier = pltpu.get_barrier_semaphore()
    each(1, n, lambda t: pl.semaphore_signal(
        barrier, inc=1, device_id={"space": lax.rem(me + t, n)}, device_id_type=MESH
    ))

    bits = EXTENT.bit_length() - 1
    low = EXTENT - 1

    def angles(p, site):
        coords = (site & low, (site >> bits) & low, site >> (2 * bits))
        winding = sum(step * coord for step, coord in zip(MOMENTA[p], coords) if step) & low
        return winding.astype(F32) * (2.0 * math.pi / EXTENT)

    tiles = length // 128
    compact = me * length + 128 * lax.broadcasted_iota(
        jnp.int32, (tiles, 128), 0
    ) + lax.broadcasted_iota(jnp.int32, (tiles, 128), 1)
    for slot, p in enumerate(moving):
        angle = angles(p, compact)
        for part, values in enumerate((jnp.cos(angle), jnp.sin(angle))):
            trig[2 * slot + part : 2 * slot + part + 1, :] = jnp.concatenate(
                [values[tile : tile + 1] for tile in range(tiles)], axis=1
            )
    for i, p in enumerate(fixed):
        angle = angles(p, 2 * length * lax.broadcasted_iota(jnp.int32, (chips, nvec), 0))
        turn[2 * i] = jnp.cos(angle)[:, None]
        turn[2 * i + 1] = jnp.sin(angle)[:, None]
    load(1)

    def core_copy(group, colour):
        owners = pl.ds(group.first, group.owners)
        return remote(
            blocks.at[colour, owners, 1 - core], from_core.at[colour, owners], core_send,
            core_recv.at[group.index, colour], partner,
        )

    def send_sums(group, colour):
        core_copy(group, colour).wait_recv()

        def send(owner, other):
            summed[colour, pl.ds(owner, 1)] = (
                blocks[colour, pl.ds(owner, 1), pl.ds(core, 1)][:, 0]
                + from_core[colour, pl.ds(owner, 1)]
            ).astype(BF16)
            remote(
                summed.at[colour, owner], from_chips.at[colour, chip], chip_send,
                chip_recv.at[colour], other * 2 + core,
            ).start()

        group.each_owner(send)

    def project(group, colour):
        rows = slots * group.width * 8
        acc[:rows] = jnp.zeros((rows, nvec), F32)
        picked = slice(group.left, group.left + group.width)

        def step(step):
            sites = pl.ds(pl.multiple_of(step * chunk, chunk), chunk)
            real = prop[0, colour, picked, :, sites].astype(F32)
            imag = prop[1, colour, picked, :, sites].astype(F32)
            straight = jnp.concatenate([real, imag], axis=1)
            crossed = jnp.concatenate([imag, -real], axis=1)
            first, second = [straight], [crossed]
            for slot in range(len(moving)):
                cosine = trig[2 * slot : 2 * slot + 1, sites][None]
                sine = trig[2 * slot + 1 : 2 * slot + 2, sites][None]
                first.append(cosine * straight + sine * crossed)
                second.append(cosine * crossed - sine * straight)
            first = jnp.concatenate(first).reshape(rows, chunk).astype(BF16)
            second = jnp.concatenate(second).reshape(rows, chunk).astype(BF16)
            dims = (((1,), (1,)), ((), ()))
            acc[:rows] += lax.dot_general(
                first, eig[0, colour, :, sites], dims, preferred_element_type=F32
            ) + lax.dot_general(
                second, eig[1, colour, :, sites], dims, preferred_element_type=F32
            )

        each(0, steps, step)
        made = (acc[:rows] * scale_in).reshape(slots, group.owners, 2, 8, nvec)
        for slot in range(slots):
            blocks[colour, group.first : group.first + group.owners, :, slot] = made[slot]

    pending = []
    for group in plan:
        for colour in range(3):
            if group.index == 0:
                for copy in loads[colour]:
                    copy.wait()
                if colour == 0:
                    load(2)
                    small_loads = (
                        pltpu.make_async_copy(table_hbm, table_weights, load_sem.at[6]),
                    )
                    for copy in small_loads:
                        copy.start()
            project(group, colour)
            if group.index == 0 and colour == 0:
                pl.semaphore_wait(barrier, n - 1)
            core_copy(group, colour).start()
            if group.index == 0 and colour == 0:

                def send_index(t):
                    peer = lax.rem(me + t, n)
                    remote(order.at[peer], wanted.at[me], index_send, index_recv, peer).start()

                each(1, n, send_index)
                wanted[pl.ds(me, 1)] = order[pl.ds(me, 1)]
            if pending:
                send_sums(*pending.pop())
            pending.append((group, colour))
    send_sums(*pending.pop())

    terms = term_rows.shape[1]
    for copy in small_loads:
        copy.wait()

    def contract(group):
        eye = lax.broadcasted_iota(jnp.int32, (terms, terms), 0) == lax.broadcasted_iota(
            jnp.int32, (terms, terms), 1
        )
        lane = lax.broadcasted_iota(jnp.int32, (terms, 24), 1)
        lane_channel = (4 * (lane >> 3) + (lane & 3)).astype(F32)
        lane_imag = (lane >> 2) & 1
        picks = []
        for which in range(2):
            row = term_rows[which : which + 1, :].astype(F32)
            column = jnp.sum(jnp.where(eye, row, 0.0), axis=1, keepdims=True)
            for part in range(2):
                hit = (lane_channel == column) & (lane_imag == part)
                picks.append(jnp.where(hit, 1.0, 0.0))
        picks = jnp.concatenate(picks).astype(BF16)
        sub = lax.broadcasted_iota(jnp.int32, (24, terms), 0)
        target = 4 * (sub >> 3) + (sub & 3) == term_rows[2:3, :]
        signs = (2 * term_sign[...] - 1).astype(F32)
        place_real = jnp.where(target & (((sub >> 2) & 1) == 0), signs, 0.0).astype(BF16)
        place_imag = jnp.where(target & (((sub >> 2) & 1) == 1), signs, 0.0).astype(BF16)
        weights = table_weights[sink[0, 0]]
        weight_real, weight_imag = weights[0:1, :], weights[1:2, :]

        totals = []
        for colour in range(3):
            own = blocks[colour, pl.ds(group.mine, 1), pl.ds(core, 1)][0, 0]
            own = own + from_core[colour, pl.ds(group.mine, 1)][0]
            landed(from_chips.at[colour, pl.ds(0, chips - 1)], chip_recv.at[colour])

            def turned(part, source_chip):
                kept = []
                for i in range(len(fixed)):
                    kept.append(turn[2 * i, pl.ds(source_chip, 1)][0] * part[0])
                    kept.append(turn[2 * i + 1, pl.ds(source_chip, 1)][0] * part[0])
                return kept

            def add_sum(t, carry, colour=colour):
                other = lax.rem(chip + chips - t, chips)
                part = from_chips[colour, pl.ds(other, 1)][0].astype(F32)
                return tuple(a + b for a, b in zip(carry, (part, *turned(part, other))))

            total, *kept = lax.fori_loop(1, chips, add_sum, (own, *turned(own, chip)))
            extra = [
                kept[2 * i] - swap_halves(kept[2 * i + 1]) for i in range(len(fixed))
            ]
            totals.append([total[slot] for slot in range(slots)] + extra)

        count = slots + len(fixed)
        block = jnp.concatenate([
            jnp.concatenate([total[unit] for total in totals]) for unit in range(count)
        ], axis=1)
        picked = dot_exact(picks, block)
        first_real, first_imag = picked[:terms], picked[terms : 2 * terms]
        other_real, other_imag = picked[2 * terms : 3 * terms], picked[3 * terms :]
        real_products, imag_products = [], []
        for unit in range(count):
            lanes = slice(unit * nvec, (unit + 1) * nvec)
            o_real, o_imag = other_real[:, lanes], other_imag[:, lanes]
            f_real, f_imag = first_real[:, lanes], first_imag[:, lanes]
            second_real = jnp.sum(
                weight_real * o_real - weight_imag * o_imag, axis=1, keepdims=True
            )
            second_imag = jnp.sum(
                weight_real * o_imag + weight_imag * o_real, axis=1, keepdims=True
            )
            real_products.append(f_real * second_real - f_imag * second_imag)
            imag_products.append(f_real * second_imag + f_imag * second_real)
        made = dot_exact(place_real, jnp.concatenate(real_products, axis=1)) + dot_exact(
            place_imag, jnp.concatenate(imag_products, axis=1)
        )
        acc[:24, :] = made[:, :nvec]
        for i in range(len(fixed)):
            acc[24 * (i + 1) : 24 * (i + 2), :] = made[:, (slots + i) * nvec : (slots + i + 1) * nvec]
        rest = made[:, nvec : slots * nvec].reshape(3, 8, (slots - 1) * nvec).astype(BF16)

        def merged(colour, other):
            value = acc[8 * colour : 8 * colour + 8, :]
            for i in range(len(fixed)):
                side_value = acc[24 * (i + 1) + 8 * colour : 24 * (i + 1) + 8 * colour + 8, :]
                value = value + turn[2 * i, pl.ds(other, 1)][0] * side_value
                value = value + turn[2 * i + 1, pl.ds(other, 1)][0] * swap_halves(side_value)
            return value.astype(BF16)

        for colour in range(3):
            others = [rest[colour, :, slot * nvec : (slot + 1) * nvec] for slot in range(slots - 1)]

            def send_coeffs(other, colour=colour, others=others):
                ready[colour, pl.ds(other, 1), 0] = merged(colour, other)[None]
                for slot in range(slots - 1):
                    ready[colour, pl.ds(other, 1), slot + 1] = others[slot][None]
                remote(
                    ready.at[colour, other], coeffs.at[colour, core, group.mine], all_send,
                    all_recv.at[group.index, colour], other * 2 + core,
                ).start()

            far_chips(send_coeffs)
            near_chips(send_coeffs)
            coeffs[colour, pl.ds(core, 1), pl.ds(group.mine, 1), 0] = merged(colour, chip)[None, None]
            for slot in range(slots - 1):
                coeffs[colour, pl.ds(core, 1), pl.ds(group.mine, 1), slot + 1] = others[slot][None, None]

    def build(peer_chip):
        position = lax.broadcasted_iota(jnp.int32, (length, piece), 0)
        for which in range(2):
            local = wanted[pl.ds(peer_chip * 2 + which, 1)][0] - me * length
            onehot[pl.ds(peer_chip, 1), :, which * piece : (which + 1) * piece] = jnp.where(
                position == local, 1.0, 0.0
            ).astype(BF16)[None]

    def build_all():
        landed(wanted.at[pl.ds(0, n - 1)], index_recv)
        each(0, chips, build)

    for i, group in enumerate(plan):
        if i == 0 and len(plan) == 1:
            build_all()
        pl.when(group.owns)(functools.partial(contract, group))
        if i == 0 and len(plan) > 1:
            build_all()

    def relay(group, colour):
        def take(count):
            landed(coeffs.at[colour, core, pl.ds(0, count)], all_recv.at[group.index, colour])

        pl.when(group.owns)(lambda: take(group.owners - 1))
        pl.when(jnp.logical_not(group.owns))(lambda: take(group.owners))
        owners = pl.ds(group.first, group.owners)
        remote(
            coeffs.at[colour, core, owners], coeffs.at[colour, core, owners], fwd_send,
            fwd_recv.at[group.index, colour], partner,
        ).start()

    def rebuild(group, colour):
        owners = pl.ds(group.first, group.owners)
        landed(coeffs.at[colour, 1 - core, owners], fwd_recv.at[group.index, colour])
        table = coeffs[colour, :, group.first : group.first + group.owners].astype(F32)
        real_rows, imag_rows = [], []
        for slot in range(slots):
            cells = [table[which, o, slot] for o in range(group.owners) for which in range(2)]
            reals = jnp.concatenate([cell[:4] for cell in cells])
            imags = jnp.concatenate([cell[4:] for cell in cells])
            real_rows += [reals, imags]
            imag_rows += [-imags, reals]
        quarter = 4 * group.width
        rows = slots * 2 * quarter
        lhs[0, :rows] = jnp.concatenate(real_rows).astype(BF16)
        lhs[1, :rows] = jnp.concatenate(imag_rows).astype(BF16)

        def step(step):
            sites = pl.ds(pl.multiple_of(step * chunk, chunk), chunk)
            grid = jnp.dot(
                lhs[0, :rows], eig[0, colour, :, sites], preferred_element_type=F32
            ) + jnp.dot(lhs[1, :rows], eig[1, colour, :, sites], preferred_element_type=F32)
            grid = grid.reshape(slots, 2, quarter, chunk)
            real, imag = grid[0, 0], grid[0, 1]
            for slot in range(len(moving)):
                cosine = trig[2 * slot : 2 * slot + 1, sites]
                sine = trig[2 * slot + 1 : 2 * slot + 2, sites]
                real = real + cosine * grid[slot + 1, 0] - sine * grid[slot + 1, 1]
                imag = imag + cosine * grid[slot + 1, 1] + sine * grid[slot + 1, 0]
            source[:quarter, sites] = (real * scale_out).astype(BF16)
            source[quarter : 2 * quarter, sites] = (imag * scale_out).astype(BF16)

        each(0, steps, step)

    def distribute(group, colour, last):
        picked = pl.ds(group.left, group.width)
        if direct:
            lanes = pl.ds(pl.multiple_of(me * piece, piece), piece)
            target = out.at[:, colour, picked, :, lanes]
        else:
            target = out.at[me, colour, :, picked]

        def choose(peer_chip):
            chosen = jnp.dot(
                source[: 8 * group.width], onehot[pl.ds(peer_chip, 1)][0], preferred_element_type=F32
            )
            for which in range(2):
                values = chosen[:, which * piece : (which + 1) * piece]
                staged[
                    pl.ds(peer_chip * 2 + which, 1), colour, :, group.left : group.left + group.width
                ] = values.reshape(1, 2, group.width, 4, piece).astype(BF16)

        def send_pieces(other):
            choose(other)
            for which in range(2):
                peer = other * 2 + which
                remote(staged.at[peer, colour, :, picked], target, out_send, out_recv, peer).start()

        if last:
            near_chips(send_pieces)
            far_chips(send_pieces)
        else:
            far_chips(send_pieces)
            near_chips(send_pieces)
        choose(chip)
        remote(staged.at[partner, colour, :, picked], target, out_send, out_recv, partner).start()
        pltpu.make_async_copy(staged.at[me, colour, :, picked], target, own_sem).start()

    work = [(group, colour) for group in plan for colour in range(3)]
    relay(*work[0])
    for i, (group, colour) in enumerate(work):
        rebuild(group, colour)
        if i + 1 < len(work):
            relay(*work[i + 1])
        distribute(group, colour, i + 1 == len(work))

    owns = functools.reduce(jnp.logical_or, [group.owns for group in plan])
    total_owners = 2 * sum(groups)

    def sent_sums(count):
        sent(summed.at[:, pl.ds(0, count)], chip_send)

    sent(from_core, core_send)

    @pl.when(owns)
    def _():
        sent_sums(total_owners - 1)
        sent(ready.at[:, pl.ds(0, chips - 1)], all_send)

    pl.when(jnp.logical_not(owns))(lambda: sent_sums(total_owners))
    sent(coeffs.at[:, 0], fwd_send)
    sent(wanted.at[pl.ds(0, n - 1)], index_send)
    pltpu.make_async_copy(staged.at[0], staged.at[0], own_sem).wait()
    sent(staged.at[pl.ds(0, n - 1)], out_send)
    landed(staged.at[pl.ds(0, n - 1)], out_recv)


def on_device(
    propagator, eigvecs, operator_weights, sink_time, term_index, term_sign, solver_order
):
    columns, length = propagator.shape[3:]
    nvec = eigvecs.shape[2]
    n = lax.axis_size("space")
    chips = n // 2
    piece = length // n
    groups = (columns // 4,)
    fixed = tuple(
        p for p in range(1, NMOM)
        if MOMENTA[p][:2] == (0, 0) and EXTENT * EXTENT % (2 * length) == 0
    )
    moving = tuple(p for p in range(1, NMOM) if p not in fixed)
    assert 4 * sum(groups) == columns and sum(groups) <= chips // 2
    slots = 1 + len(moving)
    owners = 2 * sum(groups)
    rows = slots * columns * 8
    site_rows = columns * 8
    cell = (slots, 8, nvec)
    direct = piece % 128 == 0
    out_shape = (2, 3, columns, 4, length) if direct else (n, 3, 2, columns, 4, piece)
    propagator = propagator.transpose(0, 1, 3, 2, 4)
    vmem = pl.BlockSpec(memory_space=pltpu.VMEM)
    hbm = pl.BlockSpec(memory_space=pltpu.HBM)
    dma = pltpu.SemaphoreType.DMA
    gathered = pl.pallas_call(
        functools.partial(
            kernel, n, groups, columns, 1.0 / math.sqrt(3.0 * length * n),
            1.0 / math.sqrt(NMOM * nvec), 512, moving, fixed, direct,
        ),
        out_shape=pltpu.VMEM(out_shape, BF16),
        in_specs=[hbm, hbm, pl.BlockSpec(memory_space=pltpu.SMEM), hbm, vmem, vmem, vmem],
        out_specs=pl.BlockSpec(memory_space=pl.ANY),
        scratch_shapes=[
            pltpu.VMEM(propagator.shape, BF16),
            pltpu.VMEM(eigvecs.shape, BF16),
            pltpu.VMEM(operator_weights.shape, F32),
            pltpu.VMEM((2 * len(moving), length), F32),
            pltpu.VMEM((2 * max(len(fixed), 1), chips, 1, nvec), F32),
            pltpu.VMEM((rows, nvec), F32),
            pltpu.VMEM((3, owners, 2) + cell, F32),
            pltpu.VMEM((3, owners) + cell, F32),
            pltpu.VMEM((3, owners) + cell, BF16),
            pltpu.VMEM((3, chips) + cell, BF16),
            pltpu.VMEM((3, chips) + cell, BF16),
            pltpu.VMEM((3, 2, owners) + cell, BF16),
            pltpu.VMEM((2, rows, nvec), BF16),
            pltpu.VMEM((site_rows, length), BF16),
            pltpu.VMEM((n, 1, piece), jnp.int32),
            pltpu.VMEM((chips, length, 2 * piece), BF16),
            pltpu.VMEM((n, 3, 2, columns, 4, piece), BF16),
            dma((8,)), dma((len(groups), 3)), dma((3,)), dma((len(groups), 3)), dma((len(groups), 3)),
            dma((9,)),
        ],
        compiler_params=pltpu.CompilerParams(
            collective_id=0, has_side_effects=True, vmem_limit_bytes=int(48 * 2**20)
        ),
    )(
        *(
            x if x.size == 1 else pltpu.with_memory_space_constraint(x, pltpu.HBM)
            for x in (
                propagator, eigvecs, sink_time.reshape(1, 1), operator_weights,
                term_index.T, term_sign.reshape(1, -1), solver_order.reshape(n, 1, piece),
            )
        )
    )
    if direct:
        return gathered.transpose(0, 1, 3, 2, 4)
    placed = gathered.transpose(2, 1, 4, 3, 0, 5)
    return placed.reshape(2, 3, 4, columns, length)


def solution(mesh):
    return jax.shard_map(
        on_device,
        mesh=mesh,
        in_specs=(
            P("grp", None, None, None, "space"),
            P("grp", None, None, "space"),
            P("grp", None, None),
            P("grp"),
            P(),
            P(),
            P("space"),
        ),
        out_specs=P("grp", None, None, None, "space"),
        check_vma=False,
    )
```

```python
import functools
import math

import jax
import jax.numpy as jnp
from jax import lax
from jax.experimental import pallas as pl
from jax.experimental.pallas import tpu as pltpu
from jax.sharding import PartitionSpec as P

NMOM = 4
EXTENT = 64
MOMENTA = ((0, 0, 0), (1, 0, 0), (0, 1, 0), (0, 0, 1))
F32 = jnp.float32
BF16 = jnp.bfloat16
MESH = pl.DeviceIdType.MESH


def swap_halves(x):
    top, bottom = x[..., :4, :], x[..., 4:, :]
    return jnp.concatenate([-bottom, top], axis=-2)


def dot_exact(a, b):
    high = b.astype(BF16)
    low = (b - high.astype(F32)).astype(BF16)
    return jnp.dot(a, high, preferred_element_type=F32) + jnp.dot(a, low, preferred_element_type=F32)


def kernel(
    n, groups, columns, scale_in, scale_out, chunk, moving, fixed, direct,
    prop_hbm, eig_hbm, sink, table_hbm, term_rows_hbm, term_sign_hbm, order_hbm, out,
    prop, eig, table_weights, term_rows, term_sign, order, trig, turn, acc, blocks, from_core, summed, from_chips, ready, coeffs,
    lhs, source, wanted, onehot, staged,
    load_sem, core_recv, chip_recv, all_recv, fwd_recv, sems,
):
    me = lax.axis_index("space")
    chips = n // 2
    half = chips // 2
    core = lax.rem(me, 2)
    chip = me // 2
    side = chip // half
    partner = me + 1 - 2 * core
    length = eig.shape[-1]
    nvec = eig.shape[2]
    piece = order.shape[-1]
    steps = length // chunk
    slots = 1 + len(moving)
    core_send, chip_send, all_send, fwd_send, index_send, index_recv, out_send, out_recv, own_sem = (
        sems.at[i] for i in range(9)
    )

    def each(lower, upper, body):
        def step(i, carry):
            body(i)
            return carry

        lax.fori_loop(lower, upper, step, 0)

    def far_chips(body):
        each(0, half, lambda t: body((1 - side) * half + lax.rem(chip + t, half)))

    def near_chips(body):
        each(1, half, lambda t: body(side * half + lax.rem(chip + t, half)))

    def remote(src, dst, send_sem, recv_sem, device):
        return pltpu.make_async_remote_copy(
            src_ref=src, dst_ref=dst, send_sem=send_sem, recv_sem=recv_sem,
            device_id={"space": device}, device_id_type=MESH,
        )

    def sent(ref, sem):
        remote(ref, ref, sem, sem, partner).wait_send()

    def landed(ref, sem):
        remote(ref, ref, sem, sem, partner).wait_recv()

    class Group:
        def __init__(self, index, start, depth):
            self.index, self.start, self.depth = index, start, depth
            self.first = 2 * start
            self.owners = 2 * depth
            self.left, self.width = 4 * start, 4 * depth
            below = chip - (half - start - depth)
            above = chip - (half + start)
            self.owns = ((below >= 0) & (below < depth)) | ((above >= 0) & (above < depth))
            self.mine = self.first + jnp.where(chip < half, below, depth + above)

        def chip_of(self, owner):
            return jnp.where(
                owner < self.depth, half - self.start - self.depth + owner,
                half + self.start + owner - self.depth,
            )

        def each_owner(self, body):
            def step(t):
                owner = lax.rem(t + (1 - side) * self.depth, self.owners)
                other = self.chip_of(owner)

                @pl.when(other != chip)
                def _():
                    body(self.first + owner, other)

            each(0, self.owners, step)

    plan, start = [], 0
    for index, depth in enumerate(groups):
        plan.append(Group(index, start, depth))
        start += depth

    def load_of(colour, lower, upper, sem):
        sites = slice(lower, upper)
        return (
            pltpu.make_async_copy(
                prop_hbm.at[:, colour, :, :, sites], prop.at[:, colour, :, :, sites],
                load_sem.at[sem],
            ),
            pltpu.make_async_copy(
                eig_hbm.at[:, colour, :, sites], eig.at[:, colour, :, sites], load_sem.at[sem + 1]
            ),
        )

    def start(copies):
        for copy in copies:
            copy.start()

    def finish(copies):
        for copy in copies:
            copy.wait()

    middle = length // 2
    first_loads = (load_of(0, 0, middle, 0), load_of(0, middle, length, 2))
    later_loads = (load_of(1, 0, length, 4), load_of(2, 0, length, 6))
    small_loads = tuple(
        pltpu.make_async_copy(remote_ref, own_ref, load_sem.at[8 + i])
        for i, (remote_ref, own_ref) in enumerate((
            (order_hbm, order), (table_hbm, table_weights), (term_rows_hbm, term_rows),
            (term_sign_hbm, term_sign),
        ))
    )
    start(first_loads[0])
    start(first_loads[1])
    barrier = pltpu.get_barrier_semaphore()
    each(1, n, lambda t: pl.semaphore_signal(
        barrier, inc=1, device_id={"space": lax.rem(me + t, n)}, device_id_type=MESH
    ))

    bits = EXTENT.bit_length() - 1
    low = EXTENT - 1

    def angles(p, site):
        coords = (site & low, (site >> bits) & low, site >> (2 * bits))
        winding = sum(step * coord for step, coord in zip(MOMENTA[p], coords) if step) & low
        return winding.astype(F32) * (2.0 * math.pi / EXTENT)

    tiles = length // 128
    compact = me * length + 128 * lax.broadcasted_iota(
        jnp.int32, (tiles, 128), 0
    ) + lax.broadcasted_iota(jnp.int32, (tiles, 128), 1)
    for slot, p in enumerate(moving):
        angle = angles(p, compact)
        for part, values in enumerate((jnp.cos(angle), jnp.sin(angle))):
            trig[2 * slot + part : 2 * slot + part + 1, :] = jnp.concatenate(
                [values[tile : tile + 1] for tile in range(tiles)], axis=1
            )
    for i, p in enumerate(fixed):
        angle = angles(p, 2 * length * lax.broadcasted_iota(jnp.int32, (chips, nvec), 0))
        turn[2 * i] = jnp.cos(angle)[:, None]
        turn[2 * i + 1] = jnp.sin(angle)[:, None]
    start(small_loads)
    start(later_loads[0])

    def core_copy(group, colour):
        owners = pl.ds(group.first, group.owners)
        return remote(
            blocks.at[colour, owners, 1 - core], from_core.at[colour, owners], core_send,
            core_recv.at[group.index, colour], partner,
        )

    def send_sums(group, colour):
        core_copy(group, colour).wait_recv()

        def send(owner, other):
            summed[colour, pl.ds(owner, 1)] = (
                blocks[colour, pl.ds(owner, 1), pl.ds(core, 1)][:, 0]
                + from_core[colour, pl.ds(owner, 1)]
            ).astype(BF16)
            remote(
                summed.at[colour, owner], from_chips.at[colour, chip], chip_send,
                chip_recv.at[colour], other * 2 + core,
            ).start()

        group.each_owner(send)

    def project(group, colour, between=None):
        rows = slots * group.width * 8
        acc[:rows] = jnp.zeros((rows, nvec), F32)
        picked = slice(group.left, group.left + group.width)

        def step(step):
            sites = pl.ds(pl.multiple_of(step * chunk, chunk), chunk)
            real = prop[0, colour, picked, :, sites].astype(F32)
            imag = prop[1, colour, picked, :, sites].astype(F32)
            straight = jnp.concatenate([real, imag], axis=1)
            crossed = jnp.concatenate([imag, -real], axis=1)
            first, second = [straight], [crossed]
            for slot in range(len(moving)):
                cosine = trig[2 * slot : 2 * slot + 1, sites][None]
                sine = trig[2 * slot + 1 : 2 * slot + 2, sites][None]
                first.append(cosine * straight + sine * crossed)
                second.append(cosine * crossed - sine * straight)
            first = jnp.concatenate(first).reshape(rows, chunk).astype(BF16)
            second = jnp.concatenate(second).reshape(rows, chunk).astype(BF16)
            dims = (((1,), (1,)), ((), ()))
            acc[:rows] += lax.dot_general(
                first, eig[0, colour, :, sites], dims, preferred_element_type=F32
            ) + lax.dot_general(
                second, eig[1, colour, :, sites], dims, preferred_element_type=F32
            )

        if between is None:
            each(0, steps, step)
        else:
            each(0, steps // 2, step)
            between()
            each(steps // 2, steps, step)
        made = (acc[:rows] * scale_in).reshape(slots, group.owners, 2, 8, nvec)
        for slot in range(slots):
            blocks[colour, group.first : group.first + group.owners, :, slot] = made[slot]

    pending = []
    for group in plan:
        for colour in range(3):
            if group.index > 0:
                project(group, colour)
            elif colour == 0:
                finish(first_loads[0])
                start(later_loads[1])
                project(group, colour, lambda: finish(first_loads[1]))
            else:
                finish(later_loads[colour - 1])
                project(group, colour)
            if group.index == 0 and colour == 0:
                pl.semaphore_wait(barrier, n - 1)
            core_copy(group, colour).start()
            if group.index == 0 and colour == 0:
                finish(small_loads[:1])

                def send_index(t):
                    peer = lax.rem(me + t, n)
                    remote(order.at[peer], wanted.at[me], index_send, index_recv, peer).start()

                each(1, n, send_index)
                wanted[pl.ds(me, 1)] = order[pl.ds(me, 1)]
            if pending:
                send_sums(*pending.pop())
            pending.append((group, colour))
    send_sums(*pending.pop())

    terms = term_rows.shape[1]
    finish(small_loads[1:])

    def contract(group):
        eye = lax.broadcasted_iota(jnp.int32, (terms, terms), 0) == lax.broadcasted_iota(
            jnp.int32, (terms, terms), 1
        )
        lane = lax.broadcasted_iota(jnp.int32, (terms, 24), 1)
        lane_channel = (4 * (lane >> 3) + (lane & 3)).astype(F32)
        lane_imag = (lane >> 2) & 1
        picks = []
        for which in range(2):
            row = term_rows[which : which + 1, :].astype(F32)
            column = jnp.sum(jnp.where(eye, row, 0.0), axis=1, keepdims=True)
            for part in range(2):
                hit = (lane_channel == column) & (lane_imag == part)
                picks.append(jnp.where(hit, 1.0, 0.0))
        picks = jnp.concatenate(picks).astype(BF16)
        sub = lax.broadcasted_iota(jnp.int32, (24, terms), 0)
        target = 4 * (sub >> 3) + (sub & 3) == term_rows[2:3, :]
        signs = (2 * term_sign[...] - 1).astype(F32)
        place_real = jnp.where(target & (((sub >> 2) & 1) == 0), signs, 0.0).astype(BF16)
        place_imag = jnp.where(target & (((sub >> 2) & 1) == 1), signs, 0.0).astype(BF16)
        weights = table_weights[sink[0, 0]]
        weight_real, weight_imag = weights[0:1, :], weights[1:2, :]

        totals = []
        for colour in range(3):
            own = blocks[colour, pl.ds(group.mine, 1), pl.ds(core, 1)][0, 0]
            own = own + from_core[colour, pl.ds(group.mine, 1)][0]
            landed(from_chips.at[colour, pl.ds(0, chips - 1)], chip_recv.at[colour])

            def turned(part, source_chip):
                kept = []
                for i in range(len(fixed)):
                    kept.append(turn[2 * i, pl.ds(source_chip, 1)][0] * part[0])
                    kept.append(turn[2 * i + 1, pl.ds(source_chip, 1)][0] * part[0])
                return kept

            def add_sum(t, carry, colour=colour):
                other = lax.rem(chip + chips - t, chips)
                part = from_chips[colour, pl.ds(other, 1)][0].astype(F32)
                return tuple(a + b for a, b in zip(carry, (part, *turned(part, other))))

            total, *kept = lax.fori_loop(1, chips, add_sum, (own, *turned(own, chip)))
            extra = [
                kept[2 * i] - swap_halves(kept[2 * i + 1]) for i in range(len(fixed))
            ]
            totals.append([total[slot] for slot in range(slots)] + extra)

        count = slots + len(fixed)
        block = jnp.concatenate([
            jnp.concatenate([total[unit] for total in totals]) for unit in range(count)
        ], axis=1)
        picked = dot_exact(picks, block)
        first_real, first_imag = picked[:terms], picked[terms : 2 * terms]
        other_real, other_imag = picked[2 * terms : 3 * terms], picked[3 * terms :]
        real_products, imag_products = [], []
        for unit in range(count):
            lanes = slice(unit * nvec, (unit + 1) * nvec)
            o_real, o_imag = other_real[:, lanes], other_imag[:, lanes]
            f_real, f_imag = first_real[:, lanes], first_imag[:, lanes]
            second_real = jnp.sum(
                weight_real * o_real - weight_imag * o_imag, axis=1, keepdims=True
            )
            second_imag = jnp.sum(
                weight_real * o_imag + weight_imag * o_real, axis=1, keepdims=True
            )
            real_products.append(f_real * second_real - f_imag * second_imag)
            imag_products.append(f_real * second_imag + f_imag * second_real)
        made = dot_exact(place_real, jnp.concatenate(real_products, axis=1)) + dot_exact(
            place_imag, jnp.concatenate(imag_products, axis=1)
        )
        acc[:24, :] = made[:, :nvec]
        for i in range(len(fixed)):
            acc[24 * (i + 1) : 24 * (i + 2), :] = made[:, (slots + i) * nvec : (slots + i + 1) * nvec]
        rest = made[:, nvec : slots * nvec].reshape(3, 8, (slots - 1) * nvec).astype(BF16)

        def merged(colour, other):
            value = acc[8 * colour : 8 * colour + 8, :]
            for i in range(len(fixed)):
                side_value = acc[24 * (i + 1) + 8 * colour : 24 * (i + 1) + 8 * colour + 8, :]
                value = value + turn[2 * i, pl.ds(other, 1)][0] * side_value
                value = value + turn[2 * i + 1, pl.ds(other, 1)][0] * swap_halves(side_value)
            return value.astype(BF16)

        for colour in range(3):
            others = [rest[colour, :, slot * nvec : (slot + 1) * nvec] for slot in range(slots - 1)]

            def send_coeffs(other, colour=colour, others=others):
                ready[colour, pl.ds(other, 1), 0] = merged(colour, other)[None]
                for slot in range(slots - 1):
                    ready[colour, pl.ds(other, 1), slot + 1] = others[slot][None]
                remote(
                    ready.at[colour, other], coeffs.at[colour, core, group.mine], all_send,
                    all_recv.at[group.index, colour], other * 2 + core,
                ).start()

            far_chips(send_coeffs)
            near_chips(send_coeffs)
            coeffs[colour, pl.ds(core, 1), pl.ds(group.mine, 1), 0] = merged(colour, chip)[None, None]
            for slot in range(slots - 1):
                coeffs[colour, pl.ds(core, 1), pl.ds(group.mine, 1), slot + 1] = others[slot][None, None]

    def build(peer_chip):
        position = lax.broadcasted_iota(jnp.int32, (length, piece), 0)
        for which in range(2):
            local = wanted[pl.ds(peer_chip * 2 + which, 1)][0] - me * length
            onehot[pl.ds(peer_chip, 1), :, which * piece : (which + 1) * piece] = jnp.where(
                position == local, 1.0, 0.0
            ).astype(BF16)[None]

    def build_all():
        landed(wanted.at[pl.ds(0, n - 1)], index_recv)
        each(0, chips, build)

    for i, group in enumerate(plan):
        if i == 0 and len(plan) == 1:
            build_all()
        pl.when(group.owns)(functools.partial(contract, group))
        if i == 0 and len(plan) > 1:
            build_all()

    def relay(group, colour):
        def take(count):
            landed(coeffs.at[colour, core, pl.ds(0, count)], all_recv.at[group.index, colour])

        pl.when(group.owns)(lambda: take(group.owners - 1))
        pl.when(jnp.logical_not(group.owns))(lambda: take(group.owners))
        owners = pl.ds(group.first, group.owners)
        remote(
            coeffs.at[colour, core, owners], coeffs.at[colour, core, owners], fwd_send,
            fwd_recv.at[group.index, colour], partner,
        ).start()

    def rebuild(group, colour, place):
        owners = pl.ds(group.first, group.owners)
        landed(coeffs.at[colour, 1 - core, owners], fwd_recv.at[group.index, colour])
        table = coeffs[colour, :, group.first : group.first + group.owners].astype(F32)
        real_rows, imag_rows = [], []
        for slot in range(slots):
            cells = [table[which, o, slot] for o in range(group.owners) for which in range(2)]
            reals = jnp.concatenate([cell[:4] for cell in cells])
            imags = jnp.concatenate([cell[4:] for cell in cells])
            real_rows += [reals, imags]
            imag_rows += [-imags, reals]
        quarter = 4 * group.width
        rows = slots * 2 * quarter
        lhs[0, :rows] = jnp.concatenate(real_rows).astype(BF16)
        lhs[1, :rows] = jnp.concatenate(imag_rows).astype(BF16)

        def step(step):
            sites = pl.ds(pl.multiple_of(step * chunk, chunk), chunk)
            grid = jnp.dot(
                lhs[0, :rows], eig[0, colour, :, sites], preferred_element_type=F32
            ) + jnp.dot(lhs[1, :rows], eig[1, colour, :, sites], preferred_element_type=F32)
            grid = grid.reshape(slots, 2, quarter, chunk)
            real, imag = grid[0, 0], grid[0, 1]
            for slot in range(len(moving)):
                cosine = trig[2 * slot : 2 * slot + 1, sites]
                sine = trig[2 * slot + 1 : 2 * slot + 2, sites]
                real = real + cosine * grid[slot + 1, 0] - sine * grid[slot + 1, 1]
                imag = imag + cosine * grid[slot + 1, 1] + sine * grid[slot + 1, 0]
            base = 2 * quarter * place
            source[base : base + quarter, sites] = (real * scale_out).astype(BF16)
            source[base + quarter : base + 2 * quarter, sites] = (imag * scale_out).astype(BF16)

        each(0, steps, step)

    def distribute(group, colours, last):
        picked = pl.ds(group.left, group.width)
        taken = pl.ds(colours[0], len(colours))
        if direct:
            lanes = pl.ds(pl.multiple_of(me * piece, piece), piece)
            target = out.at[:, taken, picked, :, lanes]
        else:
            target = out.at[me, :, taken, picked]

        def choose(peer_chip):
            chosen = jnp.dot(
                source[: 8 * group.width * len(colours)], onehot[pl.ds(peer_chip, 1)][0],
                preferred_element_type=F32,
            )
            for which in range(2):
                values = chosen[:, which * piece : (which + 1) * piece].reshape(
                    len(colours), 2, group.width, 4, piece
                ).astype(BF16)
                for i, colour in enumerate(colours):
                    staged[
                        pl.ds(peer_chip * 2 + which, 1), :, colour,
                        group.left : group.left + group.width,
                    ] = values[i : i + 1]

        def send_pieces(other):
            choose(other)
            for which in range(2):
                peer = other * 2 + which
                remote(
                    staged.at[peer, :, taken, picked], target, out_send, out_recv, peer
                ).start()

        if last:
            near_chips(send_pieces)
            far_chips(send_pieces)
        else:
            far_chips(send_pieces)
            near_chips(send_pieces)
        choose(chip)
        remote(staged.at[partner, :, taken, picked], target, out_send, out_recv, partner).start()
        pltpu.make_async_copy(staged.at[me, :, taken, picked], target, own_sem).start()

    batches = [(0, (0,)), (0, (1, 2))] + [(index, (0, 1, 2)) for index in range(1, len(plan))]
    batches = [(plan[index], colours) for index, colours in batches]
    work = [(group, colour) for group, colours in batches for colour in colours]
    relay(*work[0])
    for batch, (group, colours) in enumerate(batches):
        for place, colour in enumerate(colours):
            rebuild(group, colour, place)
            done = work.index((group, colour)) + 1
            if done < len(work):
                relay(*work[done])
        distribute(group, colours, batch + 1 == len(batches))

    owns = functools.reduce(jnp.logical_or, [group.owns for group in plan])
    total_owners = 2 * sum(groups)

    def sent_sums(count):
        sent(summed.at[:, pl.ds(0, count)], chip_send)

    sent(from_core, core_send)

    @pl.when(owns)
    def _():
        sent_sums(total_owners - 1)
        sent(ready.at[:, pl.ds(0, chips - 1)], all_send)

    pl.when(jnp.logical_not(owns))(lambda: sent_sums(total_owners))
    sent(coeffs.at[:, 0], fwd_send)
    sent(wanted.at[pl.ds(0, n - 1)], index_send)
    pltpu.make_async_copy(staged.at[0], staged.at[0], own_sem).wait()
    sent(staged.at[pl.ds(0, n - 1)], out_send)
    landed(staged.at[pl.ds(0, n - 1)], out_recv)


def on_device(
    propagator, eigvecs, operator_weights, sink_time, term_index, term_sign, solver_order
):
    columns, length = propagator.shape[3:]
    nvec = eigvecs.shape[2]
    n = lax.axis_size("space")
    chips = n // 2
    piece = length // n
    groups = (columns // 4 - 1, 1)
    fixed = tuple(
        p for p in range(1, NMOM)
        if MOMENTA[p][:2] == (0, 0) and EXTENT * EXTENT % (2 * length) == 0
    )
    moving = tuple(p for p in range(1, NMOM) if p not in fixed)
    assert 4 * sum(groups) == columns and sum(groups) <= chips // 2
    slots = 1 + len(moving)
    owners = 2 * sum(groups)
    rows = slots * columns * 8
    site_rows = columns * 8
    cell = (slots, 8, nvec)
    direct = piece % 128 == 0
    out_shape = (2, 3, columns, 4, length) if direct else (n, 2, 3, columns, 4, piece)
    propagator = propagator.transpose(0, 1, 3, 2, 4)
    smem = pl.BlockSpec(memory_space=pltpu.SMEM)
    hbm = pl.BlockSpec(memory_space=pltpu.HBM)
    dma = pltpu.SemaphoreType.DMA
    gathered = pl.pallas_call(
        functools.partial(
            kernel, n, groups, columns, 1.0 / math.sqrt(3.0 * length * n),
            1.0 / math.sqrt(NMOM * nvec), 512, moving, fixed, direct,
        ),
        out_shape=pltpu.VMEM(out_shape, BF16),
        in_specs=[hbm, hbm, smem, hbm, hbm, hbm, hbm],
        out_specs=pl.BlockSpec(memory_space=pl.ANY),
        scratch_shapes=[
            pltpu.VMEM(propagator.shape, BF16),
            pltpu.VMEM(eigvecs.shape, BF16),
            pltpu.VMEM(operator_weights.shape, F32),
            pltpu.VMEM(term_index.shape[::-1], jnp.int32),
            pltpu.VMEM((1,) + term_sign.shape, jnp.int32),
            pltpu.VMEM((n, 1, piece), jnp.int32),
            pltpu.VMEM((2 * len(moving), length), F32),
            pltpu.VMEM((2 * max(len(fixed), 1), chips, 1, nvec), F32),
            pltpu.VMEM((rows, nvec), F32),
            pltpu.VMEM((3, owners, 2) + cell, F32),
            pltpu.VMEM((3, owners) + cell, F32),
            pltpu.VMEM((3, owners) + cell, BF16),
            pltpu.VMEM((3, chips) + cell, BF16),
            pltpu.VMEM((3, chips) + cell, BF16),
            pltpu.VMEM((3, 2, owners) + cell, BF16),
            pltpu.VMEM((2, rows, nvec), BF16),
            pltpu.VMEM((2 * site_rows, length), BF16),
            pltpu.VMEM((n, 1, piece), jnp.int32),
            pltpu.VMEM((chips, length, 2 * piece), BF16),
            pltpu.VMEM((n, 2, 3, columns, 4, piece), BF16),
            dma((12,)), dma((len(groups), 3)), dma((3,)), dma((len(groups), 3)), dma((len(groups), 3)),
            dma((9,)),
        ],
        compiler_params=pltpu.CompilerParams(
            collective_id=0, has_side_effects=True, vmem_limit_bytes=int(48 * 2**20)
        ),
    )(
        *(
            x if x.size == 1 else pltpu.with_memory_space_constraint(x, pltpu.HBM)
            for x in (
                propagator, eigvecs, sink_time.reshape(1, 1), operator_weights,
                term_index.T, term_sign.reshape(1, -1), solver_order.reshape(n, 1, piece),
            )
        )
    )
    if direct:
        return gathered.transpose(0, 1, 3, 2, 4)
    placed = gathered.transpose(1, 2, 4, 3, 0, 5)
    return placed.reshape(2, 3, 4, columns, length)


def solution(mesh):
    return jax.shard_map(
        on_device,
        mesh=mesh,
        in_specs=(
            P("grp", None, None, None, "space"),
            P("grp", None, None, "space"),
            P("grp", None, None),
            P("grp"),
            P(),
            P(),
            P("space"),
        ),
        out_specs=P("grp", None, None, None, "space"),
        check_vma=False,
    )
```

```python
import functools
import math

import jax
import jax.numpy as jnp
from jax import lax
from jax.experimental import pallas as pl
from jax.experimental.pallas import tpu as pltpu
from jax.sharding import PartitionSpec as P

NMOM = 4
EXTENT = 64
MOMENTA = ((0, 0, 0), (1, 0, 0), (0, 1, 0), (0, 0, 1))
F32 = jnp.float32
BF16 = jnp.bfloat16
MESH = pl.DeviceIdType.MESH


def swap_halves(x):
    top, bottom = x[..., :4, :], x[..., 4:, :]
    return jnp.concatenate([-bottom, top], axis=-2)


def dot_exact(a, b):
    high = b.astype(BF16)
    low = (b - high.astype(F32)).astype(BF16)
    return jnp.dot(a, high, preferred_element_type=F32) + jnp.dot(a, low, preferred_element_type=F32)


def kernel(
    n, groups, columns, scale_in, scale_out, chunk, moving, fixed, direct,
    prop_hbm, eig_hbm, sink, table_hbm, term_rows_hbm, term_sign_hbm, order_hbm, out,
    prop, eig, table_weights, term_rows, term_sign, order, trig, turn, acc, blocks, from_core, summed, from_chips, ready, coeffs,
    lhs, source, wanted, onehot, staged,
    load_sem, core_recv, chip_recv, all_recv, fwd_recv, sems,
):
    me = lax.axis_index("space")
    chips = n // 2
    half = chips // 2
    core = lax.rem(me, 2)
    chip = me // 2
    side = chip // half
    partner = me + 1 - 2 * core
    length = eig.shape[-1]
    nvec = eig.shape[2]
    piece = order.shape[-1]
    steps = length // chunk
    slots = 1 + len(moving)
    core_send, chip_send, all_send, fwd_send, index_send, index_recv, out_send, out_recv, own_sem = (
        sems.at[i] for i in range(9)
    )

    def each(lower, upper, body):
        def step(i, carry):
            body(i)
            return carry

        lax.fori_loop(lower, upper, step, 0)

    def far_chips(body):
        each(0, half, lambda t: body((1 - side) * half + lax.rem(chip + t, half)))

    def near_chips(body):
        each(1, half, lambda t: body(side * half + lax.rem(chip + t, half)))

    def remote(src, dst, send_sem, recv_sem, device):
        return pltpu.make_async_remote_copy(
            src_ref=src, dst_ref=dst, send_sem=send_sem, recv_sem=recv_sem,
            device_id={"space": device}, device_id_type=MESH,
        )

    def sent(ref, sem):
        remote(ref, ref, sem, sem, partner).wait_send()

    def landed(ref, sem):
        remote(ref, ref, sem, sem, partner).wait_recv()

    class Group:
        def __init__(self, index, start, depth):
            self.index, self.start, self.depth = index, start, depth
            self.first = 2 * start
            self.owners = 2 * depth
            self.left, self.width = 4 * start, 4 * depth
            below = chip - (half - start - depth)
            above = chip - (half + start)
            self.owns = ((below >= 0) & (below < depth)) | ((above >= 0) & (above < depth))
            self.mine = self.first + jnp.where(chip < half, below, depth + above)

        def chip_of(self, owner):
            return jnp.where(
                owner < self.depth, half - self.start - self.depth + owner,
                half + self.start + owner - self.depth,
            )

        def each_owner(self, body):
            def step(t):
                owner = lax.rem(t + (1 - side) * self.depth, self.owners)
                other = self.chip_of(owner)

                @pl.when(other != chip)
                def _():
                    body(self.first + owner, other)

            each(0, self.owners, step)

    plan, start = [], 0
    for index, depth in enumerate(groups):
        plan.append(Group(index, start, depth))
        start += depth

    middle = length // 2

    def load(colour, part):
        sites = slice(part * middle, (part + 1) * middle)
        sem = 4 * colour + 2 * part
        return (
            pltpu.make_async_copy(
                prop_hbm.at[:, colour, :, :, sites], prop.at[:, colour, :, :, sites],
                load_sem.at[sem],
            ),
            pltpu.make_async_copy(
                eig_hbm.at[:, colour, :, sites], eig.at[:, colour, :, sites], load_sem.at[sem + 1]
            ),
        )

    def start(copies):
        for copy in copies:
            copy.start()

    def finish(copies):
        for copy in copies:
            copy.wait()

    small_loads = tuple(
        pltpu.make_async_copy(remote_ref, own_ref, load_sem.at[12 + i])
        for i, (remote_ref, own_ref) in enumerate((
            (order_hbm, order), (table_hbm, table_weights), (term_rows_hbm, term_rows),
            (term_sign_hbm, term_sign),
        ))
    )
    start(load(0, 0))
    start(load(0, 1))
    barrier = pltpu.get_barrier_semaphore()
    each(1, n, lambda t: pl.semaphore_signal(
        barrier, inc=1, device_id={"space": lax.rem(me + t, n)}, device_id_type=MESH
    ))

    bits = EXTENT.bit_length() - 1
    low = EXTENT - 1

    def angles(p, site):
        coords = (site & low, (site >> bits) & low, site >> (2 * bits))
        winding = sum(step * coord for step, coord in zip(MOMENTA[p], coords) if step) & low
        return winding.astype(F32) * (2.0 * math.pi / EXTENT)

    tiles = length // 128
    compact = me * length + 128 * lax.broadcasted_iota(
        jnp.int32, (tiles, 128), 0
    ) + lax.broadcasted_iota(jnp.int32, (tiles, 128), 1)
    for slot, p in enumerate(moving):
        angle = angles(p, compact)
        for part, values in enumerate((jnp.cos(angle), jnp.sin(angle))):
            trig[2 * slot + part : 2 * slot + part + 1, :] = jnp.concatenate(
                [values[tile : tile + 1] for tile in range(tiles)], axis=1
            )
    for i, p in enumerate(fixed):
        angle = angles(p, 2 * length * lax.broadcasted_iota(jnp.int32, (chips, nvec), 0))
        turn[2 * i] = jnp.cos(angle)[:, None]
        turn[2 * i + 1] = jnp.sin(angle)[:, None]
    start(small_loads)
    start(load(1, 0))
    start(load(1, 1))

    def core_copy(group, colour):
        owners = pl.ds(group.first, group.owners)
        return remote(
            blocks.at[colour, 1 - core, owners], from_core.at[colour, owners], core_send,
            core_recv.at[group.index, colour], partner,
        )

    def send_sums(group, colour):
        core_copy(group, colour).wait_recv()

        def send(owner, other):
            summed[colour, owner] = (
                blocks[colour, core, owner] + from_core[colour, owner]
            ).astype(BF16)
            remote(
                summed.at[colour, owner], from_chips.at[colour, chip], chip_send,
                chip_recv.at[colour], other * 2 + core,
            ).start()

        group.each_owner(send)

    def project(group, colour, between):
        quarter = slots * 4 * group.width
        wide = -(-quarter // 128) * 128
        picked = slice(group.left, group.left + group.width)
        total = None
        for part in range(2):
            between(part)
            sites = slice(part * middle, (part + 1) * middle)
            real = prop[0, colour, picked, :, sites].astype(F32).reshape(4 * group.width, middle)
            imag = prop[1, colour, picked, :, sites].astype(F32).reshape(4 * group.width, middle)
            reals, imags = [real], [imag]
            for slot in range(len(moving)):
                cosine = trig[2 * slot : 2 * slot + 1, sites]
                sine = trig[2 * slot + 1 : 2 * slot + 2, sites]
                reals.append(cosine * real + sine * imag)
                imags.append(cosine * imag - sine * real)
            spare = [jnp.zeros((wide - quarter, middle), F32)] if wide > quarter else []
            rows = jnp.concatenate(reals + spare + imags + spare).astype(BF16)
            both = jnp.concatenate([eig[0, colour, :, sites], eig[1, colour, :, sites]])
            made = lax.dot_general(
                both, rows, (((1,), (1,)), ((), ())), preferred_element_type=F32
            )
            total = made if total is None else total + made
        with_real, with_imag = total[:nvec] * scale_in, total[nvec:] * scale_in
        real = (with_real[:, :wide] + with_imag[:, wide:]).T[:quarter]
        imag = (with_real[:, wide:] - with_imag[:, :wide]).T[:quarter]
        shape = (slots, 2, group.owners, 4, nvec)
        made = jnp.concatenate([real.reshape(shape), imag.reshape(shape)], axis=3)
        for slot in range(slots):
            blocks[colour, :, group.first : group.first + group.owners, slot] = made[slot]

    def send_index(t):
        peer = lax.rem(me + t, n)
        remote(order.at[peer], wanted.at[me], index_send, index_recv, peer).start()

    for group in plan:
        opening = group.index == 0

        def stage(colour, group=group, opening=opening):
            def between(part):
                if opening:
                    finish(load(colour, part))
                    if part == 0:

                        @pl.when(colour == 0)
                        def _():
                            start(load(2, 0))
                            start(load(2, 1))

            project(group, colour, between)
            if opening:
                pl.when(colour == 0)(lambda: pl.semaphore_wait(barrier, n - 1))
            core_copy(group, colour).start()

            @pl.when(colour == 0)
            def _():
                if opening:
                    finish(small_loads[:1])
                    each(1, n, send_index)
                    wanted[pl.ds(me, 1)] = order[pl.ds(me, 1)]
                else:
                    send_sums(plan[group.index - 1], 2)

            pl.when(colour > 0)(lambda: send_sums(group, colour - 1))

        each(0, 3, stage)
    send_sums(plan[-1], 2)

    terms = term_rows.shape[1]
    finish(small_loads[1:])

    def contract(group):
        eye = lax.broadcasted_iota(jnp.int32, (terms, terms), 0) == lax.broadcasted_iota(
            jnp.int32, (terms, terms), 1
        )
        lane = lax.broadcasted_iota(jnp.int32, (terms, 24), 1)
        lane_channel = (4 * (lane >> 3) + (lane & 3)).astype(F32)
        lane_imag = (lane >> 2) & 1
        picks = []
        for which in range(2):
            row = term_rows[which : which + 1, :].astype(F32)
            column = jnp.sum(jnp.where(eye, row, 0.0), axis=1, keepdims=True)
            for part in range(2):
                hit = (lane_channel == column) & (lane_imag == part)
                picks.append(jnp.where(hit, 1.0, 0.0))
        picks = jnp.concatenate(picks).astype(BF16)
        sub = lax.broadcasted_iota(jnp.int32, (24, terms), 0)
        target = 4 * (sub >> 3) + (sub & 3) == term_rows[2:3, :]
        signs = (2 * term_sign[...] - 1).astype(F32)
        place_real = jnp.where(target & (((sub >> 2) & 1) == 0), signs, 0.0).astype(BF16)
        place_imag = jnp.where(target & (((sub >> 2) & 1) == 1), signs, 0.0).astype(BF16)
        weights = table_weights[sink[0, 0]]
        weight_real, weight_imag = weights[0:1, :], weights[1:2, :]

        totals = []
        for colour in range(3):
            own = blocks[colour, core, group.mine] + from_core[colour, group.mine]
            landed(from_chips.at[colour, pl.ds(0, chips - 1)], chip_recv.at[colour])

            def turned(part, source_chip):
                kept = []
                for i in range(len(fixed)):
                    kept.append(turn[2 * i, pl.ds(source_chip, 1)][0] * part[0])
                    kept.append(turn[2 * i + 1, pl.ds(source_chip, 1)][0] * part[0])
                return kept

            def add_sum(t, carry, colour=colour):
                other = lax.rem(chip + chips - t, chips)
                part = from_chips[colour, pl.ds(other, 1)][0].astype(F32)
                return tuple(a + b for a, b in zip(carry, (part, *turned(part, other))))

            total, *kept = lax.fori_loop(1, chips, add_sum, (own, *turned(own, chip)))
            extra = [
                kept[2 * i] - swap_halves(kept[2 * i + 1]) for i in range(len(fixed))
            ]
            totals.append([total[slot] for slot in range(slots)] + extra)

        count = slots + len(fixed)
        block = jnp.concatenate([
            jnp.concatenate([total[unit] for total in totals]) for unit in range(count)
        ], axis=1)
        picked = dot_exact(picks, block)
        first_real, first_imag = picked[:terms], picked[terms : 2 * terms]
        other_real, other_imag = picked[2 * terms : 3 * terms], picked[3 * terms :]
        real_products, imag_products = [], []
        for unit in range(count):
            lanes = slice(unit * nvec, (unit + 1) * nvec)
            o_real, o_imag = other_real[:, lanes], other_imag[:, lanes]
            f_real, f_imag = first_real[:, lanes], first_imag[:, lanes]
            second_real = jnp.sum(
                weight_real * o_real - weight_imag * o_imag, axis=1, keepdims=True
            )
            second_imag = jnp.sum(
                weight_real * o_imag + weight_imag * o_real, axis=1, keepdims=True
            )
            real_products.append(f_real * second_real - f_imag * second_imag)
            imag_products.append(f_real * second_imag + f_imag * second_real)
        made = dot_exact(place_real, jnp.concatenate(real_products, axis=1)) + dot_exact(
            place_imag, jnp.concatenate(imag_products, axis=1)
        )
        acc[:24, :] = made[:, :nvec]
        for i in range(len(fixed)):
            acc[24 * (i + 1) : 24 * (i + 2), :] = made[:, (slots + i) * nvec : (slots + i + 1) * nvec]
        rest = made[:, nvec : slots * nvec].reshape(3, 8, (slots - 1) * nvec).astype(BF16)

        def merged(colour, other):
            value = acc[8 * colour : 8 * colour + 8, :]
            for i in range(len(fixed)):
                side_value = acc[24 * (i + 1) + 8 * colour : 24 * (i + 1) + 8 * colour + 8, :]
                value = value + turn[2 * i, pl.ds(other, 1)][0] * side_value
                value = value + turn[2 * i + 1, pl.ds(other, 1)][0] * swap_halves(side_value)
            return value.astype(BF16)

        for colour in range(3):
            others = [rest[colour, :, slot * nvec : (slot + 1) * nvec] for slot in range(slots - 1)]

            def send_coeffs(other, colour=colour, others=others):
                ready[colour, pl.ds(other, 1), 0] = merged(colour, other)[None]
                for slot in range(slots - 1):
                    ready[colour, pl.ds(other, 1), slot + 1] = others[slot][None]
                remote(
                    ready.at[colour, other], coeffs.at[colour, core, group.mine], all_send,
                    all_recv.at[group.index, colour], other * 2 + core,
                ).start()

            far_chips(send_coeffs)
            near_chips(send_coeffs)
            coeffs[colour, pl.ds(core, 1), pl.ds(group.mine, 1), 0] = merged(colour, chip)[None, None]
            for slot in range(slots - 1):
                coeffs[colour, pl.ds(core, 1), pl.ds(group.mine, 1), slot + 1] = others[slot][None, None]

    def build(peer_chip):
        position = lax.broadcasted_iota(jnp.int32, (length, piece), 0)
        for which in range(2):
            local = wanted[pl.ds(peer_chip * 2 + which, 1)][0] - me * length
            onehot[pl.ds(peer_chip, 1), :, which * piece : (which + 1) * piece] = jnp.where(
                position == local, 1.0, 0.0
            ).astype(BF16)[None]

    def build_all():
        landed(wanted.at[pl.ds(0, n - 1)], index_recv)
        each(0, chips, build)

    for i, group in enumerate(plan):
        if i == 0 and len(plan) == 1:
            build_all()
        pl.when(group.owns)(functools.partial(contract, group))
        if i == 0 and len(plan) > 1:
            build_all()

    def relay(group, colour):
        def take(count):
            landed(coeffs.at[colour, core, pl.ds(0, count)], all_recv.at[group.index, colour])

        pl.when(group.owns)(lambda: take(group.owners - 1))
        pl.when(jnp.logical_not(group.owns))(lambda: take(group.owners))
        owners = pl.ds(group.first, group.owners)
        remote(
            coeffs.at[colour, core, owners], coeffs.at[colour, core, owners], fwd_send,
            fwd_recv.at[group.index, colour], partner,
        ).start()

    def rebuild(group, colour, place):
        landed(
            coeffs.at[colour, 1 - core, pl.ds(group.first, group.owners)],
            fwd_recv.at[group.index, colour],
        )
        height = group.width * slots * 8
        lhs[:height] = coeffs[colour, :, group.first : group.first + group.owners].reshape(
            height, nvec
        )
        base = pl.multiple_of(place * 8 * group.width, 8 * group.width)

        def step(step):
            sites = pl.ds(pl.multiple_of(step * chunk, chunk), chunk)
            x, y = (
                jnp.dot(
                    lhs[:height], eig[part, colour, :, sites], preferred_element_type=F32
                ).reshape(group.width, slots, 8, chunk)
                for part in range(2)
            )
            straight, crossed = x[:, 0], y[:, 0]
            for slot in range(len(moving)):
                cosine = trig[2 * slot : 2 * slot + 1, sites][None]
                sine = trig[2 * slot + 1 : 2 * slot + 2, sites][None]
                straight = straight + cosine * x[:, slot + 1] - sine * y[:, slot + 1]
                crossed = crossed + cosine * y[:, slot + 1] + sine * x[:, slot + 1]
            made = (straight + swap_halves(crossed)) * scale_out
            source[pl.ds(base, 8 * group.width), sites] = made.reshape(
                8 * group.width, chunk
            ).astype(BF16)

        each(0, steps, step)

    def distribute(group, colours, last):
        picked = pl.ds(group.left, group.width)
        taken = pl.ds(colours[0], len(colours))
        height = 8 * group.width * len(colours)
        if direct:
            lanes = pl.ds(pl.multiple_of(me * piece, piece), piece)
            target = out.at[:, taken, picked, :, lanes]
        else:
            target = out.at[me, :, taken, picked]

        def send_pieces(t):
            if last:
                near = (t < half - 1) | (t == chips - 1)
                step = jnp.where(t == chips - 1, 0, t + 1)
            else:
                near, step = t >= half, t + 1
            other = jnp.where(near, side, 1 - side) * half + lax.rem(chip + step, half)
            chosen = jnp.dot(source[:height], onehot[other], preferred_element_type=F32)
            chosen = chosen.reshape(len(colours), group.width, 8, 2 * piece)
            for which in range(2):
                values = chosen[..., which * piece : (which + 1) * piece]
                for i, colour in enumerate(colours):
                    for part in range(2):
                        staged[
                            2 * other + which, part, colour, group.left : group.left + group.width
                        ] = values[i, :, 4 * part : 4 * part + 4].astype(BF16)

            def send(peer):
                remote(
                    staged.at[peer, :, taken, picked], target, out_send, out_recv, peer
                ).start()

            @pl.when(other != chip)
            def _():
                send(2 * other)
                send(2 * other + 1)

            @pl.when(other == chip)
            def _():
                send(partner)
                pltpu.make_async_copy(staged.at[me, :, taken, picked], target, own_sem).start()

        each(0, chips, send_pieces)

    batches = [(plan[0], (0,)), (plan[0], (1, 2))] + [(group, (0, 1, 2)) for group in plan[1:]]
    relay(plan[0], 0)
    for i, (group, colours) in enumerate(batches):
        each(colours[0], colours[-1] + 1, lambda colour: rebuild(group, colour, colour - colours[0]))
        if i + 1 < len(batches):
            following, later = batches[i + 1]
            each(later[0], later[-1] + 1, lambda colour: relay(following, colour))
        distribute(group, colours, i + 1 == len(batches))

    owns = functools.reduce(jnp.logical_or, [group.owns for group in plan])
    total_owners = 2 * sum(groups)

    def sent_sums(count):
        sent(summed.at[:, pl.ds(0, count)], chip_send)

    sent(from_core, core_send)

    @pl.when(owns)
    def _():
        sent_sums(total_owners - 1)
        sent(ready.at[:, pl.ds(0, chips - 1)], all_send)

    pl.when(jnp.logical_not(owns))(lambda: sent_sums(total_owners))
    sent(coeffs.at[:, 0], fwd_send)
    sent(wanted.at[pl.ds(0, n - 1)], index_send)
    pltpu.make_async_copy(staged.at[0], staged.at[0], own_sem).wait()
    sent(staged.at[pl.ds(0, n - 1)], out_send)
    landed(staged.at[pl.ds(0, n - 1)], out_recv)


def on_device(
    propagator, eigvecs, operator_weights, sink_time, term_index, term_sign, solver_order
):
    columns, length = propagator.shape[3:]
    nvec = eigvecs.shape[2]
    n = lax.axis_size("space")
    chips = n // 2
    piece = length // n
    groups = (2,) * (columns // 8) + (1,) * (columns % 8 // 4)
    fixed = tuple(
        p for p in range(1, NMOM)
        if MOMENTA[p][:2] == (0, 0) and EXTENT * EXTENT % (2 * length) == 0
    )
    moving = tuple(p for p in range(1, NMOM) if p not in fixed)
    assert 4 * sum(groups) == columns and sum(groups) <= chips // 2
    slots = 1 + len(moving)
    owners = 2 * sum(groups)
    rows = slots * columns * 8
    site_rows = columns * 8
    cell = (slots, 8, nvec)
    direct = piece % 128 == 0
    out_shape = (2, 3, columns, 4, length) if direct else (n, 2, 3, columns, 4, piece)
    propagator = propagator.transpose(0, 1, 3, 2, 4)
    smem = pl.BlockSpec(memory_space=pltpu.SMEM)
    hbm = pl.BlockSpec(memory_space=pltpu.HBM)
    dma = pltpu.SemaphoreType.DMA
    gathered = pl.pallas_call(
        functools.partial(
            kernel, n, groups, columns, 1.0 / math.sqrt(3.0 * length * n),
            1.0 / math.sqrt(NMOM * nvec), 512, moving, fixed, direct,
        ),
        out_shape=pltpu.VMEM(out_shape, BF16),
        in_specs=[hbm, hbm, smem, hbm, hbm, hbm, hbm],
        out_specs=pl.BlockSpec(memory_space=pl.ANY),
        scratch_shapes=[
            pltpu.VMEM(propagator.shape, BF16),
            pltpu.VMEM(eigvecs.shape, BF16),
            pltpu.VMEM(operator_weights.shape, F32),
            pltpu.VMEM(term_index.shape[::-1], jnp.int32),
            pltpu.VMEM((1,) + term_sign.shape, jnp.int32),
            pltpu.VMEM((n, 1, piece), jnp.int32),
            pltpu.VMEM((2 * len(moving), length), F32),
            pltpu.VMEM((2 * max(len(fixed), 1), chips, 1, nvec), F32),
            pltpu.VMEM((24 * (1 + len(fixed)), nvec), F32),
            pltpu.VMEM((3, 2, owners) + cell, F32),
            pltpu.VMEM((3, owners) + cell, F32),
            pltpu.VMEM((3, owners) + cell, BF16),
            pltpu.VMEM((3, chips) + cell, BF16),
            pltpu.VMEM((3, chips) + cell, BF16),
            pltpu.VMEM((3, 2, owners) + cell, BF16),
            pltpu.VMEM((rows, nvec), BF16),
            pltpu.VMEM((2 * site_rows, length), BF16),
            pltpu.VMEM((n, 1, piece), jnp.int32),
            pltpu.VMEM((chips, length, 2 * piece), BF16),
            pltpu.VMEM((n, 2, 3, columns, 4, piece), BF16),
            dma((16,)), dma((len(groups), 3)), dma((3,)), dma((len(groups), 3)), dma((len(groups), 3)),
            dma((9,)),
        ],
        compiler_params=pltpu.CompilerParams(
            collective_id=0, has_side_effects=True, vmem_limit_bytes=int(48 * 2**20)
        ),
    )(
        *(
            x if x.size == 1 else pltpu.with_memory_space_constraint(x, pltpu.HBM)
            for x in (
                propagator, eigvecs, sink_time.reshape(1, 1), operator_weights,
                term_index.T, term_sign.reshape(1, -1), solver_order.reshape(n, 1, piece),
            )
        )
    )
    if direct:
        return gathered.transpose(0, 1, 3, 2, 4)
    placed = gathered.transpose(1, 2, 4, 3, 0, 5)
    return placed.reshape(2, 3, 4, columns, length)


def solution(mesh):
    return jax.shard_map(
        on_device,
        mesh=mesh,
        in_specs=(
            P("grp", None, None, None, "space"),
            P("grp", None, None, "space"),
            P("grp", None, None),
            P("grp"),
            P(),
            P(),
            P("space"),
        ),
        out_specs=P("grp", None, None, None, "space"),
        check_vma=False,
    )
```

```python
import functools
import math

import jax
import jax.numpy as jnp
from jax import lax
from jax.experimental import pallas as pl
from jax.experimental.pallas import tpu as pltpu
from jax.sharding import PartitionSpec as P

NMOM = 4
EXTENT = 64
MOMENTA = ((0, 0, 0), (1, 0, 0), (0, 1, 0), (0, 0, 1))
F32 = jnp.float32
BF16 = jnp.bfloat16
MESH = pl.DeviceIdType.MESH


def swap_halves(x):
    top, bottom = x[..., :4, :], x[..., 4:, :]
    return jnp.concatenate([-bottom, top], axis=-2)


def dot_exact(a, b):
    high = b.astype(BF16)
    low = (b - high.astype(F32)).astype(BF16)
    return jnp.dot(a, high, preferred_element_type=F32) + jnp.dot(a, low, preferred_element_type=F32)


def kernel(
    n, groups, columns, scale_in, scale_out, chunk, moving, fixed, direct,
    prop_hbm, eig_hbm, sink, table_hbm, term_rows_hbm, term_sign_hbm, order_hbm, out,
    prop, eig, table_weights, term_rows, term_sign, order, trig, turn, acc, blocks, from_core, summed, from_chips, ready, coeffs, rest,
    lhs, source, wanted, onehot, staged,
    load_sem, core_recv, chip_recv, all_recv, fwd_recv, mate_recv, sems,
):
    me = lax.axis_index("space")
    chips = n // 2
    half = chips // 2
    core = lax.rem(me, 2)
    chip = me // 2
    side = chip // half
    partner = me + 1 - 2 * core
    length = eig.shape[-1]
    nvec = eig.shape[2]
    piece = order.shape[-1]
    steps = length // chunk
    slots = 1 + len(moving)
    (
        core_send, chip_send, all_send, fwd_send, pass_send, partner_send, index_send, index_recv,
        out_send, out_recv, own_sem,
    ) = (sems.at[i] for i in range(11))

    def each(lower, upper, body):
        def step(i, carry):
            body(i)
            return carry

        lax.fori_loop(lower, upper, step, 0)

    def far_chips(body):
        each(0, half, lambda t: body((1 - side) * half + lax.rem(chip + t, half)))

    def near_chips(body):
        each(1, half, lambda t: body(side * half + lax.rem(chip + t, half)))

    def remote(src, dst, send_sem, recv_sem, device):
        return pltpu.make_async_remote_copy(
            src_ref=src, dst_ref=dst, send_sem=send_sem, recv_sem=recv_sem,
            device_id={"space": device}, device_id_type=MESH,
        )

    def sent(ref, sem):
        remote(ref, ref, sem, sem, partner).wait_send()

    def landed(ref, sem):
        remote(ref, ref, sem, sem, partner).wait_recv()

    class Group:
        def __init__(self, index, start, depth):
            self.index, self.start, self.depth = index, start, depth
            self.first = 2 * start
            self.owners = 2 * depth
            self.left, self.width = 4 * start, 4 * depth
            below = chip - (half - start - depth)
            above = chip - (half + start)
            self.owns = ((below >= 0) & (below < depth)) | ((above >= 0) & (above < depth))
            self.mine = self.first + jnp.where(chip < half, below, depth + above)
            place = self.mine - self.first
            self.seat = core * self.owners + place
            self.mate_chip = jnp.where(place < depth, half + place, half - 2 * depth + place)
            self.passes = (chip >= half - depth) & (chip < half + depth)
            mate = jnp.where(chip < half, chip - half + 2 * depth, chip - half)
            self.mate_seat = core * self.owners + mate

        def chip_of(self, owner):
            return jnp.where(
                owner < self.depth, half - self.start - self.depth + owner,
                half + self.start + owner - self.depth,
            )

        def each_owner(self, body):
            def step(t):
                owner = lax.rem(t + (1 - side) * self.depth, self.owners)
                other = self.chip_of(owner)

                @pl.when(other != chip)
                def _():
                    body(self.first + owner, other)

            each(0, self.owners, step)

    plan, start = [], 0
    for index, depth in enumerate(groups):
        plan.append(Group(index, start, depth))
        start += depth

    middle = length // 2

    def load(colour, part):
        sites = slice(part * middle, (part + 1) * middle)
        sem = 4 * colour + 2 * part
        return (
            pltpu.make_async_copy(
                prop_hbm.at[:, colour, :, :, sites], prop.at[:, colour, :, :, sites],
                load_sem.at[sem],
            ),
            pltpu.make_async_copy(
                eig_hbm.at[:, colour, :, sites], eig.at[:, colour, :, sites], load_sem.at[sem + 1]
            ),
        )

    def start(copies):
        for copy in copies:
            copy.start()

    def finish(copies):
        for copy in copies:
            copy.wait()

    small_loads = tuple(
        pltpu.make_async_copy(remote_ref, own_ref, load_sem.at[12 + i])
        for i, (remote_ref, own_ref) in enumerate((
            (order_hbm, order), (table_hbm, table_weights), (term_rows_hbm, term_rows),
            (term_sign_hbm, term_sign),
        ))
    )
    start(load(0, 0))
    start(load(0, 1))
    barrier = pltpu.get_barrier_semaphore()
    each(1, n, lambda t: pl.semaphore_signal(
        barrier, inc=1, device_id={"space": lax.rem(me + t, n)}, device_id_type=MESH
    ))

    bits = EXTENT.bit_length() - 1
    low = EXTENT - 1

    def angles(p, site):
        coords = (site & low, (site >> bits) & low, site >> (2 * bits))
        winding = sum(step * coord for step, coord in zip(MOMENTA[p], coords) if step) & low
        return winding.astype(F32) * (2.0 * math.pi / EXTENT)

    tiles = length // 128
    compact = me * length + 128 * lax.broadcasted_iota(
        jnp.int32, (tiles, 128), 0
    ) + lax.broadcasted_iota(jnp.int32, (tiles, 128), 1)
    for slot, p in enumerate(moving):
        angle = angles(p, compact)
        for part, values in enumerate((jnp.cos(angle), jnp.sin(angle))):
            trig[2 * slot + part : 2 * slot + part + 1, :] = jnp.concatenate(
                [values[tile : tile + 1] for tile in range(tiles)], axis=1
            )
    for i, p in enumerate(fixed):
        angle = angles(p, 2 * length * lax.broadcasted_iota(jnp.int32, (chips, nvec), 0))
        turn[2 * i] = jnp.cos(angle)[:, None]
        turn[2 * i + 1] = jnp.sin(angle)[:, None]
    start(small_loads)
    start(load(1, 0))
    start(load(1, 1))

    def core_copy(group, colour):
        owners = pl.ds(group.first, group.owners)
        return remote(
            blocks.at[colour, 1 - core, owners], from_core.at[colour, owners], core_send,
            core_recv.at[group.index, colour], partner,
        )

    def send_sums(group, colour):
        core_copy(group, colour).wait_recv()

        def send(owner, other):
            summed[colour, owner] = (
                blocks[colour, core, owner] + from_core[colour, owner]
            ).astype(BF16)
            remote(
                summed.at[colour, owner], from_chips.at[colour, chip], chip_send,
                chip_recv.at[colour], other * 2 + core,
            ).start()

        group.each_owner(send)

    def project(group, colour, between):
        quarter = slots * 4 * group.width
        wide = -(-quarter // 128) * 128
        picked = slice(group.left, group.left + group.width)
        total = None
        for part in range(2):
            between(part)
            sites = slice(part * middle, (part + 1) * middle)
            real = prop[0, colour, picked, :, sites].astype(F32).reshape(4 * group.width, middle)
            imag = prop[1, colour, picked, :, sites].astype(F32).reshape(4 * group.width, middle)
            reals, imags = [real], [imag]
            for slot in range(len(moving)):
                cosine = trig[2 * slot : 2 * slot + 1, sites]
                sine = trig[2 * slot + 1 : 2 * slot + 2, sites]
                reals.append(cosine * real + sine * imag)
                imags.append(cosine * imag - sine * real)
            spare = [jnp.zeros((wide - quarter, middle), F32)] if wide > quarter else []
            rows = jnp.concatenate(reals + spare + imags + spare).astype(BF16)
            both = jnp.concatenate([eig[0, colour, :, sites], eig[1, colour, :, sites]])
            made = lax.dot_general(
                both, rows, (((1,), (1,)), ((), ())), preferred_element_type=F32
            )
            total = made if total is None else total + made
        with_real, with_imag = total[:nvec] * scale_in, total[nvec:] * scale_in
        real = (with_real[:, :wide] + with_imag[:, wide:]).T[:quarter]
        imag = (with_real[:, wide:] - with_imag[:, :wide]).T[:quarter]
        shape = (slots, 2, group.owners, 4, nvec)
        made = jnp.concatenate([real.reshape(shape), imag.reshape(shape)], axis=3)
        for slot in range(slots):
            blocks[colour, :, group.first : group.first + group.owners, slot] = made[slot]

    def send_index(t):
        peer = lax.rem(me + t, n)
        remote(order.at[peer], wanted.at[me], index_send, index_recv, peer).start()

    for group in plan:
        opening = group.index == 0

        def stage(colour, group=group, opening=opening):
            def between(part):
                if opening:
                    finish(load(colour, part))
                    if part == 0:

                        @pl.when(colour == 0)
                        def _():
                            start(load(2, 0))
                            start(load(2, 1))

            project(group, colour, between)
            if opening:
                pl.when(colour == 0)(lambda: pl.semaphore_wait(barrier, n - 1))
            core_copy(group, colour).start()

            @pl.when(colour == 0)
            def _():
                if opening:
                    finish(small_loads[:1])
                    each(1, n, send_index)
                    wanted[pl.ds(me, 1)] = order[pl.ds(me, 1)]
                else:
                    send_sums(plan[group.index - 1], 2)

            pl.when(colour > 0)(lambda: send_sums(group, colour - 1))

        each(0, 3, stage)
    send_sums(plan[-1], 2)

    terms = term_rows.shape[1]
    finish(small_loads[1:])

    def spread(cell, arrived, sem, last_sem):
        def send(other):
            for which in range(2):
                remote(cell, cell, sem, arrived, other * 2 + which).start()

        near_chips(send)
        remote(cell, cell, last_sem, arrived, partner).start()

    def pass_on(group):
        def step(colour):
            cell = rest.at[colour, group.mate_seat]
            landed(cell, mate_recv.at[colour])
            spread(cell, all_recv.at[group.index, colour], pass_send, partner_send)

        each(0, 3, step)

    def contract(group):
        eye = lax.broadcasted_iota(jnp.int32, (terms, terms), 0) == lax.broadcasted_iota(
            jnp.int32, (terms, terms), 1
        )
        lane = lax.broadcasted_iota(jnp.int32, (terms, 24), 1)
        lane_channel = (4 * (lane >> 3) + (lane & 3)).astype(F32)
        lane_imag = (lane >> 2) & 1
        picks = []
        for which in range(2):
            row = term_rows[which : which + 1, :].astype(F32)
            column = jnp.sum(jnp.where(eye, row, 0.0), axis=1, keepdims=True)
            for part in range(2):
                hit = (lane_channel == column) & (lane_imag == part)
                picks.append(jnp.where(hit, 1.0, 0.0))
        picks = jnp.concatenate(picks).astype(BF16)
        sub = lax.broadcasted_iota(jnp.int32, (24, terms), 0)
        target = 4 * (sub >> 3) + (sub & 3) == term_rows[2:3, :]
        signs = (2 * term_sign[...] - 1).astype(F32)
        place_real = jnp.where(target & (((sub >> 2) & 1) == 0), signs, 0.0).astype(BF16)
        place_imag = jnp.where(target & (((sub >> 2) & 1) == 1), signs, 0.0).astype(BF16)
        weights = table_weights[sink[0, 0]]
        weight_real, weight_imag = weights[0:1, :], weights[1:2, :]

        totals = []
        for colour in range(3):
            own = blocks[colour, core, group.mine] + from_core[colour, group.mine]
            landed(from_chips.at[colour, pl.ds(0, chips - 1)], chip_recv.at[colour])

            def turned(part, source_chip):
                kept = []
                for i in range(len(fixed)):
                    kept.append(turn[2 * i, pl.ds(source_chip, 1)][0] * part[0])
                    kept.append(turn[2 * i + 1, pl.ds(source_chip, 1)][0] * part[0])
                return kept

            def add_sum(t, carry, colour=colour):
                other = lax.rem(chip + chips - t, chips)
                part = from_chips[colour, pl.ds(other, 1)][0].astype(F32)
                return tuple(a + b for a, b in zip(carry, (part, *turned(part, other))))

            total, *kept = lax.fori_loop(1, chips, add_sum, (own, *turned(own, chip)))
            extra = [
                kept[2 * i] - swap_halves(kept[2 * i + 1]) for i in range(len(fixed))
            ]
            totals.append([total[slot] for slot in range(slots)] + extra)

        count = slots + len(fixed)
        block = jnp.concatenate([
            jnp.concatenate([total[unit] for total in totals]) for unit in range(count)
        ], axis=1)
        picked = dot_exact(picks, block)
        first_real, first_imag = picked[:terms], picked[terms : 2 * terms]
        other_real, other_imag = picked[2 * terms : 3 * terms], picked[3 * terms :]
        real_products, imag_products = [], []
        for unit in range(count):
            lanes = slice(unit * nvec, (unit + 1) * nvec)
            o_real, o_imag = other_real[:, lanes], other_imag[:, lanes]
            f_real, f_imag = first_real[:, lanes], first_imag[:, lanes]
            second_real = jnp.sum(
                weight_real * o_real - weight_imag * o_imag, axis=1, keepdims=True
            )
            second_imag = jnp.sum(
                weight_real * o_imag + weight_imag * o_real, axis=1, keepdims=True
            )
            real_products.append(f_real * second_real - f_imag * second_imag)
            imag_products.append(f_real * second_imag + f_imag * second_real)
        made = dot_exact(place_real, jnp.concatenate(real_products, axis=1)) + dot_exact(
            place_imag, jnp.concatenate(imag_products, axis=1)
        )
        if group.index > 0:
            for unit in range(count):
                part = made[:, unit * nvec : (unit + 1) * nvec].reshape(3, 8, nvec).astype(BF16)
                for colour in range(3):
                    rest[colour, group.seat, unit] = part[colour]

            def send_rest(colour):
                cell = rest.at[colour, group.seat]
                remote(
                    cell, cell, all_send, mate_recv.at[colour], group.mate_chip * 2 + core
                ).start()
                spread(cell, all_recv.at[group.index, colour], all_send, all_send)

            each(0, 3, send_rest)
            return
        acc[:24, :] = made[:, :nvec]
        for i in range(len(fixed)):
            acc[24 * (i + 1) : 24 * (i + 2), :] = made[:, (slots + i) * nvec : (slots + i + 1) * nvec]
        plain = made[:, nvec : slots * nvec].reshape(3, 8, (slots - 1) * nvec).astype(BF16)

        def merged(colour, other):
            value = acc[8 * colour : 8 * colour + 8, :]
            for i in range(len(fixed)):
                side_value = acc[24 * (i + 1) + 8 * colour : 24 * (i + 1) + 8 * colour + 8, :]
                value = value + turn[2 * i, other] * side_value
                value = value + turn[2 * i + 1, other] * swap_halves(side_value)
            return value.astype(BF16)

        for colour in range(3):
            others = [plain[colour, :, slot * nvec : (slot + 1) * nvec] for slot in range(slots - 1)]
            target = coeffs.at[colour, core, group.mine]
            coeffs[colour, core, group.mine, 0] = merged(colour, chip)
            for slot in range(slots - 1):
                coeffs[colour, core, group.mine, slot + 1] = others[slot]

            def send_coeffs(other, colour=colour, others=others, target=target):
                ready[colour, other, 0] = merged(colour, other)
                for slot in range(slots - 1):
                    ready[colour, other, slot + 1] = others[slot]
                remote(
                    ready.at[colour, other], target, all_send, all_recv.at[group.index, colour],
                    other * 2 + core,
                ).start()

            far_chips(send_coeffs)
            near_chips(send_coeffs)

    def build(peer_chip):
        position = lax.broadcasted_iota(jnp.int32, (length, piece), 0)
        for which in range(2):
            local = wanted[pl.ds(peer_chip * 2 + which, 1)][0] - me * length
            onehot[pl.ds(peer_chip, 1), :, which * piece : (which + 1) * piece] = jnp.where(
                position == local, 1.0, 0.0
            ).astype(BF16)[None]

    def build_all():
        landed(wanted.at[pl.ds(0, n - 1)], index_recv)
        each(0, chips, build)

    for i, group in enumerate(plan):
        if i == 0 and len(plan) == 1:
            build_all()
        pl.when(group.owns)(functools.partial(contract, group))
        if i == 0 and len(plan) > 1:
            build_all()

    def relay(colour):
        group = plan[0]

        def take(count):
            landed(coeffs.at[colour, core, pl.ds(0, count)], all_recv.at[0, colour])

        pl.when(group.owns)(lambda: take(group.owners - 1))
        pl.when(jnp.logical_not(group.owns))(lambda: take(group.owners))
        cells = coeffs.at[colour, core]
        remote(cells, cells, fwd_send, fwd_recv.at[colour], partner).start()

    def rebuild(group, colour):
        height = group.width * slots * 8
        if group.index == 0:
            landed(coeffs.at[colour, 1 - core], fwd_recv.at[colour])
            lhs[: group.width] = coeffs[colour].reshape(group.width, slots, 8, nvec)
        else:
            for passes in range(2):
                for owns in range(2):

                    @pl.when((group.passes == (passes == 1)) & (group.owns == (owns == 1)))
                    def _(count=2 * group.owners - passes - owns):
                        landed(
                            rest.at[colour, pl.ds(0, count)], all_recv.at[group.index, colour]
                        )

            table = rest[colour].reshape(group.width, slots + len(fixed), 8, nvec)
            still = table[:, 0].astype(F32)
            for i in range(len(fixed)):
                turned = table[:, slots + i].astype(F32)
                still = still + turn[2 * i, chip] * turned
                still = still + turn[2 * i + 1, chip] * swap_halves(turned)
            lhs[: group.width, 0] = still.astype(BF16)
            lhs[: group.width, 1:] = table[:, 1:slots]
        base = pl.multiple_of(colour * 8 * group.width, 8 * group.width)

        def step(step):
            sites = pl.ds(pl.multiple_of(step * chunk, chunk), chunk)
            x, y = (
                jnp.dot(
                    lhs[: group.width].reshape(height, nvec), eig[part, colour, :, sites],
                    preferred_element_type=F32,
                ).reshape(group.width, slots, 8, chunk)
                for part in range(2)
            )
            straight, crossed = x[:, 0], y[:, 0]
            for slot in range(len(moving)):
                cosine = trig[2 * slot : 2 * slot + 1, sites][None]
                sine = trig[2 * slot + 1 : 2 * slot + 2, sites][None]
                straight = straight + cosine * x[:, slot + 1] - sine * y[:, slot + 1]
                crossed = crossed + cosine * y[:, slot + 1] + sine * x[:, slot + 1]
            made = (straight + swap_halves(crossed)) * scale_out
            source[pl.ds(base, 8 * group.width), sites] = made.reshape(
                8 * group.width, chunk
            ).astype(BF16)

        each(0, steps, step)

    def distribute(group, colours, far):
        picked = pl.ds(group.left, group.width)
        taken = pl.ds(colours[0], len(colours))
        height = 8 * group.width * len(colours)
        base = 8 * group.width * colours[0]
        if direct:
            lanes = pl.ds(pl.multiple_of(me * piece, piece), piece)
            target = out.at[:, taken, picked, :, lanes]
        else:
            target = out.at[me, :, taken, picked]

        def send_pieces(t):
            other = (1 - side if far else side) * half + lax.rem(chip + t, half)
            chosen = jnp.dot(
                source[base : base + height], onehot[other], preferred_element_type=F32
            )
            chosen = chosen.reshape(len(colours), group.width, 8, 2 * piece)
            for which in range(2):
                values = chosen[..., which * piece : (which + 1) * piece]
                for i, colour in enumerate(colours):
                    for part in range(2):
                        staged[
                            2 * other + which, part, colour, group.left : group.left + group.width
                        ] = values[i, :, 4 * part : 4 * part + 4].astype(BF16)

            def send(peer):
                remote(
                    staged.at[peer, :, taken, picked], target, out_send, out_recv, peer
                ).start()

            if far:
                send(2 * other)
                send(2 * other + 1)
            else:

                @pl.when(other != chip)
                def _():
                    send(2 * other)
                    send(2 * other + 1)

                @pl.when(other == chip)
                def _():
                    send(partner)
                    pltpu.make_async_copy(
                        staged.at[me, :, taken, picked], target, own_sem
                    ).start()

        each(0 if far else 1, half if far else half + 1, send_pieces)

    relay(0)
    rebuild(plan[0], 0)
    distribute(plan[0], (0,), True)
    each(1, 3, relay)
    pl.when(plan[1].passes)(functools.partial(pass_on, plan[1]))
    each(1, 3, lambda colour: rebuild(plan[0], colour))
    distribute(plan[0], (1, 2), True)
    distribute(plan[0], (0, 1, 2), False)
    rebuild(plan[1], 0)
    distribute(plan[1], (0,), True)
    each(1, 3, lambda colour: rebuild(plan[1], colour))
    distribute(plan[1], (0, 1, 2), False)
    distribute(plan[1], (1, 2), True)

    owns = functools.reduce(jnp.logical_or, [group.owns for group in plan])
    total_owners = 2 * sum(groups)

    def sent_sums(count):
        sent(summed.at[:, pl.ds(0, count)], chip_send)

    sent(from_core, core_send)

    pl.when(owns)(lambda: sent_sums(total_owners - 1))
    pl.when(jnp.logical_not(owns))(lambda: sent_sums(total_owners))

    line = 8 * (slots + len(fixed)) * nvec // length

    @pl.when(plan[0].owns)
    def _():
        sent(ready.at[:, pl.ds(0, chips - 1)], all_send)

    @pl.when(plan[1].owns)
    def _():
        sent(eig.at[0, :, pl.ds(0, 2 * half * line)], all_send)

    @pl.when(plan[1].passes)
    def _():
        sent(eig.at[0, :, pl.ds(0, 2 * (half - 1) * line)], pass_send)
        sent(rest.at[:, 0], partner_send)

    sent(coeffs.at[:, 0], fwd_send)
    sent(wanted.at[pl.ds(0, n - 1)], index_send)
    pltpu.make_async_copy(staged.at[0], staged.at[0], own_sem).wait()
    sent(staged.at[pl.ds(0, n - 1)], out_send)
    landed(staged.at[pl.ds(0, n - 1)], out_recv)


def on_device(
    propagator, eigvecs, operator_weights, sink_time, term_index, term_sign, solver_order
):
    columns, length = propagator.shape[3:]
    nvec = eigvecs.shape[2]
    n = lax.axis_size("space")
    chips = n // 2
    piece = length // n
    groups = (1,) * (columns % 8 // 4) + (2,) * (columns // 8)
    fixed = tuple(
        p for p in range(1, NMOM)
        if MOMENTA[p][:2] == (0, 0) and EXTENT * EXTENT % (2 * length) == 0
    )
    moving = tuple(p for p in range(1, NMOM) if p not in fixed)
    assert 4 * sum(groups) == columns and sum(groups) <= chips // 2
    slots = 1 + len(moving)
    owners = 2 * sum(groups)
    assert len(groups) == 2 and 8 * (slots + len(fixed)) * nvec % length == 0
    cell = (slots, 8, nvec)
    direct = piece % 128 == 0
    out_shape = (2, 3, columns, 4, length) if direct else (n, 2, 3, columns, 4, piece)
    propagator = propagator.transpose(0, 1, 3, 2, 4)
    smem = pl.BlockSpec(memory_space=pltpu.SMEM)
    hbm = pl.BlockSpec(memory_space=pltpu.HBM)
    dma = pltpu.SemaphoreType.DMA
    gathered = pl.pallas_call(
        functools.partial(
            kernel, n, groups, columns, 1.0 / math.sqrt(3.0 * length * n),
            1.0 / math.sqrt(NMOM * nvec), length, moving, fixed, direct,
        ),
        out_shape=pltpu.VMEM(out_shape, BF16),
        in_specs=[hbm, hbm, smem, hbm, hbm, hbm, hbm],
        out_specs=pl.BlockSpec(memory_space=pl.ANY),
        scratch_shapes=[
            pltpu.VMEM(propagator.shape, BF16),
            pltpu.VMEM(eigvecs.shape, BF16),
            pltpu.VMEM(operator_weights.shape, F32),
            pltpu.VMEM(term_index.shape[::-1], jnp.int32),
            pltpu.VMEM((1,) + term_sign.shape, jnp.int32),
            pltpu.VMEM((n, 1, piece), jnp.int32),
            pltpu.VMEM((2 * len(moving), length), F32),
            pltpu.VMEM((2 * max(len(fixed), 1), chips, 1, nvec), F32),
            pltpu.VMEM((24 * (1 + len(fixed)), nvec), F32),
            pltpu.VMEM((3, 2, owners) + cell, F32),
            pltpu.VMEM((3, owners) + cell, F32),
            pltpu.VMEM((3, owners) + cell, BF16),
            pltpu.VMEM((3, chips) + cell, BF16),
            pltpu.VMEM((3, chips) + cell, BF16),
            pltpu.VMEM((3, 2, 2 * groups[0]) + cell, BF16),
            pltpu.VMEM((3, 4 * groups[1], slots + len(fixed), 8, nvec), BF16),
            pltpu.VMEM((4 * max(groups), slots, 8, nvec), BF16),
            pltpu.VMEM((12 * 8 * max(groups), length), BF16),
            pltpu.VMEM((n, 1, piece), jnp.int32),
            pltpu.VMEM((chips, length, 2 * piece), BF16),
            pltpu.VMEM((n, 2, 3, columns, 4, piece), BF16),
            dma((16,)), dma((len(groups), 3)), dma((3,)), dma((len(groups), 3)), dma((3,)), dma((3,)),
            dma((11,)),
        ],
        compiler_params=pltpu.CompilerParams(
            collective_id=0, has_side_effects=True, vmem_limit_bytes=int(48 * 2**20)
        ),
    )(
        *(
            x if x.size == 1 else pltpu.with_memory_space_constraint(x, pltpu.HBM)
            for x in (
                propagator, eigvecs, sink_time.reshape(1, 1), operator_weights,
                term_index.T, term_sign.reshape(1, -1), solver_order.reshape(n, 1, piece),
            )
        )
    )
    if direct:
        return gathered.transpose(0, 1, 3, 2, 4)
    placed = gathered.transpose(1, 2, 4, 3, 0, 5)
    return placed.reshape(2, 3, 4, columns, length)


def solution(mesh):
    return jax.shard_map(
        on_device,
        mesh=mesh,
        in_specs=(
            P("grp", None, None, None, "space"),
            P("grp", None, None, "space"),
            P("grp", None, None),
            P("grp"),
            P(),
            P(),
            P("space"),
        ),
        out_specs=P("grp", None, None, None, "space"),
        check_vma=False,
    )
```

```python
import functools
import math

import jax
import jax.numpy as jnp
from jax import lax
from jax.experimental import pallas as pl
from jax.experimental.pallas import tpu as pltpu
from jax.sharding import PartitionSpec as P

NMOM = 4
EXTENT = 64
MOMENTA = ((0, 0, 0), (1, 0, 0), (0, 1, 0), (0, 0, 1))
F32 = jnp.float32
BF16 = jnp.bfloat16
MESH = pl.DeviceIdType.MESH


def swap_halves(x):
    top, bottom = x[..., :4, :], x[..., 4:, :]
    return jnp.concatenate([-bottom, top], axis=-2)


def dot_exact(a, b):
    high = b.astype(BF16)
    low = (b - high.astype(F32)).astype(BF16)
    return jnp.dot(a, high, preferred_element_type=F32) + jnp.dot(a, low, preferred_element_type=F32)


def kernel(
    n, depth, columns, scale_in, scale_out, chunk, moving, fixed, direct,
    prop_hbm, eig_hbm, sink, table_hbm, term_rows_hbm, term_sign_hbm, order_hbm, out,
    prop, eig, table_weights, term_rows, term_sign, order, trig, turn, acc,
    blocks_a, blocks_b, from_core_a, from_core_b, summed_a, summed_b, from_chips_a, from_chips_b,
    ready, coeffs, rest, lhs, source, wanted, onehot, staged,
    load_sem, core_recv, chip_recv, all_recv, fwd_recv, mate_recv, pass_send, sems,
):
    me = lax.axis_index("space")
    chips = n // 2
    half = chips // 2
    core = lax.rem(me, 2)
    chip = me // 2
    side = chip // half
    partner = me + 1 - 2 * core
    length = eig.shape[-1]
    nvec = eig.shape[2]
    piece = order.shape[-1]
    steps = length // chunk
    slots = 1 + len(moving)
    (
        core_send_a, core_send_b, chip_send_a, chip_send_b, all_send_a, all_send_b, fwd_send_a,
        fwd_send_b, index_send, index_recv, out_send, out_recv, own_sem,
    ) = (sems.at[i] for i in range(13))

    def each(lower, upper, body):
        def step(i, carry):
            body(i)
            return carry

        lax.fori_loop(lower, upper, step, 0)

    def far_chips(body):
        each(0, half, lambda t: body((1 - side) * half + lax.rem(chip + t, half)))

    def near_chips(body):
        each(1, half, lambda t: body(side * half + lax.rem(chip + t, half)))

    def remote(src, dst, send_sem, recv_sem, device):
        return pltpu.make_async_remote_copy(
            src_ref=src, dst_ref=dst, send_sem=send_sem, recv_sem=recv_sem,
            device_id={"space": device}, device_id_type=MESH,
        )

    def sent(ref, sem):
        remote(ref, ref, sem, sem, partner).wait_send()

    def landed(ref, sem):
        remote(ref, ref, sem, sem, partner).wait_recv()

    owners = 2 * depth
    central = (chip >= half - depth) & (chip < half + depth)
    place = chip - half + depth

    def each_owner(body):
        def step(t):
            owner = lax.rem(t + (1 - side) * depth, owners)
            other = half - depth + owner

            @pl.when(other != chip)
            def _():
                body(owner, other)

        each(0, owners, step)

    class Group:
        def __init__(self, index, left, cores, *refs):
            self.index, self.left, self.cores = index, left, cores
            self.width = owners * len(cores)
            self.owns = central & (core == 1) if len(cores) == 1 else central
            self.row = core if len(cores) == 2 else 0
            self.blocks, self.from_core, self.summed, self.from_chips = refs[:4]
            self.core_send, self.chip_send = refs[4:]

    plan = (
        Group(
            0, 0, (1,), blocks_a, from_core_a, summed_a, from_chips_a, core_send_a, chip_send_a
        ),
        Group(
            1, owners, (0, 1), blocks_b, from_core_b, summed_b, from_chips_b, core_send_b,
            chip_send_b,
        ),
    )

    middle = length // 2

    def load(colour, part):
        sites = slice(part * middle, (part + 1) * middle)
        sem = 4 * colour + 2 * part
        return (
            pltpu.make_async_copy(
                prop_hbm.at[:, colour, :, :, sites], prop.at[:, colour, :, :, sites],
                load_sem.at[sem],
            ),
            pltpu.make_async_copy(
                eig_hbm.at[:, colour, :, sites], eig.at[:, colour, :, sites], load_sem.at[sem + 1]
            ),
        )

    def start(copies):
        for copy in copies:
            copy.start()

    def finish(copies):
        for copy in copies:
            copy.wait()

    small_loads = tuple(
        pltpu.make_async_copy(remote_ref, own_ref, load_sem.at[12 + i])
        for i, (remote_ref, own_ref) in enumerate((
            (order_hbm, order), (table_hbm, table_weights), (term_rows_hbm, term_rows),
            (term_sign_hbm, term_sign),
        ))
    )
    start(load(0, 0))
    start(load(0, 1))
    barrier = pltpu.get_barrier_semaphore()
    each(1, n, lambda t: pl.semaphore_signal(
        barrier, inc=1, device_id={"space": lax.rem(me + t, n)}, device_id_type=MESH
    ))

    bits = EXTENT.bit_length() - 1
    low = EXTENT - 1

    def angles(p, site):
        coords = (site & low, (site >> bits) & low, site >> (2 * bits))
        winding = sum(step * coord for step, coord in zip(MOMENTA[p], coords) if step) & low
        return winding.astype(F32) * (2.0 * math.pi / EXTENT)

    tiles = length // 128
    compact = me * length + 128 * lax.broadcasted_iota(
        jnp.int32, (tiles, 128), 0
    ) + lax.broadcasted_iota(jnp.int32, (tiles, 128), 1)
    for slot, p in enumerate(moving):
        angle = angles(p, compact)
        for part, values in enumerate((jnp.cos(angle), jnp.sin(angle))):
            trig[2 * slot + part : 2 * slot + part + 1, :] = jnp.concatenate(
                [values[tile : tile + 1] for tile in range(tiles)], axis=1
            )
    for i, p in enumerate(fixed):
        angle = angles(p, 2 * length * lax.broadcasted_iota(jnp.int32, (chips, nvec), 0))
        turn[2 * i] = jnp.cos(angle)[:, None]
        turn[2 * i + 1] = jnp.sin(angle)[:, None]
    start(small_loads)
    start(load(1, 0))
    start(load(1, 1))

    def core_copy(group, colour):
        row = 1 - core if len(group.cores) == 2 else 0
        return remote(
            group.blocks.at[colour, row], group.from_core.at[colour], group.core_send,
            core_recv.at[group.index, colour], partner,
        )

    def exchange(group, colour):
        if len(group.cores) == 2:
            core_copy(group, colour).start()
        else:
            pl.when(core == 0)(lambda: core_copy(group, colour).start())

    def send_sums(group, colour):
        def run():
            core_copy(group, colour).wait_recv()

            def send(owner, other):
                group.summed[colour, owner] = (
                    group.blocks[colour, group.row, owner] + group.from_core[colour, owner]
                ).astype(BF16)
                remote(
                    group.summed.at[colour, owner], group.from_chips.at[colour, chip],
                    group.chip_send, chip_recv.at[group.index, colour], other * 2 + core,
                ).start()

            each_owner(send)

        if len(group.cores) == 2:
            run()
        else:
            pl.when(core == 1)(run)

    def project(group, colour, between):
        quarter = slots * 4 * group.width
        wide = -(-quarter // 128) * 128
        picked = slice(group.left, group.left + group.width)
        total = None
        for part in range(2):
            between(part)
            sites = slice(part * middle, (part + 1) * middle)
            real = prop[0, colour, picked, :, sites].astype(F32).reshape(4 * group.width, middle)
            imag = prop[1, colour, picked, :, sites].astype(F32).reshape(4 * group.width, middle)
            reals, imags = [real], [imag]
            for slot in range(len(moving)):
                cosine = trig[2 * slot : 2 * slot + 1, sites]
                sine = trig[2 * slot + 1 : 2 * slot + 2, sites]
                reals.append(cosine * real + sine * imag)
                imags.append(cosine * imag - sine * real)
            spare = [jnp.zeros((wide - quarter, middle), F32)] if wide > quarter else []
            rows = jnp.concatenate(reals + spare + imags + spare).astype(BF16)
            both = jnp.concatenate([eig[0, colour, :, sites], eig[1, colour, :, sites]])
            made = lax.dot_general(
                both, rows, (((1,), (1,)), ((), ())), preferred_element_type=F32
            )
            total = made if total is None else total + made
        with_real, with_imag = total[:nvec] * scale_in, total[nvec:] * scale_in
        real = (with_real[:, :wide] + with_imag[:, wide:]).T[:quarter]
        imag = (with_real[:, wide:] - with_imag[:, :wide]).T[:quarter]
        shape = (slots, len(group.cores), owners, 4, nvec)
        made = jnp.concatenate([real.reshape(shape), imag.reshape(shape)], axis=3)
        for slot in range(slots):
            group.blocks[colour, :, :, slot] = made[slot]

    def send_index(t):
        peer = lax.rem(me + t, n)
        remote(order.at[peer], wanted.at[me], index_send, index_recv, peer).start()

    for group in plan:
        opening = group.index == 0

        def stage(colour, group=group, opening=opening):
            def between(part):
                if opening:
                    finish(load(colour, part))
                    if part == 0:

                        @pl.when(colour == 0)
                        def _():
                            start(load(2, 0))
                            start(load(2, 1))

            project(group, colour, between)
            if opening:
                pl.when(colour == 0)(lambda: pl.semaphore_wait(barrier, n - 1))
            exchange(group, colour)

            @pl.when(colour == 0)
            def _():
                if opening:
                    finish(small_loads[:1])
                    each(1, n, send_index)
                    wanted[pl.ds(me, 1)] = order[pl.ds(me, 1)]
                else:
                    send_sums(plan[group.index - 1], 2)

            pl.when(colour > 0)(lambda: send_sums(group, colour - 1))

        each(0, 3, stage)
    send_sums(plan[-1], 2)

    terms = term_rows.shape[1]
    finish(small_loads[1:])

    def spread(cell, colour, sem):
        near_chips(
            lambda other: remote(
                cell, cell, sem, all_recv.at[1, colour], other * 2 + core
            ).start()
        )

    def pass_on(colour):
        cell = rest.at[colour, core * owners + lax.rem(place + depth, owners)]
        landed(cell, mate_recv.at[colour])
        spread(cell, colour, pass_send.at[colour])

    def contract(group):
        eye = lax.broadcasted_iota(jnp.int32, (terms, terms), 0) == lax.broadcasted_iota(
            jnp.int32, (terms, terms), 1
        )
        lane = lax.broadcasted_iota(jnp.int32, (terms, 24), 1)
        lane_channel = (4 * (lane >> 3) + (lane & 3)).astype(F32)
        lane_imag = (lane >> 2) & 1
        picks = []
        for which in range(2):
            row = term_rows[which : which + 1, :].astype(F32)
            column = jnp.sum(jnp.where(eye, row, 0.0), axis=1, keepdims=True)
            for part in range(2):
                hit = (lane_channel == column) & (lane_imag == part)
                picks.append(jnp.where(hit, 1.0, 0.0))
        picks = jnp.concatenate(picks).astype(BF16)
        sub = lax.broadcasted_iota(jnp.int32, (24, terms), 0)
        target = 4 * (sub >> 3) + (sub & 3) == term_rows[2:3, :]
        signs = (2 * term_sign[...] - 1).astype(F32)
        place_real = jnp.where(target & (((sub >> 2) & 1) == 0), signs, 0.0).astype(BF16)
        place_imag = jnp.where(target & (((sub >> 2) & 1) == 1), signs, 0.0).astype(BF16)
        weights = table_weights[sink[0, 0]]
        weight_real, weight_imag = weights[0:1, :], weights[1:2, :]

        totals = []
        for colour in range(3):
            own = group.blocks[colour, group.row, place] + group.from_core[colour, place]
            landed(
                group.from_chips.at[colour, pl.ds(0, chips - 1)], chip_recv.at[group.index, colour]
            )

            def turned(part, source_chip):
                kept = []
                for i in range(len(fixed)):
                    kept.append(turn[2 * i, pl.ds(source_chip, 1)][0] * part[0])
                    kept.append(turn[2 * i + 1, pl.ds(source_chip, 1)][0] * part[0])
                return kept

            def add_sum(t, carry, colour=colour):
                other = lax.rem(chip + chips - t, chips)
                part = group.from_chips[colour, other].astype(F32)
                return tuple(a + b for a, b in zip(carry, (part, *turned(part, other))))

            total, *kept = lax.fori_loop(1, chips, add_sum, (own, *turned(own, chip)))
            extra = [
                kept[2 * i] - swap_halves(kept[2 * i + 1]) for i in range(len(fixed))
            ]
            totals.append([total[slot] for slot in range(slots)] + extra)

        count = slots + len(fixed)
        block = jnp.concatenate([
            jnp.concatenate([total[unit] for total in totals]) for unit in range(count)
        ], axis=1)
        picked = dot_exact(picks, block)
        first_real, first_imag = picked[:terms], picked[terms : 2 * terms]
        other_real, other_imag = picked[2 * terms : 3 * terms], picked[3 * terms :]
        real_products, imag_products = [], []
        for unit in range(count):
            lanes = slice(unit * nvec, (unit + 1) * nvec)
            o_real, o_imag = other_real[:, lanes], other_imag[:, lanes]
            f_real, f_imag = first_real[:, lanes], first_imag[:, lanes]
            second_real = jnp.sum(
                weight_real * o_real - weight_imag * o_imag, axis=1, keepdims=True
            )
            second_imag = jnp.sum(
                weight_real * o_imag + weight_imag * o_real, axis=1, keepdims=True
            )
            real_products.append(f_real * second_real - f_imag * second_imag)
            imag_products.append(f_real * second_imag + f_imag * second_real)
        made = dot_exact(place_real, jnp.concatenate(real_products, axis=1)) + dot_exact(
            place_imag, jnp.concatenate(imag_products, axis=1)
        )
        if group.index > 0:
            for unit in range(count):
                part = made[:, unit * nvec : (unit + 1) * nvec].reshape(3, 8, nvec).astype(BF16)
                for colour in range(3):
                    rest[colour, core * owners + place, unit] = part[colour]

            mate = half - depth + lax.rem(place + depth, owners)

            def send_mate(colour):
                cell = rest.at[colour, core * owners + place]
                remote(cell, cell, all_send_b, mate_recv.at[colour], mate * 2 + core).start()

            each(0, 3, send_mate)
            each(
                0, 3,
                lambda colour: spread(rest.at[colour, core * owners + place], colour, all_send_b),
            )
            return
        acc[:24, :] = made[:, :nvec]
        for i in range(len(fixed)):
            acc[24 * (i + 1) : 24 * (i + 2), :] = made[:, (slots + i) * nvec : (slots + i + 1) * nvec]
        plain = made[:, nvec : slots * nvec].reshape(3, 8, (slots - 1) * nvec).astype(BF16)

        def merged(colour, other):
            value = acc[8 * colour : 8 * colour + 8, :]
            for i in range(len(fixed)):
                side_value = acc[24 * (i + 1) + 8 * colour : 24 * (i + 1) + 8 * colour + 8, :]
                value = value + turn[2 * i, other] * side_value
                value = value + turn[2 * i + 1, other] * swap_halves(side_value)
            return value.astype(BF16)

        for colour in range(3):
            others = [plain[colour, :, slot * nvec : (slot + 1) * nvec] for slot in range(slots - 1)]
            target = coeffs.at[colour, place]
            coeffs[colour, place, 0] = merged(colour, chip)
            for slot in range(slots - 1):
                coeffs[colour, place, slot + 1] = others[slot]

            def send_coeffs(other, colour=colour, others=others, target=target):
                ready[colour, other, 0] = merged(colour, other)
                for slot in range(slots - 1):
                    ready[colour, other, slot + 1] = others[slot]
                remote(
                    ready.at[colour, other], target, all_send_a, all_recv.at[group.index, colour],
                    other * 2 + core,
                ).start()

            far_chips(send_coeffs)
            near_chips(send_coeffs)

    def build(peer_chip):
        position = lax.broadcasted_iota(jnp.int32, (length, piece), 0)
        for which in range(2):
            local = wanted[pl.ds(peer_chip * 2 + which, 1)][0] - me * length
            onehot[pl.ds(peer_chip, 1), :, which * piece : (which + 1) * piece] = jnp.where(
                position == local, 1.0, 0.0
            ).astype(BF16)[None]

    def build_all():
        landed(wanted.at[pl.ds(0, n - 1)], index_recv)
        each(0, chips, build)

    for i, group in enumerate(plan):
        if i == 0 and len(plan) == 1:
            build_all()
        pl.when(group.owns)(functools.partial(contract, group))
        if i == 0 and len(plan) > 1:
            build_all()

    def relay(group, colour):
        index = group.index

        def take(count):
            pieces = (coeffs, rest)[index].at[colour, pl.ds(0, count)]
            landed(pieces, all_recv.at[index, colour])

        def run():
            pl.when(central)(lambda: take(owners - 1 if index == 0 else owners - 2))
            pl.when(jnp.logical_not(central))(lambda: take(owners))
            if index == 0:
                cells = coeffs.at[colour]
            else:
                cells = rest.at[colour, pl.ds(core * owners, owners)]
            remote(
                cells, cells, (fwd_send_a, fwd_send_b)[index], fwd_recv.at[index, colour], partner
            ).start()

        if index == 0:
            pl.when(core == 1)(run)
        else:
            run()

    def rebuild(group, colour):
        height = group.width * slots * 8
        if group.index == 0:
            pl.when(core == 0)(lambda: landed(coeffs.at[colour], fwd_recv.at[0, colour]))
            lhs[: group.width] = coeffs[colour]
        else:
            landed(rest.at[colour, pl.ds((1 - core) * owners, owners)], fwd_recv.at[1, colour])
            table = rest[colour].reshape(group.width, slots + len(fixed), 8, nvec)
            still = table[:, 0].astype(F32)
            for i in range(len(fixed)):
                turned = table[:, slots + i].astype(F32)
                still = still + turn[2 * i, chip] * turned
                still = still + turn[2 * i + 1, chip] * swap_halves(turned)
            lhs[: group.width, 0] = still.astype(BF16)
            lhs[: group.width, 1:] = table[:, 1:slots]
        base = pl.multiple_of(colour * 8 * group.width, 8 * group.width)

        def step(step):
            sites = pl.ds(pl.multiple_of(step * chunk, chunk), chunk)
            x, y = (
                jnp.dot(
                    lhs[: group.width].reshape(height, nvec), eig[part, colour, :, sites],
                    preferred_element_type=F32,
                ).reshape(group.width, slots, 8, chunk)
                for part in range(2)
            )
            straight, crossed = x[:, 0], y[:, 0]
            for slot in range(len(moving)):
                cosine = trig[2 * slot : 2 * slot + 1, sites][None]
                sine = trig[2 * slot + 1 : 2 * slot + 2, sites][None]
                straight = straight + cosine * x[:, slot + 1] - sine * y[:, slot + 1]
                crossed = crossed + cosine * y[:, slot + 1] + sine * x[:, slot + 1]
            made = (straight + swap_halves(crossed)) * scale_out
            source[pl.ds(base, 8 * group.width), sites] = made.reshape(
                8 * group.width, chunk
            ).astype(BF16)

        each(0, steps, step)

    def distribute(group, colours, far):
        picked = pl.ds(group.left, group.width)
        taken = pl.ds(colours[0], len(colours))
        height = 8 * group.width * len(colours)
        base = 8 * group.width * colours[0]
        if direct:
            lanes = pl.ds(pl.multiple_of(me * piece, piece), piece)
            target = out.at[:, taken, picked, :, lanes]
        else:
            target = out.at[me, :, taken, picked]

        def send_pieces(t):
            if far:
                step = t + lax.rem(chip, 2) * (1 - 2 * lax.rem(t, 2))
                other = jnp.where(side == 0, chips - 1 - step, step)
            else:
                local = chip - side * half
                step = jnp.where(t >= local, t + 1, t)
                other = side * half + jnp.where(t == half - 1, local, step)
            chosen = jnp.dot(
                source[base : base + height], onehot[other], preferred_element_type=F32
            )
            chosen = chosen.reshape(len(colours), group.width, 8, 2 * piece)
            for which in range(2):
                values = chosen[..., which * piece : (which + 1) * piece]
                for i, colour in enumerate(colours):
                    for part in range(2):
                        staged[
                            2 * other + which, part, colour, group.left : group.left + group.width
                        ] = values[i, :, 4 * part : 4 * part + 4].astype(BF16)

            def send(peer):
                remote(
                    staged.at[peer, :, taken, picked], target, out_send, out_recv, peer
                ).start()

            if far:
                send(2 * other)
                send(2 * other + 1)
            else:

                @pl.when(other != chip)
                def _():
                    send(2 * other)
                    send(2 * other + 1)

                @pl.when(other == chip)
                def _():
                    send(partner)
                    pltpu.make_async_copy(
                        staged.at[me, :, taken, picked], target, own_sem
                    ).start()

        each(0, half, send_pieces)

    early, late = plan
    relay(early, 0)
    rebuild(early, 0)
    distribute(early, (0,), True)
    each(1, 3, lambda colour: relay(early, colour))
    each(1, 3, lambda colour: rebuild(early, colour))
    pl.when(central)(lambda: each(0, 3, pass_on))
    distribute(early, (1, 2), True)
    relay(late, 0)
    distribute(early, (0, 1, 2), False)
    rebuild(late, 0)
    distribute(late, (0,), True)
    each(1, 3, lambda colour: relay(late, colour))
    each(1, 3, lambda colour: rebuild(late, colour))
    distribute(late, (0, 1, 2), False)
    distribute(late, (1, 2), True)

    def close(group):
        pl.when(central)(lambda: sent(group.summed.at[:, pl.ds(0, owners - 1)], group.chip_send))
        pl.when(jnp.logical_not(central))(lambda: sent(group.summed, group.chip_send))

    @pl.when(core == 0)
    def _():
        sent(from_core_a, core_send_a)

    @pl.when(core == 1)
    def _():
        close(early)
        sent(coeffs, fwd_send_a)

    sent(from_core_b, core_send_b)
    close(late)
    sent(rest.at[:, pl.ds(0, owners)], fwd_send_b)

    @pl.when(early.owns)
    def _():
        sent(ready.at[:, pl.ds(0, chips - 1)], all_send_a)

    @pl.when(late.owns)
    def _():
        line = 8 * (slots + len(fixed)) * nvec // length
        sent(eig.at[0, :, pl.ds(0, half * line)], all_send_b)
        for colour in range(3):
            sent(prop.at[0, :, pl.ds(0, (half - 1) // 3)], pass_send.at[colour])

    sent(wanted.at[pl.ds(0, n - 1)], index_send)
    pltpu.make_async_copy(staged.at[0], staged.at[0], own_sem).wait()
    sent(staged.at[pl.ds(0, n - 1)], out_send)
    landed(staged.at[pl.ds(0, n - 1)], out_recv)


def on_device(
    propagator, eigvecs, operator_weights, sink_time, term_index, term_sign, solver_order
):
    columns, length = propagator.shape[3:]
    nvec = eigvecs.shape[2]
    n = lax.axis_size("space")
    chips = n // 2
    piece = length // n
    depth = columns // 6
    fixed = tuple(
        p for p in range(1, NMOM)
        if MOMENTA[p][:2] == (0, 0) and EXTENT * EXTENT % (2 * length) == 0
    )
    moving = tuple(p for p in range(1, NMOM) if p not in fixed)
    assert 6 * depth == columns and depth <= chips // 2 and (chips // 2 - 1) % 3 == 0
    slots = 1 + len(moving)
    owners = 2 * depth
    assert 8 * (slots + len(fixed)) * nvec == 4 * length
    cell = (slots, 8, nvec)
    direct = piece % 128 == 0
    out_shape = (2, 3, columns, 4, length) if direct else (n, 2, 3, columns, 4, piece)
    propagator = propagator.transpose(0, 1, 3, 2, 4)
    smem = pl.BlockSpec(memory_space=pltpu.SMEM)
    hbm = pl.BlockSpec(memory_space=pltpu.HBM)
    dma = pltpu.SemaphoreType.DMA
    gathered = pl.pallas_call(
        functools.partial(
            kernel, n, depth, columns, 1.0 / math.sqrt(3.0 * length * n),
            1.0 / math.sqrt(NMOM * nvec), length, moving, fixed, direct,
        ),
        out_shape=pltpu.VMEM(out_shape, BF16),
        in_specs=[hbm, hbm, smem, hbm, hbm, hbm, hbm],
        out_specs=pl.BlockSpec(memory_space=pl.ANY),
        scratch_shapes=[
            pltpu.VMEM(propagator.shape, BF16),
            pltpu.VMEM(eigvecs.shape, BF16),
            pltpu.VMEM(operator_weights.shape, F32),
            pltpu.VMEM(term_index.shape[::-1], jnp.int32),
            pltpu.VMEM((1,) + term_sign.shape, jnp.int32),
            pltpu.VMEM((n, 1, piece), jnp.int32),
            pltpu.VMEM((2 * len(moving), length), F32),
            pltpu.VMEM((2 * max(len(fixed), 1), chips, 1, nvec), F32),
            pltpu.VMEM((24 * (1 + len(fixed)), nvec), F32),
            pltpu.VMEM((3, 1, owners) + cell, F32),
            pltpu.VMEM((3, 2, owners) + cell, F32),
            pltpu.VMEM((3, owners) + cell, F32),
            pltpu.VMEM((3, owners) + cell, F32),
            pltpu.VMEM((3, owners) + cell, BF16),
            pltpu.VMEM((3, owners) + cell, BF16),
            pltpu.VMEM((3, chips) + cell, BF16),
            pltpu.VMEM((3, chips) + cell, BF16),
            pltpu.VMEM((3, chips) + cell, BF16),
            pltpu.VMEM((3, owners) + cell, BF16),
            pltpu.VMEM((3, 2 * owners, slots + len(fixed), 8, nvec), BF16),
            pltpu.VMEM((2 * owners, slots, 8, nvec), BF16),
            pltpu.VMEM((3 * 8 * 2 * owners, length), BF16),
            pltpu.VMEM((n, 1, piece), jnp.int32),
            pltpu.VMEM((chips, length, 2 * piece), BF16),
            pltpu.VMEM((n, 2, 3, columns, 4, piece), BF16),
            dma((16,)), dma((2, 3)), dma((2, 3)), dma((2, 3)), dma((2, 3)), dma((3,)), dma((3,)),
            dma((13,)),
        ],
        compiler_params=pltpu.CompilerParams(
            collective_id=0, has_side_effects=True, vmem_limit_bytes=int(48 * 2**20)
        ),
    )(
        *(
            x if x.size == 1 else pltpu.with_memory_space_constraint(x, pltpu.HBM)
            for x in (
                propagator, eigvecs, sink_time.reshape(1, 1), operator_weights,
                term_index.T, term_sign.reshape(1, -1), solver_order.reshape(n, 1, piece),
            )
        )
    )
    if direct:
        return gathered.transpose(0, 1, 3, 2, 4)
    placed = gathered.transpose(1, 2, 4, 3, 0, 5)
    return placed.reshape(2, 3, 4, columns, length)


def solution(mesh):
    return jax.shard_map(
        on_device,
        mesh=mesh,
        in_specs=(
            P("grp", None, None, None, "space"),
            P("grp", None, None, "space"),
            P("grp", None, None),
            P("grp"),
            P(),
            P(),
            P("space"),
        ),
        out_specs=P("grp", None, None, None, "space"),
        check_vma=False,
    )
```

```python
import functools
import math

import jax
import jax.numpy as jnp
from jax import lax
from jax.experimental import pallas as pl
from jax.experimental.pallas import tpu as pltpu
from jax.sharding import PartitionSpec as P

NMOM = 4
EXTENT = 64
MOMENTA = ((0, 0, 0), (1, 0, 0), (0, 1, 0), (0, 0, 1))
F32 = jnp.float32
BF16 = jnp.bfloat16
MESH = pl.DeviceIdType.MESH


def swap_halves(x):
    top, bottom = x[..., :4, :], x[..., 4:, :]
    return jnp.concatenate([-bottom, top], axis=-2)


def dot_exact(a, b):
    high = b.astype(BF16)
    low = (b - high.astype(F32)).astype(BF16)
    return jnp.dot(a, high, preferred_element_type=F32) + jnp.dot(a, low, preferred_element_type=F32)


def kernel(
    n, depth, columns, scale_in, scale_out, chunk, moving, fixed, direct,
    prop_hbm, eig_hbm, sink, table_hbm, term_rows_hbm, term_sign_hbm, order_hbm, out,
    prop, eig, table_weights, term_rows, term_sign, order, trig, turn, acc,
    blocks_a, blocks_b, from_core_a, from_core_b, summed_a, summed_b, from_chips_a, from_chips_b,
    ready, coeffs, rest, lhs, source, wanted, onehot, staged,
    load_sem, core_recv, chip_recv, all_recv, fwd_recv, mate_recv, pass_send, sems,
):
    me = lax.axis_index("space")
    chips = n // 2
    half = chips // 2
    core = lax.rem(me, 2)
    chip = me // 2
    side = chip // half
    partner = me + 1 - 2 * core
    length = eig.shape[-1]
    nvec = eig.shape[2]
    piece = order.shape[-1]
    steps = length // chunk
    slots = 1 + len(moving)
    (
        core_send_a, core_send_b, chip_send_a, chip_send_b, all_send_a, all_send_b, fwd_send_a,
        fwd_send_b, index_send, index_recv, out_send, out_recv, own_sem,
    ) = (sems.at[i] for i in range(13))

    def each(lower, upper, body):
        def step(i, carry):
            body(i)
            return carry

        lax.fori_loop(lower, upper, step, 0)

    def far_chips(body):
        each(0, half, lambda t: body((1 - side) * half + lax.rem(chip + t, half)))

    def near_chips(body):
        each(1, half, lambda t: body(side * half + lax.rem(chip + t, half)))

    def remote(src, dst, send_sem, recv_sem, device):
        return pltpu.make_async_remote_copy(
            src_ref=src, dst_ref=dst, send_sem=send_sem, recv_sem=recv_sem,
            device_id={"space": device}, device_id_type=MESH,
        )

    def sent(ref, sem):
        remote(ref, ref, sem, sem, partner).wait_send()

    def landed(ref, sem):
        remote(ref, ref, sem, sem, partner).wait_recv()

    owners = 2 * depth
    central = (chip >= half - depth) & (chip < half + depth)
    place = chip - half + depth

    def each_owner(body):
        def step(t):
            owner = lax.rem(t + (1 - side) * depth, owners)
            other = half - depth + owner

            @pl.when(other != chip)
            def _():
                body(owner, other)

        each(0, owners, step)

    class Group:
        def __init__(self, index, left, cores, *refs):
            self.index, self.left, self.cores = index, left, cores
            self.width = owners * len(cores)
            self.owns = central & (core == 1) if len(cores) == 1 else central
            self.row = core if len(cores) == 2 else 0
            self.blocks, self.from_core, self.summed, self.from_chips = refs[:4]
            self.core_send, self.chip_send = refs[4:]

    plan = (
        Group(
            0, 0, (1,), blocks_a, from_core_a, summed_a, from_chips_a, core_send_a, chip_send_a
        ),
        Group(
            1, owners, (0, 1), blocks_b, from_core_b, summed_b, from_chips_b, core_send_b,
            chip_send_b,
        ),
    )

    middle = length // 2

    def load(colour, part):
        sites = slice(part * middle, (part + 1) * middle)
        sem = 4 * colour + 2 * part
        return (
            pltpu.make_async_copy(
                prop_hbm.at[:, colour, :, :, sites], prop.at[:, colour, :, :, sites],
                load_sem.at[sem],
            ),
            pltpu.make_async_copy(
                eig_hbm.at[:, colour, :, sites], eig.at[:, colour, :, sites], load_sem.at[sem + 1]
            ),
        )

    def start(copies):
        for copy in copies:
            copy.start()

    def finish(copies):
        for copy in copies:
            copy.wait()

    small_loads = tuple(
        pltpu.make_async_copy(remote_ref, own_ref, load_sem.at[12 + i])
        for i, (remote_ref, own_ref) in enumerate((
            (order_hbm, order), (table_hbm, table_weights), (term_rows_hbm, term_rows),
            (term_sign_hbm, term_sign),
        ))
    )
    start(load(0, 0))
    start(load(0, 1))
    barrier = pltpu.get_barrier_semaphore()
    each(1, n, lambda t: pl.semaphore_signal(
        barrier, inc=1, device_id={"space": lax.rem(me + t, n)}, device_id_type=MESH
    ))

    bits = EXTENT.bit_length() - 1
    low = EXTENT - 1

    def angles(p, site):
        coords = (site & low, (site >> bits) & low, site >> (2 * bits))
        winding = sum(step * coord for step, coord in zip(MOMENTA[p], coords) if step) & low
        return winding.astype(F32) * (2.0 * math.pi / EXTENT)

    tiles = length // 128
    compact = me * length + 128 * lax.broadcasted_iota(
        jnp.int32, (tiles, 128), 0
    ) + lax.broadcasted_iota(jnp.int32, (tiles, 128), 1)
    for slot, p in enumerate(moving):
        angle = angles(p, compact)
        for part, values in enumerate((jnp.cos(angle), jnp.sin(angle))):
            trig[2 * slot + part : 2 * slot + part + 1, :] = jnp.concatenate(
                [values[tile : tile + 1] for tile in range(tiles)], axis=1
            )
    for i, p in enumerate(fixed):
        angle = angles(p, 2 * length * lax.broadcasted_iota(jnp.int32, (chips, nvec), 0))
        turn[2 * i] = jnp.cos(angle)[:, None]
        turn[2 * i + 1] = jnp.sin(angle)[:, None]
    start(small_loads)
    start(load(1, 0))
    start(load(1, 1))

    def core_copy(group, colour):
        row = 1 - core if len(group.cores) == 2 else 0
        return remote(
            group.blocks.at[colour, row], group.from_core.at[colour], group.core_send,
            core_recv.at[group.index, colour], partner,
        )

    def exchange(group, colour):
        if len(group.cores) == 2:
            core_copy(group, colour).start()
        else:
            pl.when(core == 0)(lambda: core_copy(group, colour).start())

    def send_sums(group, colour):
        def run():
            core_copy(group, colour).wait_recv()

            def send(owner, other):
                group.summed[colour, owner] = (
                    group.blocks[colour, group.row, owner] + group.from_core[colour, owner]
                ).astype(BF16)
                remote(
                    group.summed.at[colour, owner], group.from_chips.at[colour, chip],
                    group.chip_send, chip_recv.at[group.index, colour], other * 2 + core,
                ).start()

            each_owner(send)

        if len(group.cores) == 2:
            run()
        else:
            pl.when(core == 1)(run)

    def project(group, colour, between):
        quarter = slots * 4 * group.width
        wide = -(-quarter // 128) * 128
        picked = slice(group.left, group.left + group.width)
        total = None
        for part in range(2):
            between(part)
            sites = slice(part * middle, (part + 1) * middle)
            real = prop[0, colour, picked, :, sites].astype(F32).reshape(4 * group.width, middle)
            imag = prop[1, colour, picked, :, sites].astype(F32).reshape(4 * group.width, middle)
            reals, imags = [real], [imag]
            for slot in range(len(moving)):
                cosine = trig[2 * slot : 2 * slot + 1, sites]
                sine = trig[2 * slot + 1 : 2 * slot + 2, sites]
                reals.append(cosine * real + sine * imag)
                imags.append(cosine * imag - sine * real)
            spare = [jnp.zeros((wide - quarter, middle), F32)] if wide > quarter else []
            rows = jnp.concatenate(reals + spare + imags + spare).astype(BF16)
            both = jnp.concatenate([eig[0, colour, :, sites], eig[1, colour, :, sites]])
            made = lax.dot_general(
                both, rows, (((1,), (1,)), ((), ())), preferred_element_type=F32
            )
            total = made if total is None else total + made
        with_real, with_imag = total[:nvec] * scale_in, total[nvec:] * scale_in
        real = (with_real[:, :wide] + with_imag[:, wide:]).T[:quarter]
        imag = (with_real[:, wide:] - with_imag[:, :wide]).T[:quarter]
        shape = (slots, len(group.cores), owners, 4, nvec)
        made = jnp.concatenate([real.reshape(shape), imag.reshape(shape)], axis=3)
        for slot in range(slots):
            group.blocks[colour, :, :, slot] = made[slot]

    def send_index(t):
        peer = lax.rem(me + t, n)
        remote(order.at[peer], wanted.at[me], index_send, index_recv, peer).start()

    for group in plan:
        opening = group.index == 0

        def stage(colour, group=group, opening=opening):
            def between(part):
                if opening:
                    finish(load(colour, part))
                    if part == 0:

                        @pl.when(colour == 0)
                        def _():
                            start(load(2, 0))
                            start(load(2, 1))

            project(group, colour, between)
            if opening:
                pl.when(colour == 0)(lambda: pl.semaphore_wait(barrier, n - 1))
            exchange(group, colour)

            @pl.when(colour == 0)
            def _():
                if opening:
                    finish(small_loads[:1])
                    each(1, n, send_index)
                    wanted[pl.ds(me, 1)] = order[pl.ds(me, 1)]
                else:
                    send_sums(plan[group.index - 1], 2)

            pl.when(colour > 0)(lambda: send_sums(group, colour - 1))

        each(0, 3, stage)
    send_sums(plan[-1], 2)

    terms = term_rows.shape[1]
    finish(small_loads[1:])

    def spread(cell, colour, sem):
        near_chips(
            lambda other: remote(
                cell, cell, sem, all_recv.at[1, colour], other * 2 + core
            ).start()
        )

    def pass_on(colour):
        cell = rest.at[colour, core * owners + lax.rem(place + depth, owners)]
        landed(cell, mate_recv.at[colour])
        spread(cell, colour, pass_send.at[colour])

    def contract(group):
        eye = lax.broadcasted_iota(jnp.int32, (terms, terms), 0) == lax.broadcasted_iota(
            jnp.int32, (terms, terms), 1
        )
        lane = lax.broadcasted_iota(jnp.int32, (terms, 24), 1)
        lane_channel = (4 * (lane >> 3) + (lane & 3)).astype(F32)
        lane_imag = (lane >> 2) & 1
        picks = []
        for which in range(2):
            row = term_rows[which : which + 1, :].astype(F32)
            column = jnp.sum(jnp.where(eye, row, 0.0), axis=1, keepdims=True)
            for part in range(2):
                hit = (lane_channel == column) & (lane_imag == part)
                picks.append(jnp.where(hit, 1.0, 0.0))
        picks = jnp.concatenate(picks).astype(BF16)
        sub = lax.broadcasted_iota(jnp.int32, (24, terms), 0)
        target = 4 * (sub >> 3) + (sub & 3) == term_rows[2:3, :]
        signs = (2 * term_sign[...] - 1).astype(F32)
        place_real = jnp.where(target & (((sub >> 2) & 1) == 0), signs, 0.0).astype(BF16)
        place_imag = jnp.where(target & (((sub >> 2) & 1) == 1), signs, 0.0).astype(BF16)
        weights = table_weights[sink[0, 0]]
        weight_real, weight_imag = weights[0:1, :], weights[1:2, :]

        totals = []
        for colour in range(3):
            own = group.blocks[colour, group.row, place] + group.from_core[colour, place]
            landed(
                group.from_chips.at[colour, pl.ds(0, chips - 1)], chip_recv.at[group.index, colour]
            )

            def turned(part, source_chip):
                kept = []
                for i in range(len(fixed)):
                    kept.append(turn[2 * i, pl.ds(source_chip, 1)][0] * part[0])
                    kept.append(turn[2 * i + 1, pl.ds(source_chip, 1)][0] * part[0])
                return kept

            def add_sum(t, carry, colour=colour):
                other = lax.rem(chip + chips - t, chips)
                part = group.from_chips[colour, other].astype(F32)
                return tuple(a + b for a, b in zip(carry, (part, *turned(part, other))))

            total, *kept = lax.fori_loop(1, chips, add_sum, (own, *turned(own, chip)))
            extra = [
                kept[2 * i] - swap_halves(kept[2 * i + 1]) for i in range(len(fixed))
            ]
            totals.append([total[slot] for slot in range(slots)] + extra)

        count = slots + len(fixed)
        block = jnp.concatenate([
            jnp.concatenate([total[unit] for total in totals]) for unit in range(count)
        ], axis=1)
        picked = dot_exact(picks, block)
        first_real, first_imag = picked[:terms], picked[terms : 2 * terms]
        other_real, other_imag = picked[2 * terms : 3 * terms], picked[3 * terms :]
        real_products, imag_products = [], []
        for unit in range(count):
            lanes = slice(unit * nvec, (unit + 1) * nvec)
            o_real, o_imag = other_real[:, lanes], other_imag[:, lanes]
            f_real, f_imag = first_real[:, lanes], first_imag[:, lanes]
            second_real = jnp.sum(
                weight_real * o_real - weight_imag * o_imag, axis=1, keepdims=True
            )
            second_imag = jnp.sum(
                weight_real * o_imag + weight_imag * o_real, axis=1, keepdims=True
            )
            real_products.append(f_real * second_real - f_imag * second_imag)
            imag_products.append(f_real * second_imag + f_imag * second_real)
        made = dot_exact(place_real, jnp.concatenate(real_products, axis=1)) + dot_exact(
            place_imag, jnp.concatenate(imag_products, axis=1)
        )
        if group.index > 0:
            for unit in range(count):
                part = made[:, unit * nvec : (unit + 1) * nvec].reshape(3, 8, nvec).astype(BF16)
                for colour in range(3):
                    rest[colour, core * owners + place, unit] = part[colour]

            mate = half - depth + lax.rem(place + depth, owners)

            def send_mate(colour):
                cell = rest.at[colour, core * owners + place]
                remote(cell, cell, all_send_b, mate_recv.at[colour], mate * 2 + core).start()

            each(0, 3, send_mate)
            each(
                0, 3,
                lambda colour: spread(rest.at[colour, core * owners + place], colour, all_send_b),
            )
            return
        acc[:24, :] = made[:, :nvec]
        for i in range(len(fixed)):
            acc[24 * (i + 1) : 24 * (i + 2), :] = made[:, (slots + i) * nvec : (slots + i + 1) * nvec]
        plain = made[:, nvec : slots * nvec].reshape(3, 8, (slots - 1) * nvec).astype(BF16)

        def merged(colour, other):
            value = acc[8 * colour : 8 * colour + 8, :]
            for i in range(len(fixed)):
                side_value = acc[24 * (i + 1) + 8 * colour : 24 * (i + 1) + 8 * colour + 8, :]
                value = value + turn[2 * i, other] * side_value
                value = value + turn[2 * i + 1, other] * swap_halves(side_value)
            return value.astype(BF16)

        for colour in range(3):
            others = [plain[colour, :, slot * nvec : (slot + 1) * nvec] for slot in range(slots - 1)]
            target = coeffs.at[colour, place]
            coeffs[colour, place, 0] = merged(colour, chip)
            for slot in range(slots - 1):
                coeffs[colour, place, slot + 1] = others[slot]

            def send_coeffs(other, colour=colour, others=others, target=target):
                ready[colour, other, 0] = merged(colour, other)
                for slot in range(slots - 1):
                    ready[colour, other, slot + 1] = others[slot]
                remote(
                    ready.at[colour, other], target, all_send_a, all_recv.at[group.index, colour],
                    other * 2 + core,
                ).start()

            far_chips(send_coeffs)
            near_chips(send_coeffs)

    def build(peer_chip):
        position = lax.broadcasted_iota(jnp.int32, (length, piece), 0)
        for which in range(2):
            local = wanted[pl.ds(peer_chip * 2 + which, 1)][0] - me * length
            onehot[pl.ds(peer_chip, 1), :, which * piece : (which + 1) * piece] = jnp.where(
                position == local, 1.0, 0.0
            ).astype(BF16)[None]

    def build_all():
        landed(wanted.at[pl.ds(0, n - 1)], index_recv)
        each(0, chips, build)

    def relay(group, colour):
        index = group.index

        def take(count):
            pieces = (coeffs, rest)[index].at[colour, pl.ds(0, count)]
            landed(pieces, all_recv.at[index, colour])

        def run():
            pl.when(central)(lambda: take(owners - 1 if index == 0 else owners - 2))
            pl.when(jnp.logical_not(central))(lambda: take(owners))
            if index == 0:
                cells = coeffs.at[colour]
            else:
                cells = rest.at[colour, pl.ds(core * owners, owners)]
            remote(
                cells, cells, (fwd_send_a, fwd_send_b)[index], fwd_recv.at[index, colour], partner
            ).start()

        if index == 0:
            pl.when(core == 1)(run)
        else:
            run()

    def rebuild(group, colour):
        height = group.width * slots * 8
        if group.index == 0:
            pl.when(core == 0)(lambda: landed(coeffs.at[colour], fwd_recv.at[0, colour]))
            lhs[: group.width] = coeffs[colour]
        else:
            landed(rest.at[colour, pl.ds((1 - core) * owners, owners)], fwd_recv.at[1, colour])
            table = rest[colour].reshape(group.width, slots + len(fixed), 8, nvec)
            still = table[:, 0].astype(F32)
            for i in range(len(fixed)):
                turned = table[:, slots + i].astype(F32)
                still = still + turn[2 * i, chip] * turned
                still = still + turn[2 * i + 1, chip] * swap_halves(turned)
            lhs[: group.width, 0] = still.astype(BF16)
            lhs[: group.width, 1:] = table[:, 1:slots]
        base = pl.multiple_of(colour * 8 * group.width, 8 * group.width)

        def step(step):
            sites = pl.ds(pl.multiple_of(step * chunk, chunk), chunk)
            x, y = (
                jnp.dot(
                    lhs[: group.width].reshape(height, nvec), eig[part, colour, :, sites],
                    preferred_element_type=F32,
                ).reshape(group.width, slots, 8, chunk)
                for part in range(2)
            )
            straight, crossed = x[:, 0], y[:, 0]
            for slot in range(len(moving)):
                cosine = trig[2 * slot : 2 * slot + 1, sites][None]
                sine = trig[2 * slot + 1 : 2 * slot + 2, sites][None]
                straight = straight + cosine * x[:, slot + 1] - sine * y[:, slot + 1]
                crossed = crossed + cosine * y[:, slot + 1] + sine * x[:, slot + 1]
            made = (straight + swap_halves(crossed)) * scale_out
            source[pl.ds(base, 8 * group.width), sites] = made.reshape(
                8 * group.width, chunk
            ).astype(BF16)

        each(0, steps, step)

    def distribute(group, colours, far, last=False):
        picked = pl.ds(group.left, group.width)
        taken = pl.ds(colours[0], len(colours))
        height = 8 * group.width * len(colours)
        base = 8 * group.width * colours[0]
        if direct:
            lanes = pl.ds(pl.multiple_of(me * piece, piece), piece)
            target = out.at[:, taken, picked, :, lanes]
        else:
            target = out.at[me, :, taken, picked]

        def send_pieces(t):
            if far:
                swap = 1 - 2 * lax.rem(t, 2)
                if last:
                    swap = jnp.where(t < half - 2, swap, 0)
                step = t + lax.rem(chip, 2) * swap
                other = jnp.where(side == 0, chips - 1 - step, step)
            else:
                local = chip - side * half
                step = jnp.where(t >= local, t + 1, t)
                other = side * half + jnp.where(t == half - 1, local, step)
            chosen = jnp.dot(
                source[base : base + height], onehot[other], preferred_element_type=F32
            )
            chosen = chosen.reshape(len(colours), group.width, 8, 2 * piece)
            for which in range(2):
                values = chosen[..., which * piece : (which + 1) * piece]
                for i, colour in enumerate(colours):
                    for part in range(2):
                        staged[
                            2 * other + which, part, colour, group.left : group.left + group.width
                        ] = values[i, :, 4 * part : 4 * part + 4].astype(BF16)

            def send(peer):
                remote(
                    staged.at[peer, :, taken, picked], target, out_send, out_recv, peer
                ).start()

            if far:
                send(2 * other)
                send(2 * other + 1)
            else:

                @pl.when(other != chip)
                def _():
                    send(2 * other)
                    send(2 * other + 1)

                @pl.when(other == chip)
                def _():
                    send(partner)
                    pltpu.make_async_copy(
                        staged.at[me, :, taken, picked], target, own_sem
                    ).start()

        each(0, half, send_pieces)

    early, late = plan
    pl.when(early.owns)(functools.partial(contract, early))
    build_all()
    relay(early, 0)
    pl.when(late.owns)(functools.partial(contract, late))
    rebuild(early, 0)
    distribute(early, (0,), True)
    each(1, 3, lambda colour: relay(early, colour))
    pl.when(central)(lambda: pass_on(0))
    each(1, 3, lambda colour: rebuild(early, colour))
    distribute(early, (1, 2), True)
    pl.when(central)(lambda: each(1, 3, pass_on))
    relay(late, 0)
    distribute(early, (0, 1, 2), False)
    rebuild(late, 0)
    distribute(late, (0,), True)
    each(1, 3, lambda colour: relay(late, colour))
    each(1, 3, lambda colour: rebuild(late, colour))
    distribute(late, (0, 1, 2), False)
    distribute(late, (1, 2), True, True)

    def close(group):
        pl.when(central)(lambda: sent(group.summed.at[:, pl.ds(0, owners - 1)], group.chip_send))
        pl.when(jnp.logical_not(central))(lambda: sent(group.summed, group.chip_send))

    @pl.when(core == 0)
    def _():
        sent(from_core_a, core_send_a)

    @pl.when(core == 1)
    def _():
        close(early)
        sent(coeffs, fwd_send_a)

    sent(from_core_b, core_send_b)
    close(late)
    sent(rest.at[:, pl.ds(0, owners)], fwd_send_b)

    @pl.when(early.owns)
    def _():
        sent(ready.at[:, pl.ds(0, chips - 1)], all_send_a)

    @pl.when(late.owns)
    def _():
        line = 8 * (slots + len(fixed)) * nvec // length
        sent(eig.at[0, :, pl.ds(0, half * line)], all_send_b)
        for colour in range(3):
            sent(prop.at[0, :, pl.ds(0, (half - 1) // 3)], pass_send.at[colour])

    sent(wanted.at[pl.ds(0, n - 1)], index_send)
    pltpu.make_async_copy(staged.at[0], staged.at[0], own_sem).wait()
    sent(staged.at[pl.ds(0, n - 1)], out_send)
    landed(staged.at[pl.ds(0, n - 1)], out_recv)


def on_device(
    propagator, eigvecs, operator_weights, sink_time, term_index, term_sign, solver_order
):
    columns, length = propagator.shape[3:]
    nvec = eigvecs.shape[2]
    n = lax.axis_size("space")
    chips = n // 2
    piece = length // n
    depth = columns // 6
    fixed = tuple(
        p for p in range(1, NMOM)
        if MOMENTA[p][:2] == (0, 0) and EXTENT * EXTENT % (2 * length) == 0
    )
    moving = tuple(p for p in range(1, NMOM) if p not in fixed)
    assert 6 * depth == columns and depth <= chips // 2 and (chips // 2 - 1) % 3 == 0
    slots = 1 + len(moving)
    owners = 2 * depth
    assert 8 * (slots + len(fixed)) * nvec == 4 * length
    cell = (slots, 8, nvec)
    direct = piece % 128 == 0
    out_shape = (2, 3, columns, 4, length) if direct else (n, 2, 3, columns, 4, piece)
    propagator = propagator.transpose(0, 1, 3, 2, 4)
    smem = pl.BlockSpec(memory_space=pltpu.SMEM)
    hbm = pl.BlockSpec(memory_space=pltpu.HBM)
    dma = pltpu.SemaphoreType.DMA
    gathered = pl.pallas_call(
        functools.partial(
            kernel, n, depth, columns, 1.0 / math.sqrt(3.0 * length * n),
            1.0 / math.sqrt(NMOM * nvec), length, moving, fixed, direct,
        ),
        out_shape=pltpu.VMEM(out_shape, BF16),
        in_specs=[hbm, hbm, smem, hbm, hbm, hbm, hbm],
        out_specs=pl.BlockSpec(memory_space=pl.ANY),
        scratch_shapes=[
            pltpu.VMEM(propagator.shape, BF16),
            pltpu.VMEM(eigvecs.shape, BF16),
            pltpu.VMEM(operator_weights.shape, F32),
            pltpu.VMEM(term_index.shape[::-1], jnp.int32),
            pltpu.VMEM((1,) + term_sign.shape, jnp.int32),
            pltpu.VMEM((n, 1, piece), jnp.int32),
            pltpu.VMEM((2 * len(moving), length), F32),
            pltpu.VMEM((2 * max(len(fixed), 1), chips, 1, nvec), F32),
            pltpu.VMEM((24 * (1 + len(fixed)), nvec), F32),
            pltpu.VMEM((3, 1, owners) + cell, F32),
            pltpu.VMEM((3, 2, owners) + cell, F32),
            pltpu.VMEM((3, owners) + cell, F32),
            pltpu.VMEM((3, owners) + cell, F32),
            pltpu.VMEM((3, owners) + cell, BF16),
            pltpu.VMEM((3, owners) + cell, BF16),
            pltpu.VMEM((3, chips) + cell, BF16),
            pltpu.VMEM((3, chips) + cell, BF16),
            pltpu.VMEM((3, chips) + cell, BF16),
            pltpu.VMEM((3, owners) + cell, BF16),
            pltpu.VMEM((3, 2 * owners, slots + len(fixed), 8, nvec), BF16),
            pltpu.VMEM((2 * owners, slots, 8, nvec), BF16),
            pltpu.VMEM((3 * 8 * 2 * owners, length), BF16),
            pltpu.VMEM((n, 1, piece), jnp.int32),
            pltpu.VMEM((chips, length, 2 * piece), BF16),
            pltpu.VMEM((n, 2, 3, columns, 4, piece), BF16),
            dma((16,)), dma((2, 3)), dma((2, 3)), dma((2, 3)), dma((2, 3)), dma((3,)), dma((3,)),
            dma((13,)),
        ],
        compiler_params=pltpu.CompilerParams(
            collective_id=0, has_side_effects=True, vmem_limit_bytes=int(48 * 2**20)
        ),
    )(
        *(
            x if x.size == 1 else pltpu.with_memory_space_constraint(x, pltpu.HBM)
            for x in (
                propagator, eigvecs, sink_time.reshape(1, 1), operator_weights,
                term_index.T, term_sign.reshape(1, -1), solver_order.reshape(n, 1, piece),
            )
        )
    )
    if direct:
        return gathered.transpose(0, 1, 3, 2, 4)
    placed = gathered.transpose(1, 2, 4, 3, 0, 5)
    return placed.reshape(2, 3, 4, columns, length)


def solution(mesh):
    return jax.shard_map(
        on_device,
        mesh=mesh,
        in_specs=(
            P("grp", None, None, None, "space"),
            P("grp", None, None, "space"),
            P("grp", None, None),
            P("grp"),
            P(),
            P(),
            P("space"),
        ),
        out_specs=P("grp", None, None, None, "space"),
        check_vma=False,
    )
```

```python
import functools
import math

import jax
import jax.numpy as jnp
from jax import lax
from jax.experimental import pallas as pl
from jax.experimental.pallas import tpu as pltpu
from jax.sharding import PartitionSpec as P

NMOM = 4
EXTENT = 64
MOMENTA = ((0, 0, 0), (1, 0, 0), (0, 1, 0), (0, 0, 1))
F32 = jnp.float32
BF16 = jnp.bfloat16
MESH = pl.DeviceIdType.MESH


def swap_halves(x):
    top, bottom = x[..., :4, :], x[..., 4:, :]
    return jnp.concatenate([-bottom, top], axis=-2)


def dot_exact(a, b):
    high = b.astype(BF16)
    low = (b - high.astype(F32)).astype(BF16)
    return jnp.dot(a, high, preferred_element_type=F32) + jnp.dot(a, low, preferred_element_type=F32)


def kernel(
    n, depth, columns, scale_in, scale_out, chunk, moving, fixed, direct,
    prop_hbm, eig_hbm, sink, table_hbm, term_rows_hbm, term_sign_hbm, order_hbm, out,
    prop, eig, table_weights, term_rows, term_sign, order, trig, turn, acc,
    blocks_a, blocks_b, from_core_a, from_core_b, summed_a, summed_b, from_chips_a, from_chips_b,
    ready, coeffs, rest, lhs, source, wanted, onehot, staged,
    load_sem, core_recv, chip_recv, all_recv, fwd_recv, mate_recv, pass_send, sems,
):
    me = lax.axis_index("space")
    chips = n // 2
    half = chips // 2
    core = lax.rem(me, 2)
    chip = me // 2
    side = chip // half
    partner = me + 1 - 2 * core
    length = eig.shape[-1]
    nvec = eig.shape[2]
    piece = order.shape[-1]
    steps = length // chunk
    slots = 1 + len(moving)
    (
        core_send_a, core_send_b, chip_send_a, chip_send_b, all_send_a, all_send_b, fwd_send_a,
        fwd_send_b, index_send, index_recv, out_send, out_recv, own_sem,
    ) = (sems.at[i] for i in range(13))

    def each(lower, upper, body):
        def step(i, carry):
            body(i)
            return carry

        lax.fori_loop(lower, upper, step, 0)

    def far_chips(body):
        each(0, half, lambda t: body((1 - side) * half + lax.rem(chip + t, half)))

    def near_chips(body):
        each(1, half, lambda t: body(side * half + lax.rem(chip + t, half)))

    def remote(src, dst, send_sem, recv_sem, device):
        return pltpu.make_async_remote_copy(
            src_ref=src, dst_ref=dst, send_sem=send_sem, recv_sem=recv_sem,
            device_id={"space": device}, device_id_type=MESH,
        )

    def sent(ref, sem):
        remote(ref, ref, sem, sem, partner).wait_send()

    def landed(ref, sem):
        remote(ref, ref, sem, sem, partner).wait_recv()

    owners = 2 * depth
    central = (chip >= half - depth) & (chip < half + depth)
    place = chip - half + depth

    def each_owner(body):
        def step(t):
            owner = lax.rem(t + (1 - side) * depth, owners)
            other = half - depth + owner

            @pl.when(other != chip)
            def _():
                body(owner, other)

        each(0, owners, step)

    class Group:
        def __init__(self, index, left, cores, *refs):
            self.index, self.left, self.cores = index, left, cores
            self.width = owners * len(cores)
            self.base = 3 * 8 * owners * index
            self.owns = central & (core == 1) if len(cores) == 1 else central
            self.row = core if len(cores) == 2 else 0
            self.blocks, self.from_core, self.summed, self.from_chips = refs[:4]
            self.core_send, self.chip_send = refs[4:]

    plan = (
        Group(
            0, 0, (1,), blocks_a, from_core_a, summed_a, from_chips_a, core_send_a, chip_send_a
        ),
        Group(
            1, owners, (0, 1), blocks_b, from_core_b, summed_b, from_chips_b, core_send_b,
            chip_send_b,
        ),
    )

    middle = length // 2

    def load(colour, part):
        sites = slice(part * middle, (part + 1) * middle)
        sem = 4 * colour + 2 * part
        return (
            pltpu.make_async_copy(
                prop_hbm.at[:, colour, :, :, sites], prop.at[:, colour, :, :, sites],
                load_sem.at[sem],
            ),
            pltpu.make_async_copy(
                eig_hbm.at[:, colour, :, sites], eig.at[:, colour, :, sites], load_sem.at[sem + 1]
            ),
        )

    def start(copies):
        for copy in copies:
            copy.start()

    def finish(copies):
        for copy in copies:
            copy.wait()

    small_loads = tuple(
        pltpu.make_async_copy(remote_ref, own_ref, load_sem.at[12 + i])
        for i, (remote_ref, own_ref) in enumerate((
            (order_hbm, order), (table_hbm, table_weights), (term_rows_hbm, term_rows),
            (term_sign_hbm, term_sign),
        ))
    )
    start(load(0, 0))
    start(load(0, 1))
    barrier = pltpu.get_barrier_semaphore()
    each(1, n, lambda t: pl.semaphore_signal(
        barrier, inc=1, device_id={"space": lax.rem(me + t, n)}, device_id_type=MESH
    ))

    bits = EXTENT.bit_length() - 1
    low = EXTENT - 1

    def angles(p, site):
        coords = (site & low, (site >> bits) & low, site >> (2 * bits))
        winding = sum(step * coord for step, coord in zip(MOMENTA[p], coords) if step) & low
        return winding.astype(F32) * (2.0 * math.pi / EXTENT)

    tiles = length // 128
    compact = me * length + 128 * lax.broadcasted_iota(
        jnp.int32, (tiles, 128), 0
    ) + lax.broadcasted_iota(jnp.int32, (tiles, 128), 1)
    for slot, p in enumerate(moving):
        angle = angles(p, compact)
        for part, values in enumerate((jnp.cos(angle), jnp.sin(angle))):
            trig[2 * slot + part : 2 * slot + part + 1, :] = jnp.concatenate(
                [values[tile : tile + 1] for tile in range(tiles)], axis=1
            )
    for i, p in enumerate(fixed):
        angle = angles(p, 2 * length * lax.broadcasted_iota(jnp.int32, (chips, nvec), 0))
        turn[2 * i] = jnp.cos(angle)[:, None]
        turn[2 * i + 1] = jnp.sin(angle)[:, None]
    start(small_loads)
    start(load(1, 0))
    start(load(1, 1))

    def core_copy(group, colour):
        row = 1 - core if len(group.cores) == 2 else 0
        return remote(
            group.blocks.at[colour, row], group.from_core.at[colour], group.core_send,
            core_recv.at[group.index, colour], partner,
        )

    def exchange(group, colour):
        if len(group.cores) == 2:
            core_copy(group, colour).start()
        else:
            pl.when(core == 0)(lambda: core_copy(group, colour).start())

    def send_sums(group, colour):
        def run():
            core_copy(group, colour).wait_recv()

            def send(owner, other):
                group.summed[colour, owner] = (
                    group.blocks[colour, group.row, owner] + group.from_core[colour, owner]
                ).astype(BF16)
                remote(
                    group.summed.at[colour, owner], group.from_chips.at[colour, chip],
                    group.chip_send, chip_recv.at[group.index, colour], other * 2 + core,
                ).start()

            each_owner(send)

        if len(group.cores) == 2:
            run()
        else:
            pl.when(core == 1)(run)

    def project(group, colour, between):
        quarter = slots * 4 * group.width
        wide = -(-quarter // 128) * 128
        picked = slice(group.left, group.left + group.width)
        total = None
        for part in range(2):
            between(part)
            sites = slice(part * middle, (part + 1) * middle)
            real = prop[0, colour, picked, :, sites].astype(F32).reshape(4 * group.width, middle)
            imag = prop[1, colour, picked, :, sites].astype(F32).reshape(4 * group.width, middle)
            reals, imags = [real], [imag]
            for slot in range(len(moving)):
                cosine = trig[2 * slot : 2 * slot + 1, sites]
                sine = trig[2 * slot + 1 : 2 * slot + 2, sites]
                reals.append(cosine * real + sine * imag)
                imags.append(cosine * imag - sine * real)
            spare = [jnp.zeros((wide - quarter, middle), F32)] if wide > quarter else []
            rows = jnp.concatenate(reals + spare + imags + spare).astype(BF16)
            both = jnp.concatenate([eig[0, colour, :, sites], eig[1, colour, :, sites]])
            made = lax.dot_general(
                both, rows, (((1,), (1,)), ((), ())), preferred_element_type=F32
            )
            total = made if total is None else total + made
        with_real, with_imag = total[:nvec] * scale_in, total[nvec:] * scale_in
        real = (with_real[:, :wide] + with_imag[:, wide:]).T[:quarter]
        imag = (with_real[:, wide:] - with_imag[:, :wide]).T[:quarter]
        shape = (slots, len(group.cores), owners, 4, nvec)
        made = jnp.concatenate([real.reshape(shape), imag.reshape(shape)], axis=3)
        for slot in range(slots):
            group.blocks[colour, :, :, slot] = made[slot]

    def send_index(t):
        peer = lax.rem(me + t, n)
        remote(order.at[peer], wanted.at[me], index_send, index_recv, peer).start()

    for group in plan:
        opening = group.index == 0

        def stage(colour, group=group, opening=opening):
            def between(part):
                if opening:
                    finish(load(colour, part))
                    if part == 0:

                        @pl.when(colour == 0)
                        def _():
                            start(load(2, 0))
                            start(load(2, 1))

            project(group, colour, between)
            if opening:
                pl.when(colour == 0)(lambda: pl.semaphore_wait(barrier, n - 1))
            exchange(group, colour)

            @pl.when(colour == 0)
            def _():
                if opening:
                    finish(small_loads[:1])
                    each(1, n, send_index)
                    wanted[pl.ds(me, 1)] = order[pl.ds(me, 1)]
                else:
                    send_sums(plan[group.index - 1], 2)

            pl.when(colour > 0)(lambda: send_sums(group, colour - 1))

        each(0, 3, stage)
    send_sums(plan[-1], 2)

    terms = term_rows.shape[1]
    finish(small_loads[1:])

    def spread(cell, colour, sem):
        near_chips(
            lambda other: remote(
                cell, cell, sem, all_recv.at[1, colour], other * 2 + core
            ).start()
        )

    def pass_on(colour):
        cell = rest.at[colour, core * owners + lax.rem(place + depth, owners)]
        landed(cell, mate_recv.at[colour])
        spread(cell, colour, pass_send.at[colour])

    def contract(group):
        eye = lax.broadcasted_iota(jnp.int32, (terms, terms), 0) == lax.broadcasted_iota(
            jnp.int32, (terms, terms), 1
        )
        lane = lax.broadcasted_iota(jnp.int32, (terms, 24), 1)
        lane_channel = (4 * (lane >> 3) + (lane & 3)).astype(F32)
        lane_imag = (lane >> 2) & 1
        picks = []
        for which in range(2):
            row = term_rows[which : which + 1, :].astype(F32)
            column = jnp.sum(jnp.where(eye, row, 0.0), axis=1, keepdims=True)
            for part in range(2):
                hit = (lane_channel == column) & (lane_imag == part)
                picks.append(jnp.where(hit, 1.0, 0.0))
        picks = jnp.concatenate(picks).astype(BF16)
        sub = lax.broadcasted_iota(jnp.int32, (24, terms), 0)
        target = 4 * (sub >> 3) + (sub & 3) == term_rows[2:3, :]
        signs = (2 * term_sign[...] - 1).astype(F32)
        place_real = jnp.where(target & (((sub >> 2) & 1) == 0), signs, 0.0).astype(BF16)
        place_imag = jnp.where(target & (((sub >> 2) & 1) == 1), signs, 0.0).astype(BF16)
        weights = table_weights[sink[0, 0]]
        weight_real, weight_imag = weights[0:1, :], weights[1:2, :]

        totals = []
        for colour in range(3):
            own = group.blocks[colour, group.row, place] + group.from_core[colour, place]
            landed(
                group.from_chips.at[colour, pl.ds(0, chips - 1)], chip_recv.at[group.index, colour]
            )

            def turned(part, source_chip):
                kept = []
                for i in range(len(fixed)):
                    kept.append(turn[2 * i, pl.ds(source_chip, 1)][0] * part[0])
                    kept.append(turn[2 * i + 1, pl.ds(source_chip, 1)][0] * part[0])
                return kept

            def add_sum(t, carry, colour=colour):
                other = lax.rem(chip + chips - t, chips)
                part = group.from_chips[colour, other].astype(F32)
                return tuple(a + b for a, b in zip(carry, (part, *turned(part, other))))

            total, *kept = lax.fori_loop(1, chips, add_sum, (own, *turned(own, chip)))
            extra = [
                kept[2 * i] - swap_halves(kept[2 * i + 1]) for i in range(len(fixed))
            ]
            totals.append([total[slot] for slot in range(slots)] + extra)

        count = slots + len(fixed)
        block = jnp.concatenate([
            jnp.concatenate([total[unit] for total in totals]) for unit in range(count)
        ], axis=1)
        picked = dot_exact(picks, block)
        first_real, first_imag = picked[:terms], picked[terms : 2 * terms]
        other_real, other_imag = picked[2 * terms : 3 * terms], picked[3 * terms :]
        real_products, imag_products = [], []
        for unit in range(count):
            lanes = slice(unit * nvec, (unit + 1) * nvec)
            o_real, o_imag = other_real[:, lanes], other_imag[:, lanes]
            f_real, f_imag = first_real[:, lanes], first_imag[:, lanes]
            second_real = jnp.sum(
                weight_real * o_real - weight_imag * o_imag, axis=1, keepdims=True
            )
            second_imag = jnp.sum(
                weight_real * o_imag + weight_imag * o_real, axis=1, keepdims=True
            )
            real_products.append(f_real * second_real - f_imag * second_imag)
            imag_products.append(f_real * second_imag + f_imag * second_real)
        made = dot_exact(place_real, jnp.concatenate(real_products, axis=1)) + dot_exact(
            place_imag, jnp.concatenate(imag_products, axis=1)
        )
        if group.index > 0:
            for unit in range(count):
                part = made[:, unit * nvec : (unit + 1) * nvec].reshape(3, 8, nvec).astype(BF16)
                for colour in range(3):
                    rest[colour, core * owners + place, unit] = part[colour]

            mate = half - depth + lax.rem(place + depth, owners)

            def send_mate(colour):
                cell = rest.at[colour, core * owners + place]
                remote(cell, cell, all_send_b, mate_recv.at[colour], mate * 2 + core).start()

            each(0, 3, send_mate)
            each(
                0, 3,
                lambda colour: spread(rest.at[colour, core * owners + place], colour, all_send_b),
            )
            return
        acc[:24, :] = made[:, :nvec]
        for i in range(len(fixed)):
            acc[24 * (i + 1) : 24 * (i + 2), :] = made[:, (slots + i) * nvec : (slots + i + 1) * nvec]
        plain = made[:, nvec : slots * nvec].reshape(3, 8, (slots - 1) * nvec).astype(BF16)

        def merged(colour, other):
            value = acc[8 * colour : 8 * colour + 8, :]
            for i in range(len(fixed)):
                side_value = acc[24 * (i + 1) + 8 * colour : 24 * (i + 1) + 8 * colour + 8, :]
                value = value + turn[2 * i, other] * side_value
                value = value + turn[2 * i + 1, other] * swap_halves(side_value)
            return value.astype(BF16)

        for colour in range(3):
            others = [plain[colour, :, slot * nvec : (slot + 1) * nvec] for slot in range(slots - 1)]
            target = coeffs.at[colour, place]
            coeffs[colour, place, 0] = merged(colour, chip)
            for slot in range(slots - 1):
                coeffs[colour, place, slot + 1] = others[slot]

            def send_coeffs(other, colour=colour, others=others, target=target):
                ready[colour, other, 0] = merged(colour, other)
                for slot in range(slots - 1):
                    ready[colour, other, slot + 1] = others[slot]
                remote(
                    ready.at[colour, other], target, all_send_a, all_recv.at[group.index, colour],
                    other * 2 + core,
                ).start()

            far_chips(send_coeffs)
            near_chips(send_coeffs)

    def build(peer_chip):
        position = lax.broadcasted_iota(jnp.int32, (length, piece), 0)
        for which in range(2):
            local = wanted[pl.ds(peer_chip * 2 + which, 1)][0] - me * length
            onehot[pl.ds(peer_chip, 1), :, which * piece : (which + 1) * piece] = jnp.where(
                position == local, 1.0, 0.0
            ).astype(BF16)[None]

    def build_all():
        landed(wanted.at[pl.ds(0, n - 1)], index_recv)
        each(0, chips, build)

    def relay(group, colour):
        index = group.index

        def take(count):
            pieces = (coeffs, rest)[index].at[colour, pl.ds(0, count)]
            landed(pieces, all_recv.at[index, colour])

        def run():
            pl.when(central)(lambda: take(owners - 1 if index == 0 else owners - 2))
            pl.when(jnp.logical_not(central))(lambda: take(owners))
            if index == 0:
                cells = coeffs.at[colour]
            else:
                cells = rest.at[colour, pl.ds(core * owners, owners)]
            remote(
                cells, cells, (fwd_send_a, fwd_send_b)[index], fwd_recv.at[index, colour], partner
            ).start()

        if index == 0:
            pl.when(core == 1)(run)
        else:
            run()

    def rebuild(group, colour):
        height = group.width * slots * 8
        if group.index == 0:
            pl.when(core == 0)(lambda: landed(coeffs.at[colour], fwd_recv.at[0, colour]))
            lhs[: group.width] = coeffs[colour]
        else:
            landed(rest.at[colour, pl.ds((1 - core) * owners, owners)], fwd_recv.at[1, colour])
            table = rest[colour].reshape(group.width, slots + len(fixed), 8, nvec)
            still = table[:, 0].astype(F32)
            for i in range(len(fixed)):
                turned = table[:, slots + i].astype(F32)
                still = still + turn[2 * i, chip] * turned
                still = still + turn[2 * i + 1, chip] * swap_halves(turned)
            lhs[: group.width, 0] = still.astype(BF16)
            lhs[: group.width, 1:] = table[:, 1:slots]
        base = pl.multiple_of(group.base + colour * 8 * group.width, 8 * owners)

        def step(step):
            sites = pl.ds(pl.multiple_of(step * chunk, chunk), chunk)
            x, y = (
                jnp.dot(
                    lhs[: group.width].reshape(height, nvec), eig[part, colour, :, sites],
                    preferred_element_type=F32,
                ).reshape(group.width, slots, 8, chunk)
                for part in range(2)
            )
            straight, crossed = x[:, 0], y[:, 0]
            for slot in range(len(moving)):
                cosine = trig[2 * slot : 2 * slot + 1, sites][None]
                sine = trig[2 * slot + 1 : 2 * slot + 2, sites][None]
                straight = straight + cosine * x[:, slot + 1] - sine * y[:, slot + 1]
                crossed = crossed + cosine * y[:, slot + 1] + sine * x[:, slot + 1]
            made = (straight + swap_halves(crossed)) * scale_out
            source[pl.ds(base, 8 * group.width), sites] = made.reshape(
                8 * group.width, chunk
            ).astype(BF16)

        each(0, steps, step)

    def distribute(group, colours, far, last=False):
        picked = pl.ds(group.left, group.width)
        taken = pl.ds(colours[0], len(colours))
        height = 8 * group.width * len(colours)
        base = group.base + 8 * group.width * colours[0]
        if direct:
            lanes = pl.ds(pl.multiple_of(me * piece, piece), piece)
            target = out.at[:, taken, picked, :, lanes]
        else:
            target = out.at[me, :, taken, picked]

        def send_pieces(t):
            if far:
                swap = 1 - 2 * lax.rem(t, 2)
                if last:
                    swap = jnp.where((side == 0) | (t < half - 2), swap, 0)
                step = t + lax.rem(chip, 2) * swap
                other = jnp.where(side == 0, chips - 1 - step, step)
            else:
                local = chip - side * half
                step = jnp.where(t >= local, t + 1, t)
                other = side * half + jnp.where(t == half - 1, local, step)
            chosen = jnp.dot(
                source[base : base + height], onehot[other], preferred_element_type=F32
            )
            chosen = chosen.reshape(len(colours), group.width, 8, 2 * piece)
            for which in range(2):
                values = chosen[..., which * piece : (which + 1) * piece]
                for i, colour in enumerate(colours):
                    for part in range(2):
                        staged[
                            2 * other + which, part, colour, group.left : group.left + group.width
                        ] = values[i, :, 4 * part : 4 * part + 4].astype(BF16)

            def send(peer):
                remote(
                    staged.at[peer, :, taken, picked], target, out_send, out_recv, peer
                ).start()

            if far:
                send(2 * other)
                send(2 * other + 1)
            else:

                @pl.when(other != chip)
                def _():
                    send(2 * other)
                    send(2 * other + 1)

                @pl.when(other == chip)
                def _():
                    send(partner)
                    pltpu.make_async_copy(
                        staged.at[me, :, taken, picked], target, own_sem
                    ).start()

        each(0, half, send_pieces)

    early, late = plan
    pl.when(early.owns)(functools.partial(contract, early))
    build_all()
    relay(early, 0)
    pl.when(late.owns)(functools.partial(contract, late))
    rebuild(early, 0)
    distribute(early, (0,), True)
    each(1, 3, lambda colour: relay(early, colour))
    pl.when(central)(lambda: pass_on(0))
    each(1, 3, lambda colour: rebuild(early, colour))
    distribute(early, (1, 2), True)
    pl.when(central)(lambda: each(1, 3, pass_on))
    relay(late, 0)
    rebuild(late, 0)
    distribute(late, (0,), True)
    distribute(early, (0, 1, 2), False)
    each(1, 3, lambda colour: relay(late, colour))
    each(1, 3, lambda colour: rebuild(late, colour))
    distribute(late, (0, 1, 2), False)
    distribute(late, (1, 2), True, True)

    def close(group):
        pl.when(central)(lambda: sent(group.summed.at[:, pl.ds(0, owners - 1)], group.chip_send))
        pl.when(jnp.logical_not(central))(lambda: sent(group.summed, group.chip_send))

    @pl.when(core == 0)
    def _():
        sent(from_core_a, core_send_a)

    @pl.when(core == 1)
    def _():
        close(early)
        sent(coeffs, fwd_send_a)

    sent(from_core_b, core_send_b)
    close(late)
    sent(rest.at[:, pl.ds(0, owners)], fwd_send_b)

    @pl.when(early.owns)
    def _():
        sent(ready.at[:, pl.ds(0, chips - 1)], all_send_a)

    @pl.when(late.owns)
    def _():
        line = 8 * (slots + len(fixed)) * nvec // length
        sent(eig.at[0, :, pl.ds(0, half * line)], all_send_b)
        for colour in range(3):
            sent(prop.at[0, :, pl.ds(0, (half - 1) // 3)], pass_send.at[colour])

    sent(wanted.at[pl.ds(0, n - 1)], index_send)
    pltpu.make_async_copy(staged.at[0], staged.at[0], own_sem).wait()
    sent(staged.at[pl.ds(0, n - 1)], out_send)
    landed(staged.at[pl.ds(0, n - 1)], out_recv)


def on_device(
    propagator, eigvecs, operator_weights, sink_time, term_index, term_sign, solver_order
):
    columns, length = propagator.shape[3:]
    nvec = eigvecs.shape[2]
    n = lax.axis_size("space")
    chips = n // 2
    piece = length // n
    depth = columns // 6
    fixed = tuple(
        p for p in range(1, NMOM)
        if MOMENTA[p][:2] == (0, 0) and EXTENT * EXTENT % (2 * length) == 0
    )
    moving = tuple(p for p in range(1, NMOM) if p not in fixed)
    assert 6 * depth == columns and depth <= chips // 2 and (chips // 2 - 1) % 3 == 0
    slots = 1 + len(moving)
    owners = 2 * depth
    assert 8 * (slots + len(fixed)) * nvec == 4 * length
    cell = (slots, 8, nvec)
    direct = piece % 128 == 0
    out_shape = (2, 3, columns, 4, length) if direct else (n, 2, 3, columns, 4, piece)
    propagator = propagator.transpose(0, 1, 3, 2, 4)
    smem = pl.BlockSpec(memory_space=pltpu.SMEM)
    hbm = pl.BlockSpec(memory_space=pltpu.HBM)
    dma = pltpu.SemaphoreType.DMA
    gathered = pl.pallas_call(
        functools.partial(
            kernel, n, depth, columns, 1.0 / math.sqrt(3.0 * length * n),
            1.0 / math.sqrt(NMOM * nvec), length, moving, fixed, direct,
        ),
        out_shape=pltpu.VMEM(out_shape, BF16),
        in_specs=[hbm, hbm, smem, hbm, hbm, hbm, hbm],
        out_specs=pl.BlockSpec(memory_space=pl.ANY),
        scratch_shapes=[
            pltpu.VMEM(propagator.shape, BF16),
            pltpu.VMEM(eigvecs.shape, BF16),
            pltpu.VMEM(operator_weights.shape, F32),
            pltpu.VMEM(term_index.shape[::-1], jnp.int32),
            pltpu.VMEM((1,) + term_sign.shape, jnp.int32),
            pltpu.VMEM((n, 1, piece), jnp.int32),
            pltpu.VMEM((2 * len(moving), length), F32),
            pltpu.VMEM((2 * max(len(fixed), 1), chips, 1, nvec), F32),
            pltpu.VMEM((24 * (1 + len(fixed)), nvec), F32),
            pltpu.VMEM((3, 1, owners) + cell, F32),
            pltpu.VMEM((3, 2, owners) + cell, F32),
            pltpu.VMEM((3, owners) + cell, F32),
            pltpu.VMEM((3, owners) + cell, F32),
            pltpu.VMEM((3, owners) + cell, BF16),
            pltpu.VMEM((3, owners) + cell, BF16),
            pltpu.VMEM((3, chips) + cell, BF16),
            pltpu.VMEM((3, chips) + cell, BF16),
            pltpu.VMEM((3, chips) + cell, BF16),
            pltpu.VMEM((3, owners) + cell, BF16),
            pltpu.VMEM((3, 2 * owners, slots + len(fixed), 8, nvec), BF16),
            pltpu.VMEM((2 * owners, slots, 8, nvec), BF16),
            pltpu.VMEM((3 * 8 * 3 * owners, length), BF16),
            pltpu.VMEM((n, 1, piece), jnp.int32),
            pltpu.VMEM((chips, length, 2 * piece), BF16),
            pltpu.VMEM((n, 2, 3, columns, 4, piece), BF16),
            dma((16,)), dma((2, 3)), dma((2, 3)), dma((2, 3)), dma((2, 3)), dma((3,)), dma((3,)),
            dma((13,)),
        ],
        compiler_params=pltpu.CompilerParams(
            collective_id=0, has_side_effects=True, vmem_limit_bytes=int(48 * 2**20)
        ),
    )(
        *(
            x if x.size == 1 else pltpu.with_memory_space_constraint(x, pltpu.HBM)
            for x in (
                propagator, eigvecs, sink_time.reshape(1, 1), operator_weights,
                term_index.T, term_sign.reshape(1, -1), solver_order.reshape(n, 1, piece),
            )
        )
    )
    if direct:
        return gathered.transpose(0, 1, 3, 2, 4)
    placed = gathered.transpose(1, 2, 4, 3, 0, 5)
    return placed.reshape(2, 3, 4, columns, length)


def solution(mesh):
    return jax.shard_map(
        on_device,
        mesh=mesh,
        in_specs=(
            P("grp", None, None, None, "space"),
            P("grp", None, None, "space"),
            P("grp", None, None),
            P("grp"),
            P(),
            P(),
            P("space"),
        ),
        out_specs=P("grp", None, None, None, "space"),
        check_vma=False,
    )
```
